32 devices in a mesh: ep: 4 (over z), dp: 8 (over y, x, core).
Axes of the slice: x: 2, y: 2, z: 4, core: 2. Of those that a mesh axis runs over, the one named last changes fastest.
Arguments:
- tokens: bfloat16 [16384, 256], P(('dp', 'ep'))
- dy_out: bfloat16 [16384, 256], P(('dp', 'ep'))
- dense_w1: bfloat16 [256, 256], replicated
- route_idx1: int32 [16384, 2], P(('dp', 'ep'))
- route_gate1: float32 [16384, 2], P(('dp', 'ep'))
- w_gate1: bfloat16 [8, 256, 896], P('ep')
- w_up1: bfloat16 [8, 256, 896], P('ep')
- w_down1: bfloat16 [8, 896, 256], P('ep')
- dense_w2: bfloat16 [256, 256], replicated
- route_idx2: int32 [16384, 2], P(('dp', 'ep'))
- route_gate2: float32 [16384, 2], P(('dp', 'ep'))
- w_gate2: bfloat16 [8, 256, 896], P('ep')
- w_up2: bfloat16 [8, 256, 896], P('ep')
- w_down2: bfloat16 [8, 896, 256], P('ep')
Outputs:
- output 1: bfloat16 [16384, 256], P(('dp', 'ep'))
- output 2: bfloat16 [256, 256], P(('dp', 'ep'))
- output 3: bfloat16 [8, 256, 896], P('ep', 'dp')
- output 4: bfloat16 [8, 256, 896], P('ep', 'dp')
- output 5: bfloat16 [8, 896, 256], P('ep', None, 'dp')
- output 6: bfloat16 [256, 256], P(('dp', 'ep'))
- output 7: bfloat16 [8, 256, 896], P('ep', 'dp')
- output 8: bfloat16 [8, 256, 896], P('ep', 'dp')
- output 9: bfloat16 [8, 896, 256], P('ep', None, 'dp')
All inputs are finite; a program needn't handle non-finite values.
Results may differ from the reference program's by a relative error of at most 0.02.
Values are sent between devices in bfloat16 or wider.
A program may use at most 1 GiB of HBM per device.

```python
import jax
import jax.numpy as jnp

TOK = 512
D = 256
FF = 896
EXPERTS = 8
TOP = 2
SOURCES = 32
BASE = TOK * TOP // EXPERTS
CAPACITY = 2 * BASE


def draw_routing(key):
    key_tok, key_exp, key_shift = jax.random.split(key, 3)
    tok_order = jax.vmap(lambda src_key: jax.random.permutation(src_key, TOK))(jax.random.split(key_tok, SOURCES))
    exp_order = jax.vmap(lambda src_key: jax.random.permutation(src_key, EXPERTS))(jax.random.split(key_exp, SOURCES))
    shift = jax.random.randint(key_shift, (SOURCES, EXPERTS // 2), 0, BASE // 2 + 1, dtype=jnp.int32)
    shift = shift.at[:, 0].set(BASE)
    sizes = jnp.stack([BASE + shift, BASE - shift], axis=2).reshape(SOURCES, EXPERTS)
    block_end = jnp.cumsum(sizes, axis=1, dtype=jnp.int32)
    place = jnp.arange(TOP, dtype=jnp.int32)[None, None, :] * TOK + tok_order[:, :, None].astype(jnp.int32)
    block = jax.vmap(lambda end_row, place_row: jnp.searchsorted(end_row, place_row, side='right'))(block_end, place)
    expert = jnp.take_along_axis(exp_order, block.reshape(SOURCES, TOK * TOP), axis=1)
    return expert.reshape(SOURCES * TOK, TOP).astype(jnp.int32)


def setup_inputs(seed: int = 0) -> dict:
    keys = jax.random.split(jax.random.key(seed), 14)
    n_all = SOURCES * TOK

    def normal(key, shape, scale):
        return (scale * jax.random.normal(key, shape, jnp.float32)).astype(jnp.bfloat16)

    def gates(key):
        return jax.random.uniform(key, (n_all, TOP), jnp.float32, 0.5, 1.5) * TOP ** -0.5

    return {
        'tokens': normal(keys[0], (n_all, D), 1.0),
        'dy_out': normal(keys[1], (n_all, D), 1.0),
        'dense_w1': normal(keys[2], (D, D), 0.5 * D ** -0.5),
        'route_idx1': draw_routing(keys[3]),
        'route_gate1': gates(keys[4]),
        'w_gate1': normal(keys[5], (EXPERTS, D, FF), D ** -0.5),
        'w_up1': normal(keys[6], (EXPERTS, D, FF), D ** -0.5),
        'w_down1': normal(keys[7], (EXPERTS, FF, D), FF ** -0.5),
        'dense_w2': normal(keys[8], (D, D), 0.5 * D ** -0.5),
        'route_idx2': draw_routing(keys[9]),
        'route_gate2': gates(keys[10]),
        'w_gate2': normal(keys[11], (EXPERTS, D, FF), D ** -0.5),
        'w_up2': normal(keys[12], (EXPERTS, D, FF), D ** -0.5),
        'w_down2': normal(keys[13], (EXPERTS, FF, D), FF ** -0.5),
    }


def group_rows(route_idx, n_rows):
    flat_exp = route_idx.reshape(-1)
    n_copies = flat_exp.shape[0]
    order = jnp.argsort(flat_exp, stable=True).astype(jnp.int32)
    sorted_exp = jnp.take(flat_exp, order)
    counts = jnp.zeros((EXPERTS,), jnp.int32).at[flat_exp].add(1)
    starts = jnp.cumsum(counts, dtype=jnp.int32) - counts
    dest_row = (sorted_exp * n_rows + jnp.arange(n_copies, dtype=jnp.int32) - jnp.take(starts, sorted_exp)).astype(jnp.int32)
    return jnp.zeros((n_copies,), jnp.int32).at[order].set(dest_row).reshape(route_idx.shape)


def moe_layer(x_tok, dense_w, route_idx, route_gate, w_gate, w_up, w_down):
    n_all = x_tok.shape[0]
    n_rows = SOURCES * CAPACITY
    x_wide = x_tok.astype(jnp.float32)
    mixed = (x_wide + jnp.dot(x_wide, dense_w.astype(jnp.float32), preferred_element_type=jnp.float32)).astype(jnp.bfloat16)
    flat_pos = group_rows(route_idx, n_rows)
    tok_ids = jnp.broadcast_to(jnp.arange(n_all, dtype=jnp.int32)[:, None], route_idx.shape)
    row_tok = jnp.full((EXPERTS * n_rows,), n_all, jnp.int32).at[flat_pos.reshape(-1)].set(tok_ids.reshape(-1))
    buffer = jnp.take(mixed, row_tok, axis=0, mode='fill', fill_value=0).reshape(EXPERTS, n_rows, D).astype(jnp.float32)
    a_pre = jnp.einsum('erd,edf->erf', buffer, w_gate.astype(jnp.float32))
    b_pre = jnp.einsum('erd,edf->erf', buffer, w_up.astype(jnp.float32))
    hidden = (jax.nn.silu(a_pre) * b_pre).astype(jnp.bfloat16)
    expert_out = jnp.einsum('erf,efd->erd', hidden.astype(jnp.float32), w_down.astype(jnp.float32)).astype(jnp.bfloat16)
    picked = jnp.take(expert_out.reshape(EXPERTS * n_rows, D), flat_pos, axis=0).astype(jnp.float32)
    return (mixed.astype(jnp.float32) + jnp.sum(route_gate[:, :, None] * picked, axis=1)).astype(jnp.bfloat16)


def reference(tokens, dy_out, dense_w1, route_idx1, route_gate1, w_gate1, w_up1, w_down1, dense_w2, route_idx2, route_gate2, w_gate2, w_up2, w_down2):
    def forward(x_tok, dense_a, gate_a, up_a, down_a, dense_b, gate_b, up_b, down_b):
        mid_tok = moe_layer(x_tok, dense_a, route_idx1, route_gate1, gate_a, up_a, down_a)
        return moe_layer(mid_tok, dense_b, route_idx2, route_gate2, gate_b, up_b, down_b)

    y_out, pullback = jax.vjp(forward, tokens, dense_w1, w_gate1, w_up1, w_down1, dense_w2, w_gate2, w_up2, w_down2)
    (grad_tok, grad_dense1, grad_gate1, grad_up1, grad_down1, grad_dense2, grad_gate2, grad_up2, grad_down2) = pullback(dy_out)
    return (grad_tok, grad_dense1, grad_gate1, grad_up1, grad_down1, grad_dense2, grad_gate2, grad_up2, grad_down2)
```

```python
import functools

import jax
import jax.numpy as jnp
from jax import lax
from jax.experimental import pallas as pl
from jax.experimental.pallas import tpu as pltpu
from jax.sharding import PartitionSpec as P

MESH = pl.DeviceIdType.MESH
F32, BF16 = jnp.float32, jnp.bfloat16
N_EP = 4
N_EXP = 8
CAP = 256


def nn(a, b):
    return lax.dot_general(a, b, (((1,), (0,)), ((), ())), preferred_element_type=F32)


def nt(a, b):
    return lax.dot_general(a, b, (((1,), (1,)), ((), ())), preferred_element_type=F32)


def tn(a, b):
    return lax.dot_general(a, b, (((0,), (0,)), ((), ())), preferred_element_type=F32)


def kernel(n_dp, x_ref, dy_ref, dense1, dense2, idx1, gate1, idx2, gate2, aux_ref,
           wg1_hbm, wu1_hbm, wd1_hbm, wg2_hbm, wu2_hbm, wd2_hbm,
           dx_ref, gd1_ref, ge1_ref, gd2_ref, ge2_ref,
           w_gate, w_up, w_down, auxb, posr, gater, posc, gatec, tri, ag, ret, rows_in, t_a, t_b, t_gh, hid, g_a, g_b, g_out,
           acc, mid, g_mid, gs, gr, g2, d_send, d_a, d_bs, d_b,
           w_sem, aux_send, aux_recv, ag_right, ag_left, ag_recv, ret_send, ret_recv, pair_send, pair_recv,
           plane_send, plane_recv, da_send, da_recv, db_send, db_recv):
    z = lax.axis_index('ep')
    dp = lax.axis_index('dp')
    n_chip = n_dp // 2
    core = dp % 2
    chip = dp // 2
    n_tok, d_model = x_ref.shape
    d_ff = t_a.shape[1]
    piece = d_model // n_dp

    def order(k):
        near_low = jnp.where(z == 1, jnp.where(k == 0, 1, jnp.where(k == 1, 0, k)), k)
        near_high = 3 - jnp.where(z == 2, jnp.where(k == 0, 1, jnp.where(k == 1, 0, k)), k)
        return jnp.where(z < 2, near_low, near_high)

    barrier = pltpu.get_barrier_semaphore()
    for k in range(1, N_EP):
        pl.semaphore_signal(barrier, inc=1, device_id={'ep': (z + k) % N_EP, 'dp': dp}, device_id_type=MESH)
    for k in range(1, n_dp):
        pl.semaphore_signal(barrier, inc=1, device_id={'ep': z, 'dp': (dp + k) % n_dp}, device_id_type=MESH)

    w_copies = []
    for n, (hbm, dst) in enumerate(((wg1_hbm, w_gate.at[0]), (wu1_hbm, w_up.at[0]), (wd1_hbm, w_down.at[0]),
                                    (wg2_hbm, w_gate.at[1]), (wu2_hbm, w_up.at[1]), (wd2_hbm, w_down.at[1]))):
        w_copies.append(pltpu.make_async_copy(hbm, dst, w_sem.at[n]))
        w_copies[-1].start()

    x = x_ref[...]
    ag[0, z] = (x.astype(F32) + nn(x, dense1[...])).astype(BF16)
    ag[2, z] = dy_ref[...]
    auxb[z] = aux_ref[...]

    pl.semaphore_wait(barrier, N_EP - 1 + n_dp - 1)

    def col_copy(src, dst, send, recv, to):
        return pltpu.make_async_remote_copy(src_ref=src, dst_ref=dst, send_sem=send, recv_sem=recv,
                                            device_id={'ep': to, 'dp': dp}, device_id_type=MESH)

    def row_copy(src, dst, send, recv, to):
        return pltpu.make_async_remote_copy(src_ref=src, dst_ref=dst, send_sem=send, recv_sem=recv,
                                            device_id={'ep': z, 'dp': to}, device_id_type=MESH)

    def aux_copy(k):
        return col_copy(aux_ref, auxb.at[z], aux_send.at[k], aux_recv.at[z], (z + k) % N_EP)

    for k in range(1, N_EP):
        aux_copy(k).start()

    def ag_to_right(n, s):
        return col_copy(ag.at[n, s], ag.at[n, s], ag_right.at[n, s], ag_recv.at[n, s], jnp.minimum(z + 1, N_EP - 1))

    def ag_to_left(n, s):
        return col_copy(ag.at[n, s], ag.at[n, s], ag_left.at[n, s], ag_recv.at[n, s], jnp.maximum(z - 1, 0))

    def ag_pass(n, s):
        @pl.when(jnp.logical_and(s <= z, z < N_EP - 1))
        def _():
            ag_to_right(n, s).start()

        @pl.when(jnp.logical_and(s >= z, z > 0))
        def _():
            ag_to_left(n, s).start()

    def ag_take(n, s):
        ag_to_right(n, s).wait_recv()
        ag_pass(n, s)

    def ag_step(n, k):
        inner = jnp.logical_or(z == 1, z == 2)
        outer = jnp.logical_not(inner)

        @pl.when(k == 1)
        def _():
            ag_take(n, order(1))

        @pl.when(jnp.logical_or(jnp.logical_and(k == 1, inner), jnp.logical_and(k == 2, outer)))
        def _():
            ag_take(n, order(2))

        @pl.when(k == 3)
        def _():
            ag_take(n, order(3))

    def ag_drain(n):
        def body(s, carry):
            @pl.when(jnp.logical_and(s <= z, z < N_EP - 1))
            def _():
                ag_to_right(n, s).wait_send()

            @pl.when(jnp.logical_and(s >= z, z > 0))
            def _():
                ag_to_left(n, s).wait_send()
            return carry
        lax.fori_loop(0, N_EP, body, 0)

    def ret_copy(n, s):
        return col_copy(ret.at[n, 0, s], ret.at[n, 1, z], ret_send.at[n, s], ret_recv.at[n, z], s)

    def ret_wait(n, s):
        col_copy(ret.at[n, 0, s], ret.at[n, 1, s], ret_send.at[n, s], ret_recv.at[n, s], s).wait_recv()

    def ret_drain(n):
        for k in range(1, N_EP):
            ret_copy(n, (z + k) % N_EP).wait_send()

    ag_pass(0, z)

    r_io = lax.broadcasted_iota(jnp.int32, (n_tok, n_tok), 0)
    c_io = lax.broadcasted_iota(jnp.int32, (n_tok, n_tok), 1)
    tri[...] = (c_io < r_io).astype(F32).astype(BF16)
    lane = lax.broadcasted_iota(jnp.int32, (n_tok, N_EXP), 1)
    for layer, (idx, gate) in enumerate(((idx1, gate1), (idx2, gate2))):
        hit0 = idx[:, 0:1] == lane
        hit1 = idx[:, 1:2] == lane
        hit = jnp.logical_or(hit0, hit1)
        rank = nn(tri[...], hit.astype(F32).astype(BF16))
        posc[layer] = jnp.where(hit, rank, -1.0)
        gatec[layer] = jnp.where(hit0, gate[:, 0:1], 0.0) + jnp.where(hit1, gate[:, 1:2], 0.0)
    for k in range(1, N_EP):
        s = (z + k) % N_EP
        col_copy(aux_ref, auxb.at[s], aux_send.at[k], aux_recv.at[s], s).wait_recv()
    hits = []
    for layer in range(2):
        for s in range(N_EP):
            for e in range(2):
                a = auxb[s]
                expert = (z * 2 + e).astype(F32)
                hit0 = a[4 * layer:4 * layer + 1] == expert
                hit1 = a[4 * layer + 1:4 * layer + 2] == expert
                hits.append(jnp.logical_or(hit0, hit1).astype(F32))
                gater[(layer * N_EP + s) * 2 + e] = (jnp.where(hit0, a[4 * layer + 2:4 * layer + 3], 0.0)
                                                     + jnp.where(hit1, a[4 * layer + 3:4 * layer + 4], 0.0))
    stack = jnp.concatenate(hits, axis=0)
    ranks = jnp.where(stack > 0.5, nt(stack.astype(BF16), tri[...]), -1.0)
    for n in range(4 * N_EP):
        posr[n] = ranks[n:n + 1]

    for copy in w_copies:
        copy.wait()

    slot = lax.broadcasted_iota(jnp.int32, (CAP, n_tok), 0).astype(F32)
    slot_lane = lax.broadcasted_iota(jnp.int32, (n_tok, CAP), 1).astype(F32)

    def select(layer, s, e):
        return (posr[(layer * N_EP + s) * 2 + e] == slot)

    def up_project(layer, s, e):
        rows = rows_in[layer, e, s]
        t_a[...] = nn(rows, w_gate[layer, e])
        t_b[...] = nn(rows, w_up[layer, e])

    def take_rows(layer, s, e, n):
        pick = select(layer, s, e).astype(F32).astype(BF16)
        rows_in[layer, e, s] = nn(pick, ag[n, s]).astype(BF16)

    def forward(s, e):
        take_rows(0, s, e, 0)
        up_project(0, s, e)

        def body(i, carry):
            r = pl.ds(i * 32, 32)
            a = t_a[r, :]
            hid[e, s, r, :] = (a * jax.nn.sigmoid(a) * t_b[r, :]).astype(BF16)
            return carry
        lax.fori_loop(0, CAP // 32, body, 0)
        out = nn(hid[e, s], w_down[0, e]).astype(BF16)
        ret[0, jnp.where(s == z, 1, 0), s, e] = out

    def backward(layer, s, e, n_dy, n_ret):
        up_project(layer, s, e)
        pick = select(layer, s, e)
        gate = jnp.sum(jnp.where(pick, gater[(layer * N_EP + s) * 2 + e], 0.0), axis=1, keepdims=True)
        g_out[e, s] = (nn(pick.astype(F32).astype(BF16), ag[n_dy, s]) * gate).astype(BF16)
        t_gh[...] = nt(g_out[e, s], w_down[layer, e]).astype(BF16)

        def body(i, carry):
            r = pl.ds(i * 32, 32)
            a = t_a[r, :]
            b = t_b[r, :]
            gh = t_gh[r, :].astype(F32)
            sig = jax.nn.sigmoid(a)
            hid[e, s, r, :] = (a * sig * b).astype(BF16)
            g_a[e, s, r, :] = (gh * b * sig * (1.0 + a * (1.0 - sig))).astype(BF16)
            g_b[e, s, r, :] = (gh * a * sig).astype(BF16)
            return carry
        lax.fori_loop(0, CAP // 32, body, 0)
        ret[n_ret, jnp.where(s == z, 1, 0), s, e] = (nt(g_a[e, s], w_gate[layer, e])
                                                     + nt(g_b[e, s], w_up[layer, e])).astype(BF16)

    def send_back(n, s):
        @pl.when(s != z)
        def _():
            ret_copy(n, s).start()

    def gather_back(n, layer, weighted):
        acc[...] = jnp.zeros_like(acc)

        def body(k, carry):
            s = order(k)

            @pl.when(k > 0)
            def _():
                ret_wait(n, s)

            for e in range(2):
                here = lane == s * 2 + e
                pos = jnp.sum(jnp.where(here, posc[layer], 0.0), axis=1, keepdims=True)
                got = nn((pos == slot_lane).astype(F32).astype(BF16), ret[n, 1, s, e])
                if weighted:
                    got = got * jnp.sum(jnp.where(here, gatec[layer], 0.0), axis=1, keepdims=True)
                acc[...] += got
            return carry
        lax.fori_loop(0, N_EP, body, 0)

    def weight_grads(layer):
        def body(e, carry):
            rows = rows_in[layer, e].reshape(N_EP * CAP, d_model)
            outs = g_out[e].reshape(N_EP * CAP, d_model)
            for q, (left, right) in enumerate(((rows, g_a), (rows, g_b), (outs, hid))):
                grad = tn(left, right[e].reshape(N_EP * CAP, d_ff)).astype(BF16)
                for p in range(n_dp):
                    gs[p % 2, p // 2, q * 2 + e] = grad[p * piece:(p + 1) * piece]
            return carry
        lax.fori_loop(0, 2, body, 0)

    def pair_copy(layer):
        return row_copy(gs.at[1 - core], gr.at[layer], pair_send.at[layer], pair_recv.at[layer], chip * 2 + 1 - core)

    def plane_copy(layer, k):
        to = (chip + k) % n_chip
        return row_copy(gr.at[layer, to], g2.at[layer, chip], plane_send.at[layer, k], plane_recv.at[layer, chip], to * 2 + core)

    def pair_sum(layer):
        pair_copy(layer).wait()

        def body(i, carry):
            c = i // 6
            j = i % 6
            gr[layer, c, j] = (gr[layer, c, j].astype(F32) + gs[core, c, j].astype(F32)).astype(BF16)
            return carry
        lax.fori_loop(0, n_chip * 6, body, 0)
        for k in range(1, n_chip):
            plane_copy(layer, k).start()

    def plane_sum(layer, out_ref):
        for k in range(1, n_chip):
            frm = (chip + k) % n_chip
            row_copy(gr.at[layer, frm], g2.at[layer, frm], plane_send.at[layer, k], plane_recv.at[layer, frm], frm * 2 + core).wait_recv()

        def body(j, carry):
            total = gr[layer, chip, j].astype(F32)
            for k in range(1, n_chip):
                total += g2[layer, (chip + k) % n_chip, j].astype(F32)
            out_ref[j] = total.astype(BF16)
            return carry
        lax.fori_loop(0, 6, body, 0)
        for k in range(1, n_chip):
            plane_copy(layer, k).wait_send()

    def da_copy(layer, k):
        to = (dp + k) % n_dp
        return row_copy(d_send.at[layer, to], d_a.at[layer, dp], da_send.at[layer, k], da_recv.at[layer, dp], to)

    def db_copy(layer, k):
        to = (z + k) % N_EP
        return col_copy(d_bs.at[layer, to], d_b.at[layer, z], db_send.at[layer, k], db_recv.at[layer, z], to)

    def dense_start(layer, grad):
        for p in range(n_dp):
            d_send[layer, p] = grad[p * piece:(p + 1) * piece].astype(BF16)
        for k in range(1, n_dp):
            da_copy(layer, k).start()

    def dense_middle(layer):
        for k in range(1, n_dp):
            frm = (dp + k) % n_dp
            row_copy(d_send.at[layer, frm], d_a.at[layer, frm], da_send.at[layer, k], da_recv.at[layer, frm], frm).wait_recv()
        total = d_send[layer, dp].astype(F32)
        for k in range(1, n_dp):
            total += d_a[layer, (dp + k) % n_dp].astype(F32)
        sub = piece // N_EP
        for p in range(N_EP):
            d_bs[layer, p] = total[p * sub:(p + 1) * sub].astype(BF16)
        for k in range(1, N_EP):
            db_copy(layer, k).start()

    def dense_end(layer, out_ref):
        for k in range(1, N_EP):
            frm = (z + k) % N_EP
            col_copy(d_bs.at[layer, frm], d_b.at[layer, frm], db_send.at[layer, k], db_recv.at[layer, frm], frm).wait_recv()
        total = d_bs[layer, z].astype(F32)
        for k in range(1, N_EP):
            total += d_b[layer, (z + k) % N_EP].astype(F32)
        out_ref[...] = total.astype(BF16)
        for k in range(1, n_dp):
            da_copy(layer, k).wait_send()
        for k in range(1, N_EP):
            db_copy(layer, k).wait_send()

    def forward_step(k, carry):
        s = order(k)
        ag_step(0, k)

        def experts(e, c):
            forward(s, e)
            return c
        lax.fori_loop(0, 2, experts, 0)
        send_back(0, s)
        return carry
    lax.fori_loop(0, N_EP, forward_step, 0)
    ag_pass(2, z)
    gather_back(0, 0, True)
    y = (ag[0, z].astype(F32) + acc[...]).astype(BF16)
    mid[...] = y
    ag[1, z] = (y.astype(F32) + nn(y, dense2[...])).astype(BF16)
    ag_pass(1, z)

    def second_step(k, carry):
        s = order(k)
        ag_step(2, k)
        ag_step(1, k)

        def experts(e, c):
            take_rows(1, s, e, 1)
            backward(1, s, e, 2, 1)
            return c
        lax.fori_loop(0, 2, experts, 0)
        send_back(1, s)
        return carry
    lax.fori_loop(0, N_EP, second_step, 0)
    weight_grads(1)
    pair_copy(1).start()
    gather_back(1, 1, False)
    gm = (dy_ref[...].astype(F32) + acc[...]).astype(BF16)
    gx = (gm.astype(F32) + nt(gm, dense2[...])).astype(BF16)
    g_mid[...] = gx
    ag[3, z] = gx
    ag_pass(3, z)
    dense_start(1, tn(mid[...], gm))
    pair_sum(1)

    def first_step(k, carry):
        s = order(k)
        ag_step(3, k)

        def experts(e, c):
            backward(0, s, e, 3, 2)
            return c
        lax.fori_loop(0, 2, experts, 0)
        send_back(2, s)
        return carry
    lax.fori_loop(0, N_EP, first_step, 0)
    weight_grads(0)
    pair_copy(0).start()
    dense_middle(1)
    pair_sum(0)
    gather_back(2, 0, False)
    gm1 = (g_mid[...].astype(F32) + acc[...]).astype(BF16)
    dense_start(0, tn(x_ref[...], gm1))
    dx_ref[...] = (gm1.astype(F32) + nt(gm1, dense1[...])).astype(BF16)
    plane_sum(1, ge2_ref)
    dense_middle(0)
    plane_sum(0, ge1_ref)
    dense_end(1, gd2_ref)
    dense_end(0, gd1_ref)
    for n in range(4):
        ag_drain(n)
    for n in range(3):
        ret_drain(n)
    for k in range(1, N_EP):
        aux_copy(k).wait_send()


def solution(mesh):
    n_dp = mesh.shape['dp']
    n_chip = n_dp // 2
    tok_spec = P(('dp', 'ep'), None)
    exp_spec = P('ep', None, None)
    layer_specs = (P(None, None), tok_spec, tok_spec, exp_spec, exp_spec, exp_spec)
    grad_specs = (P(('dp', 'ep'), None), P('ep', 'dp', None), P('ep', 'dp', None), P('ep', None, 'dp'))

    def local_step(tokens, dy_out, dense_w1, idx1, gate1, wg1, wu1, wd1, dense_w2, idx2, gate2, wg2, wu2, wd2):
        n_tok, d_model = tokens.shape
        d_ff = wg1.shape[2]
        piece = d_model // n_dp
        sub = piece // N_EP
        aux = jnp.concatenate([idx1.astype(F32), gate1, idx2.astype(F32), gate2], axis=1).T
        vmem = pl.BlockSpec(memory_space=pltpu.VMEM)
        hbm = pl.BlockSpec(memory_space=pl.ANY)
        dma = pltpu.SemaphoreType.DMA
        outs = pl.pallas_call(
            functools.partial(kernel, n_dp),
            out_shape=(jax.ShapeDtypeStruct((n_tok, d_model), BF16),
                       jax.ShapeDtypeStruct((sub, d_model), BF16), jax.ShapeDtypeStruct((6, piece, d_ff), BF16),
                       jax.ShapeDtypeStruct((sub, d_model), BF16), jax.ShapeDtypeStruct((6, piece, d_ff), BF16)),
            in_specs=[vmem] * 9 + [hbm] * 6,
            out_specs=[vmem] * 5,
            scratch_shapes=[
                pltpu.VMEM((2, 2, d_model, d_ff), BF16), pltpu.VMEM((2, 2, d_model, d_ff), BF16), pltpu.VMEM((2, 2, d_ff, d_model), BF16),
                pltpu.VMEM((N_EP, 8, n_tok), F32), pltpu.VMEM((4 * N_EP, 1, n_tok), F32), pltpu.VMEM((4 * N_EP, 1, n_tok), F32),
                pltpu.VMEM((2, n_tok, N_EXP), F32), pltpu.VMEM((2, n_tok, N_EXP), F32), pltpu.VMEM((n_tok, n_tok), BF16),
                pltpu.VMEM((4, N_EP, n_tok, d_model), BF16), pltpu.VMEM((3, 2, N_EP, 2, CAP, d_model), BF16),
                pltpu.VMEM((2, 2, N_EP, CAP, d_model), BF16), pltpu.VMEM((CAP, d_ff), F32), pltpu.VMEM((CAP, d_ff), F32),
                pltpu.VMEM((CAP, d_ff), BF16), pltpu.VMEM((2, N_EP, CAP, d_ff), BF16), pltpu.VMEM((2, N_EP, CAP, d_ff), BF16),
                pltpu.VMEM((2, N_EP, CAP, d_ff), BF16), pltpu.VMEM((2, N_EP, CAP, d_model), BF16),
                pltpu.VMEM((n_tok, d_model), F32), pltpu.VMEM((n_tok, d_model), BF16), pltpu.VMEM((n_tok, d_model), BF16),
                pltpu.VMEM((2, n_chip, 6, piece, d_ff), BF16), pltpu.VMEM((2, n_chip, 6, piece, d_ff), BF16),
                pltpu.VMEM((2, n_chip, 6, piece, d_ff), BF16),
                pltpu.VMEM((2, n_dp, piece, d_model), BF16), pltpu.VMEM((2, n_dp, piece, d_model), BF16),
                pltpu.VMEM((2, N_EP, sub, d_model), BF16), pltpu.VMEM((2, N_EP, sub, d_model), BF16),
                dma((6,)), dma((N_EP,)), dma((N_EP,)), dma((4, N_EP)), dma((4, N_EP)), dma((4, N_EP)), dma((3, N_EP)), dma((3, N_EP)),
                dma((2,)), dma((2,)), dma((2, n_chip)), dma((2, n_chip)), dma((2, n_dp)), dma((2, n_dp)), dma((2, N_EP)), dma((2, N_EP)),
            ],
            compiler_params=pltpu.CompilerParams(collective_id=0, has_side_effects=True, vmem_limit_bytes=67043328),
        )(tokens, dy_out, dense_w1, dense_w2, idx1, gate1, idx2, gate2, aux, wg1, wu1, wd1, wg2, wu2, wd2)
        grad_tok, gd1, ge1, gd2, ge2 = outs
        res = [grad_tok]
        for gd, ge in ((gd1, ge1), (gd2, ge2)):
            res += [gd, ge[0:2], ge[2:4], jnp.swapaxes(ge[4:6], 1, 2)]
        return tuple(res)

    return jax.shard_map(local_step, mesh=mesh, in_specs=(tok_spec, tok_spec) + layer_specs + layer_specs,
                         out_specs=(tok_spec,) + grad_specs + grad_specs, check_vma=False)
```

```python
import functools

import jax
import jax.numpy as jnp
from jax import lax
from jax.experimental import pallas as pl
from jax.experimental.pallas import tpu as pltpu
from jax.sharding import PartitionSpec as P

MESH = pl.DeviceIdType.MESH
F32, BF16 = jnp.float32, jnp.bfloat16
N_EP = 4
scope = jax.named_scope
N_EXP = 8
CAP = 256


def nn(a, b):
    return lax.dot_general(a, b, (((1,), (0,)), ((), ())), preferred_element_type=F32)


def nt(a, b):
    return lax.dot_general(a, b, (((1,), (1,)), ((), ())), preferred_element_type=F32)


def tn(a, b):
    return lax.dot_general(a, b, (((0,), (0,)), ((), ())), preferred_element_type=F32)


def kernel(n_dp, x_ref, dy_ref, dense1, dense2, idx1, gate1, idx2, gate2,
           wg1_hbm, wu1_hbm, wd1_hbm, wg2_hbm, wu2_hbm, wd2_hbm,
           tok_out, exp_out,
           w_gate, w_up, w_down, auxs, auxb, posr, gater, posc, gatec, tri, ag, ret, back_out, back_in, rows_in, t_a, t_b, t_gh, hid, g_a, g_b, g_out,
           acc, mid, g_mid, gs, gr, g2, d_send, d_a, d_bs, d_b,
           w_sem, aux_send, aux_recv, ag_right, ag_left, ag_recv, ret_send, ret_recv, back_send, back_recv, pair_send, pair_recv,
           plane_send, plane_recv, da_send, da_recv, db_send, db_recv):
    z = lax.axis_index('ep')
    dp = lax.axis_index('dp')
    n_chip = n_dp // 2
    core = dp % 2
    chip = dp // 2
    n_tok, d_model = x_ref.shape
    d_ff = t_a.shape[2]
    piece = d_model // n_dp

    def order(k):
        near_low = jnp.where(z == 1, jnp.where(k == 0, 1, jnp.where(k == 1, 0, k)), k)
        near_high = 3 - jnp.where(z == 2, jnp.where(k == 0, 1, jnp.where(k == 1, 0, k)), k)
        return jnp.where(z < 2, near_low, near_high)

    barrier = pltpu.get_barrier_semaphore()
    for k in range(1, N_EP):
        pl.semaphore_signal(barrier, inc=1, device_id={'ep': (z + k) % N_EP, 'dp': dp}, device_id_type=MESH)
    for k in range(1, n_dp):
        pl.semaphore_signal(barrier, inc=1, device_id={'ep': z, 'dp': (dp + k) % n_dp}, device_id_type=MESH)

    w_copies = []
    for n, (hbm, dst) in enumerate(((wg1_hbm, w_gate.at[0]), (wu1_hbm, w_up.at[0]), (wd1_hbm, w_down.at[0]),
                                    (wg2_hbm, w_gate.at[1]), (wu2_hbm, w_up.at[1]), (wd2_hbm, w_down.at[1]))):
        w_copies.append(pltpu.make_async_copy(hbm, dst, w_sem.at[n]))
        w_copies[-1].start()

    auxs[0:2] = idx1[...].astype(F32)
    auxs[2:4] = gate1[...]
    auxs[4:6] = idx2[...].astype(F32)
    auxs[6:8] = gate2[...]
    x = x_ref[...]
    ag[0, z] = (x.astype(F32) + nn(x, dense1[...])).astype(BF16)
    ag[2, z] = dy_ref[...]
    auxb[z] = auxs[...]

    with scope('barrier'):
        pl.semaphore_wait(barrier, N_EP - 1 + n_dp - 1)

    def col_copy(src, dst, send, recv, to):
        return pltpu.make_async_remote_copy(src_ref=src, dst_ref=dst, send_sem=send, recv_sem=recv,
                                            device_id={'ep': to, 'dp': dp}, device_id_type=MESH)

    def row_copy(src, dst, send, recv, to):
        return pltpu.make_async_remote_copy(src_ref=src, dst_ref=dst, send_sem=send, recv_sem=recv,
                                            device_id={'ep': z, 'dp': to}, device_id_type=MESH)

    def aux_copy(k):
        return col_copy(auxs, auxb.at[z], aux_send.at[k], aux_recv.at[z], (z + k) % N_EP)

    for k in range(1, N_EP):
        aux_copy(k).start()

    def ag_to_right(n, s):
        return col_copy(ag.at[n, s], ag.at[n, s], ag_right.at[n, s], ag_recv.at[n, s], jnp.minimum(z + 1, N_EP - 1))

    def ag_to_left(n, s):
        return col_copy(ag.at[n, s], ag.at[n, s], ag_left.at[n, s], ag_recv.at[n, s], jnp.maximum(z - 1, 0))

    def ag_pass(n, s):
        @pl.when(jnp.logical_and(s <= z, z < N_EP - 1))
        def _():
            ag_to_right(n, s).start()

        @pl.when(jnp.logical_and(s >= z, z > 0))
        def _():
            ag_to_left(n, s).start()

    def ag_take(n, s):
        with scope('agw%d' % n):
            ag_to_right(n, s).wait_recv()
        ag_pass(n, s)

    def ag_step(n, k):
        inner = jnp.logical_or(z == 1, z == 2)
        outer = jnp.logical_not(inner)

        @pl.when(k == 1)
        def _():
            ag_take(n, order(1))

        @pl.when(jnp.logical_or(jnp.logical_and(k == 1, inner), jnp.logical_and(k == 2, outer)))
        def _():
            ag_take(n, order(2))

        @pl.when(k == 3)
        def _():
            ag_take(n, order(3))

    def ag_drain(n):
        def body(s, carry):
            @pl.when(jnp.logical_and(s <= z, z < N_EP - 1))
            def _():
                ag_to_right(n, s).wait_send()

            @pl.when(jnp.logical_and(s >= z, z > 0))
            def _():
                ag_to_left(n, s).wait_send()
            return carry
        lax.fori_loop(0, N_EP, body, 0)

    def ret_copy(s):
        return col_copy(ret.at[0, s], ret.at[1, z], ret_send.at[s], ret_recv.at[z], s)

    def ret_wait(s):
        col_copy(ret.at[0, s], ret.at[1, s], ret_send.at[s], ret_recv.at[s], s).wait_recv()

    def ret_drain():
        for k in range(1, N_EP):
            ret_copy((z + k) % N_EP).wait_send()

    ag_pass(0, z)

    r_io = lax.broadcasted_iota(jnp.int32, (n_tok, n_tok), 0)
    c_io = lax.broadcasted_iota(jnp.int32, (n_tok, n_tok), 1)
    tri[...] = (c_io < r_io).astype(F32).astype(BF16)
    lane = lax.broadcasted_iota(jnp.int32, (n_tok, N_EXP), 1)
    cols = auxs[...].T
    for layer in range(2):
        hit0 = cols[:, 4 * layer:4 * layer + 1] == lane.astype(F32)
        hit1 = cols[:, 4 * layer + 1:4 * layer + 2] == lane.astype(F32)
        hit = jnp.logical_or(hit0, hit1)
        rank = nn(tri[...], hit.astype(F32).astype(BF16))
        posc[layer] = jnp.where(hit, rank, -1.0)
        gatec[layer] = jnp.where(hit0, cols[:, 4 * layer + 2:4 * layer + 3], 0.0) + jnp.where(hit1, cols[:, 4 * layer + 3:4 * layer + 4], 0.0)
    for k in range(1, N_EP):
        s = (z + k) % N_EP
        col_copy(auxs, auxb.at[s], aux_send.at[k], aux_recv.at[s], s).wait_recv()
    hits = []
    for layer in range(2):
        for s in range(N_EP):
            for e in range(2):
                a = auxb[s]
                expert = (z * 2 + e).astype(F32)
                hit0 = a[4 * layer:4 * layer + 1] == expert
                hit1 = a[4 * layer + 1:4 * layer + 2] == expert
                hits.append(jnp.logical_or(hit0, hit1).astype(F32))
                gater[(layer * N_EP + s) * 2 + e] = (jnp.where(hit0, a[4 * layer + 2:4 * layer + 3], 0.0)
                                                     + jnp.where(hit1, a[4 * layer + 3:4 * layer + 4], 0.0))
    stack = jnp.concatenate(hits, axis=0)
    ranks = jnp.where(stack > 0.5, nt(stack.astype(BF16), tri[...]), -1.0)
    for n in range(4 * N_EP):
        posr[n] = ranks[n:n + 1]

    for copy in w_copies:
        copy.wait()

    slot = lax.broadcasted_iota(jnp.int32, (CAP, n_tok), 0).astype(F32)
    slot_lane = lax.broadcasted_iota(jnp.int32, (n_tok, CAP), 1).astype(F32)
    step = 32

    def select(layer, s):
        at = (layer * N_EP + s) * 2
        return [posr[at + e] == slot for e in range(2)]

    def as_bf16(picks):
        return jnp.concatenate([p.astype(F32).astype(BF16) for p in picks], axis=0)

    def take_rows(layer, s, n, pick):
        rows = nn(pick, ag[n, s]).astype(BF16)
        for e in range(2):
            rows_in[layer, e, s] = rows[e * CAP:(e + 1) * CAP]

    def up_project(layer, s, e):
        rows = rows_in[layer, e, s]
        t_a[e] = nn(rows, w_gate[layer, e])
        t_b[e] = nn(rows, w_up[layer, e])

    def forward(s):
        take_rows(0, s, 0, as_bf16(select(0, s)))
        for e in range(2):
            up_project(0, s, e)
        for e in range(2):
            for i in range(CAP // step):
                r = pl.ds(i * step, step)
                a = t_a[e, r, :]
                hid[e, s, r, :] = (a * jax.nn.sigmoid(a) * t_b[e, r, :]).astype(BF16)
            ret[jnp.where(s == z, 1, 0), s, e] = nn(hid[e, s], w_down[0, e]).astype(BF16)

    def backward(layer, s, n_dy, n_back, n_u):
        picks = select(layer, s)
        pick = as_bf16(picks)
        at = (layer * N_EP + s) * 2
        if n_u is not None:
            take_rows(layer, s, n_u, pick)
        got = nn(pick, ag[n_dy, s])
        for e in range(2):
            gate = jnp.sum(jnp.where(picks[e], gater[at + e], 0.0), axis=1, keepdims=True)
            g_out[e, s] = (got[e * CAP:(e + 1) * CAP] * gate).astype(BF16)
        for e in range(2):
            up_project(layer, s, e)
            t_gh[e] = nt(g_out[e, s], w_down[layer, e]).astype(BF16)
        parts = []
        for e in range(2):
            for i in range(CAP // step):
                r = pl.ds(i * step, step)
                a = t_a[e, r, :]
                b = t_b[e, r, :]
                gh = t_gh[e, r, :].astype(F32)
                sig = jax.nn.sigmoid(a)
                act = a * sig
                hid[e, s, r, :] = (act * b).astype(BF16)
                g_a[e, s, r, :] = (gh * b * sig * (1.0 + a * (1.0 - sig))).astype(BF16)
                g_b[e, s, r, :] = (gh * act).astype(BF16)
            parts.append((nt(g_a[e, s], w_gate[layer, e]) + nt(g_b[e, s], w_up[layer, e])).astype(BF16))
        back_out[n_back, s] = tn(pick, jnp.concatenate(parts, axis=0)).astype(BF16)

    def send_back(s):
        @pl.when(s != z)
        def _():
            ret_copy(s).start()

    def gather_back():
        acc[...] = jnp.zeros_like(acc)

        def body(k, carry):
            s = order(k)

            @pl.when(k > 0)
            def _():
                with scope('retw'):
                    ret_wait(s)

            for e in range(2):
                here = lane == s * 2 + e
                pos = jnp.sum(jnp.where(here, posc[0], 0.0), axis=1, keepdims=True)
                weight = jnp.sum(jnp.where(here, gatec[0], 0.0), axis=1, keepdims=True)
                acc[...] += nn((pos == slot_lane).astype(F32).astype(BF16), ret[1, s, e]) * weight
            return carry
        lax.fori_loop(0, N_EP, body, 0)

    inner = jnp.logical_or(z == 1, z == 2)
    outer = jnp.logical_not(inner)
    beside = jnp.where(z < 2, 1, 2)
    near_end = jnp.where(z < 2, 0, 3)

    def back_copy(n, s, slot_in, to):
        return col_copy(back_out.at[n, s], back_in.at[n, slot_in], back_send.at[n, s], back_recv.at[n, slot_in], to)

    def back_plan(s):
        dist = jnp.abs(z - s)
        slot_in = jnp.where(inner, 0, jnp.where(dist == 1, 2, jnp.where(dist == 2, 1, 3)))
        to = jnp.where(inner, 3 - z, jnp.where(dist == 2, beside, s))
        go = jnp.where(inner, dist == 2, dist > 0)
        return slot_in, to, go

    def back_start(n, s):
        slot_in, to, go = back_plan(s)

        @pl.when(go)
        def _():
            back_copy(n, s, slot_in, to).start()

    def back_wait(n, slot_in):
        with scope('bk%d%d' % (n, slot_in)):
            back_copy(n, 0, slot_in, z).wait_recv()

    def back_merge(n):
        @pl.when(inner)
        def _():
            for slot_in, s, slot_out in ((0, near_end, 2), (1, 3 - z, 3)):
                back_wait(n, slot_in)
                back_out[n, s] = (back_out[n, s].astype(F32) + back_in[n, slot_in].astype(F32)).astype(BF16)
                back_copy(n, s, slot_out, s).start()

    def back_sum(n):
        back_wait(n, 2)
        back_wait(n, 3)
        return back_out[n, z].astype(F32) + back_in[n, 2].astype(F32) + back_in[n, 3].astype(F32)

    def back_drain(n):
        for k in range(1, N_EP):
            back_copy(n, (z + k) % N_EP, 0, z).wait_send()

    def pair_copy(layer, j):
        return row_copy(gs.at[1 - core, j], gr.at[layer, j], pair_send.at[layer, j], pair_recv.at[layer, j], chip * 2 + 1 - core)

    def plane_copy(layer, j, k):
        to = (chip + k) % n_chip
        return row_copy(gr.at[layer, j, to], g2.at[layer, j, chip], plane_send.at[layer, j, k], plane_recv.at[layer, j, chip], to * 2 + core)

    def pair_finish(layer, j):
        pair_copy(layer, j).wait()
        for c in range(n_chip):
            gr[layer, j, c] = (gr[layer, j, c].astype(F32) + gs[core, j, c].astype(F32)).astype(BF16)
        for k in range(1, n_chip):
            plane_copy(layer, j, k).start()

    def weight_grads(layer):
        def body(e, carry):
            rows = rows_in[layer, e].reshape(N_EP * CAP, d_model)
            outs = g_out[e].reshape(N_EP * CAP, d_model)
            for q, (left, right) in enumerate(((outs, hid), (rows, g_a), (rows, g_b))):
                grad = tn(left, right[e].reshape(N_EP * CAP, d_ff)).astype(BF16)
                j = (q + 2) % 3 * 2 + e
                for p in range(n_dp):
                    gs[p % 2, j, p // 2] = grad[p * piece:(p + 1) * piece]
                pair_copy(layer, j).start()

                @pl.when(e > 0)
                def _():
                    pair_finish(layer, j - 1)
            return carry
        lax.fori_loop(0, 2, body, 0)
        for q in range(3):
            pair_finish(layer, (q + 2) % 3 * 2 + 1)

    def plane_sum(layer):
        def body(j, carry):
            total = gr[layer, j, chip].astype(F32)
            for k in range(1, n_chip):
                frm = (chip + k) % n_chip
                row_copy(gr.at[layer, j, frm], g2.at[layer, j, frm], plane_send.at[layer, j, k], plane_recv.at[layer, j, frm],
                         frm * 2 + core).wait_recv()
                total += g2[layer, j, frm].astype(F32)
            exp_out[layer * 6 + j] = total.astype(BF16)
            for k in range(1, n_chip):
                plane_copy(layer, j, k).wait_send()
            return carry
        lax.fori_loop(0, 6, body, 0)

    sub = piece // N_EP

    def da_copy(layer, k):
        to = (z + k) % N_EP
        return col_copy(d_send.at[layer, to], d_a.at[layer, z], da_send.at[layer, k], da_recv.at[layer, z], to)

    def db_copy(layer, k):
        to = (dp + k) % n_dp
        return row_copy(d_bs.at[layer, to], d_b.at[layer, dp], db_send.at[layer, k], db_recv.at[layer, dp], to)

    def dense_start(layer, grad):
        for q in range(N_EP):
            for p in range(n_dp):
                at = p * piece + q * sub
                d_send[layer, q, p] = grad[at:at + sub].astype(BF16)
        for k in range(1, N_EP):
            da_copy(layer, k).start()

    def dense_middle(layer):
        total = d_send[layer, z].astype(F32)
        for k in range(1, N_EP):
            frm = (z + k) % N_EP
            col_copy(d_send.at[layer, frm], d_a.at[layer, frm], da_send.at[layer, k], da_recv.at[layer, frm], frm).wait_recv()
            total += d_a[layer, frm].astype(F32)
        d_bs[layer] = total.astype(BF16)
        for k in range(1, n_dp):
            db_copy(layer, k).start()

    def dense_end(layer):
        total = d_bs[layer, dp].astype(F32)
        for k in range(1, n_dp):
            frm = (dp + k) % n_dp
            row_copy(d_bs.at[layer, frm], d_b.at[layer, frm], db_send.at[layer, k], db_recv.at[layer, frm], frm).wait_recv()
            total += d_b[layer, frm].astype(F32)
        tok_out[n_tok + layer * sub:n_tok + (layer + 1) * sub] = total.astype(BF16)
        for k in range(1, N_EP):
            da_copy(layer, k).wait_send()
        for k in range(1, n_dp):
            db_copy(layer, k).wait_send()

    def forward_step(k, carry):
        s = order(k)
        ag_step(0, k)
        with scope('f1'):
            forward(s)
        send_back(s)
        return carry
    lax.fori_loop(0, N_EP, forward_step, 0)
    gather_back()
    ag_pass(2, z)
    y = (ag[0, z].astype(F32) + acc[...]).astype(BF16)
    mid[...] = y
    ag[1, z] = (y.astype(F32) + nn(y, dense2[...])).astype(BF16)
    ag_pass(1, z)

    def second_step(k, carry):
        s = order(k)
        ag_step(2, k)
        ag_step(1, k)
        with scope('fb2'):
            backward(1, s, 2, 0, 1)
        back_start(0, s)
        return carry
    lax.fori_loop(0, N_EP, second_step, 0)
    with scope('wg1'):
        weight_grads(1)
    back_merge(0)
    gm = (dy_ref[...].astype(F32) + back_sum(0)).astype(BF16)
    gx = (gm.astype(F32) + nt(gm, dense2[...])).astype(BF16)
    g_mid[...] = gx
    ag[3, z] = gx
    ag_pass(3, z)
    dense_start(1, tn(mid[...], gm))

    def first_step(k, carry):
        s = order(k)
        ag_step(3, k)
        with scope('b1'):
            backward(0, s, 3, 1, None)
        back_start(1, s)
        return carry
    lax.fori_loop(0, N_EP, first_step, 0)
    with scope('wg0'):
        weight_grads(0)
    back_merge(1)
    with scope('dmid1'):
        dense_middle(1)
    gm1 = (g_mid[...].astype(F32) + back_sum(1)).astype(BF16)
    dense_start(0, tn(x_ref[...], gm1))
    tok_out[0:n_tok] = (gm1.astype(F32) + nt(gm1, dense1[...])).astype(BF16)
    with scope('plane1'):
        plane_sum(1)
    with scope('dend1'):
        dense_end(1)
    with scope('dmid0'):
        dense_middle(0)
    with scope('plane0'):
        plane_sum(0)
    with scope('dend0'):
        dense_end(0)
    for n in range(4):
        ag_drain(n)
    ret_drain()
    for n in range(2):
        back_drain(n)
    for k in range(1, N_EP):
        aux_copy(k).wait_send()


def solution(mesh):
    n_dp = mesh.shape['dp']
    n_chip = n_dp // 2
    tok_spec = P(('dp', 'ep'), None)
    exp_spec = P('ep', None, None)
    layer_specs = (P(None, None), tok_spec, tok_spec, exp_spec, exp_spec, exp_spec)
    grad_specs = (P(('dp', 'ep'), None), P('ep', 'dp', None), P('ep', 'dp', None), P('ep', None, 'dp'))

    def local_step(tokens, dy_out, dense_w1, idx1, gate1, wg1, wu1, wd1, dense_w2, idx2, gate2, wg2, wu2, wd2):
        n_tok, d_model = tokens.shape
        d_ff = wg1.shape[2]
        piece = d_model // n_dp
        sub = piece // N_EP
        vmem = pl.BlockSpec(memory_space=pltpu.VMEM)
        hbm = pl.BlockSpec(memory_space=pl.ANY)
        dma = pltpu.SemaphoreType.DMA
        outs = pl.pallas_call(
            functools.partial(kernel, n_dp),
            out_shape=(jax.ShapeDtypeStruct((n_tok + 2 * sub, d_model), BF16), jax.ShapeDtypeStruct((12, piece, d_ff), BF16)),
            in_specs=[vmem] * 8 + [hbm] * 6,
            out_specs=[vmem] * 2,
            scratch_shapes=[
                pltpu.VMEM((2, 2, d_model, d_ff), BF16), pltpu.VMEM((2, 2, d_model, d_ff), BF16), pltpu.VMEM((2, 2, d_ff, d_model), BF16),
                pltpu.VMEM((8, n_tok), F32), pltpu.VMEM((N_EP, 8, n_tok), F32), pltpu.VMEM((4 * N_EP, 1, n_tok), F32), pltpu.VMEM((4 * N_EP, 1, n_tok), F32),
                pltpu.VMEM((2, n_tok, N_EXP), F32), pltpu.VMEM((2, n_tok, N_EXP), F32), pltpu.VMEM((n_tok, n_tok), BF16),
                pltpu.VMEM((4, N_EP, n_tok, d_model), BF16), pltpu.VMEM((2, N_EP, 2, CAP, d_model), BF16),
                pltpu.VMEM((2, N_EP, n_tok, d_model), BF16), pltpu.VMEM((2, N_EP, n_tok, d_model), BF16),
                pltpu.VMEM((2, 2, N_EP, CAP, d_model), BF16), pltpu.VMEM((2, CAP, d_ff), F32), pltpu.VMEM((2, CAP, d_ff), F32),
                pltpu.VMEM((2, CAP, d_ff), BF16), pltpu.VMEM((2, N_EP, CAP, d_ff), BF16), pltpu.VMEM((2, N_EP, CAP, d_ff), BF16),
                pltpu.VMEM((2, N_EP, CAP, d_ff), BF16), pltpu.VMEM((2, N_EP, CAP, d_model), BF16),
                pltpu.VMEM((n_tok, d_model), F32), pltpu.VMEM((n_tok, d_model), BF16), pltpu.VMEM((n_tok, d_model), BF16),
                pltpu.VMEM((2, 6, n_chip, piece, d_ff), BF16), pltpu.VMEM((2, 6, n_chip, piece, d_ff), BF16),
                pltpu.VMEM((2, 6, n_chip, piece, d_ff), BF16),
                pltpu.VMEM((2, N_EP, n_dp, sub, d_model), BF16), pltpu.VMEM((2, N_EP, n_dp, sub, d_model), BF16),
                pltpu.VMEM((2, n_dp, sub, d_model), BF16), pltpu.VMEM((2, n_dp, sub, d_model), BF16),
                dma((6,)), dma((N_EP,)), dma((N_EP,)), dma((4, N_EP)), dma((4, N_EP)), dma((4, N_EP)), dma((N_EP,)), dma((N_EP,)),
                dma((2, N_EP)), dma((2, N_EP)), dma((2, 6)), dma((2, 6)), dma((2, 6, n_chip)), dma((2, 6, n_chip)),
                dma((2, N_EP)), dma((2, N_EP)), dma((2, n_dp)), dma((2, n_dp)),
            ],
            compiler_params=pltpu.CompilerParams(collective_id=0, has_side_effects=True, vmem_limit_bytes=67043328),
        )(tokens, dy_out, dense_w1, dense_w2, idx1.T, gate1.T, idx2.T, gate2.T, wg1, wu1, wd1, wg2, wu2, wd2)
        tok, exp = outs
        res = [tok[:n_tok]]
        for layer in range(2):
            at = layer * 6
            res += [tok[n_tok + layer * sub:n_tok + (layer + 1) * sub], exp[at:at + 2], exp[at + 2:at + 4], jnp.swapaxes(exp[at + 4:at + 6], 1, 2)]
        return tuple(res)

    return jax.shard_map(local_step, mesh=mesh, in_specs=(tok_spec, tok_spec) + layer_specs + layer_specs,
                         out_specs=(tok_spec,) + grad_specs + grad_specs, check_vma=False)
```

```python
import functools

import jax
import jax.numpy as jnp
from jax import lax
from jax.experimental import pallas as pl
from jax.experimental.pallas import tpu as pltpu
from jax.sharding import PartitionSpec as P

MESH = pl.DeviceIdType.MESH
F32, BF16 = jnp.float32, jnp.bfloat16
N_EP = 4
scope = jax.named_scope
N_EXP = 8
CAP = 256


def nn(a, b):
    return lax.dot_general(a, b, (((1,), (0,)), ((), ())), preferred_element_type=F32)


def nt(a, b):
    return lax.dot_general(a, b, (((1,), (1,)), ((), ())), preferred_element_type=F32)


def tn(a, b):
    return lax.dot_general(a, b, (((0,), (0,)), ((), ())), preferred_element_type=F32)


def kernel(n_dp, x_ref, dy_ref, dense1, dense2, idx1, gate1, idx2, gate2,
           wg1_hbm, wu1_hbm, wd1_hbm, wg2_hbm, wu2_hbm, wd2_hbm,
           tok_out, exp_out,
           w_gate, w_up, w_down, auxs, auxb, posr, gater, posc, gatec, tri, ag, ret, back_out, back_in, rows_in, t_a, t_b, t_gh, hid, g_a, g_b, g_out,
           acc, mid, g_mid, part, gs, gr, g2, d_send, d_a, d_bs, d_b, exp_v, dx_v, den_v,
           w_sem, aux_send, aux_recv, ag_right, ag_left, ag_recv, ret_send, ret_recv, back_send, back_recv, pair_send, pair_recv,
           plane_send, plane_recv, da_send, da_recv, db_send, db_recv, out_sem):
    z = lax.axis_index('ep')
    dp = lax.axis_index('dp')
    n_chip = n_dp // 2
    core = dp % 2
    chip = dp // 2
    n_tok, d_model = x_ref.shape
    d_ff = t_a.shape[2]
    piece = d_model // n_dp

    def order(k):
        near_low = jnp.where(z == 1, jnp.where(k == 0, 1, jnp.where(k == 1, 0, k)), k)
        near_high = 3 - jnp.where(z == 2, jnp.where(k == 0, 1, jnp.where(k == 1, 0, k)), k)
        return jnp.where(z < 2, near_low, near_high)

    barrier = pltpu.get_barrier_semaphore()
    for k in range(1, N_EP):
        pl.semaphore_signal(barrier, inc=1, device_id={'ep': (z + k) % N_EP, 'dp': dp}, device_id_type=MESH)
    for k in range(1, n_dp):
        pl.semaphore_signal(barrier, inc=1, device_id={'ep': z, 'dp': (dp + k) % n_dp}, device_id_type=MESH)

    w_copies = []
    for n, (hbm, dst) in enumerate(((wg1_hbm, w_gate.at[0]), (wu1_hbm, w_up.at[0]), (wd1_hbm, w_down.at[0]),
                                    (wg2_hbm, w_gate.at[1]), (wu2_hbm, w_up.at[1]), (wd2_hbm, w_down.at[1]))):
        w_copies.append(pltpu.make_async_copy(hbm, dst, w_sem.at[n]))
        w_copies[-1].start()

    auxs[0:2] = idx1[...].astype(F32)
    auxs[2:4] = gate1[...]
    auxs[4:6] = idx2[...].astype(F32)
    auxs[6:8] = gate2[...]
    x = x_ref[...]
    ag[0, z] = (x.astype(F32) + nn(x, dense1[...])).astype(BF16)
    ag[2, z] = dy_ref[...]
    auxb[z] = auxs[...]

    with scope('barrier'):
        pl.semaphore_wait(barrier, N_EP - 1 + n_dp - 1)

    def col_copy(src, dst, send, recv, to):
        return pltpu.make_async_remote_copy(src_ref=src, dst_ref=dst, send_sem=send, recv_sem=recv,
                                            device_id={'ep': to, 'dp': dp}, device_id_type=MESH)

    def row_copy(src, dst, send, recv, to):
        return pltpu.make_async_remote_copy(src_ref=src, dst_ref=dst, send_sem=send, recv_sem=recv,
                                            device_id={'ep': z, 'dp': to}, device_id_type=MESH)

    def aux_copy(k):
        return col_copy(auxs, auxb.at[z], aux_send.at[k], aux_recv.at[z], (z + k) % N_EP)

    for k in range(1, N_EP):
        aux_copy(k).start()

    def ag_to_right(n, s):
        return col_copy(ag.at[n, s], ag.at[n, s], ag_right.at[n, s], ag_recv.at[n, s], jnp.minimum(z + 1, N_EP - 1))

    def ag_to_left(n, s):
        return col_copy(ag.at[n, s], ag.at[n, s], ag_left.at[n, s], ag_recv.at[n, s], jnp.maximum(z - 1, 0))

    def ag_pass(n, s):
        @pl.when(jnp.logical_and(s <= z, z < N_EP - 1))
        def _():
            ag_to_right(n, s).start()

        @pl.when(jnp.logical_and(s >= z, z > 0))
        def _():
            ag_to_left(n, s).start()

    def ag_take(n, s):
        with scope('agw%d' % n):
            ag_to_right(n, s).wait_recv()
        ag_pass(n, s)

    def ag_step(n, k):
        inner = jnp.logical_or(z == 1, z == 2)
        outer = jnp.logical_not(inner)

        @pl.when(k == 1)
        def _():
            ag_take(n, order(1))

        @pl.when(jnp.logical_or(jnp.logical_and(k == 1, inner), jnp.logical_and(k == 2, outer)))
        def _():
            ag_take(n, order(2))

        @pl.when(k == 3)
        def _():
            ag_take(n, order(3))

    def ag_drain(n):
        def body(s, carry):
            @pl.when(jnp.logical_and(s <= z, z < N_EP - 1))
            def _():
                ag_to_right(n, s).wait_send()

            @pl.when(jnp.logical_and(s >= z, z > 0))
            def _():
                ag_to_left(n, s).wait_send()
            return carry
        lax.fori_loop(0, N_EP, body, 0)

    def ret_copy(s):
        return col_copy(ret.at[0, s], ret.at[1, z], ret_send.at[s], ret_recv.at[z], s)

    def ret_wait(s):
        col_copy(ret.at[0, s], ret.at[1, s], ret_send.at[s], ret_recv.at[s], s).wait_recv()

    def ret_drain():
        for k in range(1, N_EP):
            ret_copy((z + k) % N_EP).wait_send()

    ag_pass(0, z)

    r_io = lax.broadcasted_iota(jnp.int32, (n_tok, n_tok), 0)
    c_io = lax.broadcasted_iota(jnp.int32, (n_tok, n_tok), 1)
    tri[...] = (c_io < r_io).astype(F32).astype(BF16)
    lane = lax.broadcasted_iota(jnp.int32, (n_tok, N_EXP), 1)
    cols = auxs[...].T
    for layer in range(2):
        hit0 = cols[:, 4 * layer:4 * layer + 1] == lane.astype(F32)
        hit1 = cols[:, 4 * layer + 1:4 * layer + 2] == lane.astype(F32)
        hit = jnp.logical_or(hit0, hit1)
        rank = nn(tri[...], hit.astype(F32).astype(BF16))
        posc[layer] = jnp.where(hit, rank, -1.0)
        gatec[layer] = jnp.where(hit0, cols[:, 4 * layer + 2:4 * layer + 3], 0.0) + jnp.where(hit1, cols[:, 4 * layer + 3:4 * layer + 4], 0.0)
    for k in range(1, N_EP):
        s = (z + k) % N_EP
        col_copy(auxs, auxb.at[s], aux_send.at[k], aux_recv.at[s], s).wait_recv()
    hits = []
    for layer in range(2):
        for s in range(N_EP):
            for e in range(2):
                a = auxb[s]
                expert = (z * 2 + e).astype(F32)
                hit0 = a[4 * layer:4 * layer + 1] == expert
                hit1 = a[4 * layer + 1:4 * layer + 2] == expert
                hits.append(jnp.logical_or(hit0, hit1).astype(F32))
                gater[(layer * N_EP + s) * 2 + e] = (jnp.where(hit0, a[4 * layer + 2:4 * layer + 3], 0.0)
                                                     + jnp.where(hit1, a[4 * layer + 3:4 * layer + 4], 0.0))
    stack = jnp.concatenate(hits, axis=0)
    ranks = jnp.where(stack > 0.5, nt(stack.astype(BF16), tri[...]), -1.0)
    for n in range(4 * N_EP):
        posr[n] = ranks[n:n + 1]

    for copy in w_copies:
        copy.wait()

    slot = lax.broadcasted_iota(jnp.int32, (CAP, n_tok), 0).astype(F32)
    slot_lane = lax.broadcasted_iota(jnp.int32, (n_tok, CAP), 1).astype(F32)
    step = 32

    def select(layer, s):
        at = (layer * N_EP + s) * 2
        return [posr[at + e] == slot for e in range(2)]

    def as_bf16(picks):
        return jnp.concatenate([p.astype(F32).astype(BF16) for p in picks], axis=0)

    def take_rows(layer, s, n, pick):
        rows = nn(pick, ag[n, s]).astype(BF16)
        for e in range(2):
            rows_in[layer, e, s] = rows[e * CAP:(e + 1) * CAP]

    def up_project(layer, s, e):
        rows = rows_in[layer, e, s]
        t_a[e] = nn(rows, w_gate[layer, e])
        t_b[e] = nn(rows, w_up[layer, e])

    def forward(s):
        take_rows(0, s, 0, as_bf16(select(0, s)))
        for e in range(2):
            up_project(0, s, e)
        for e in range(2):
            for i in range(CAP // step):
                r = pl.ds(i * step, step)
                a = t_a[e, r, :]
                hid[e, s, r, :] = (a * jax.nn.sigmoid(a) * t_b[e, r, :]).astype(BF16)
            ret[jnp.where(s == z, 1, 0), s, e] = nn(hid[e, s], w_down[0, e]).astype(BF16)

    def backward(layer, s, n_dy, n_back, n_u):
        picks = select(layer, s)
        pick = as_bf16(picks)
        at = (layer * N_EP + s) * 2
        if n_u is not None:
            take_rows(layer, s, n_u, pick)
        got = nn(pick, ag[n_dy, s])
        for e in range(2):
            gate = jnp.sum(jnp.where(picks[e], gater[at + e], 0.0), axis=1, keepdims=True)
            g_out[e, s] = (got[e * CAP:(e + 1) * CAP] * gate).astype(BF16)
        for e in range(2):
            up_project(layer, s, e)
            t_gh[e] = nt(g_out[e, s], w_down[layer, e]).astype(BF16)
        parts = []
        for e in range(2):
            for i in range(CAP // step):
                r = pl.ds(i * step, step)
                a = t_a[e, r, :]
                b = t_b[e, r, :]
                gh = t_gh[e, r, :].astype(F32)
                sig = jax.nn.sigmoid(a)
                act = a * sig
                hid[e, s, r, :] = (act * b).astype(BF16)
                g_a[e, s, r, :] = (gh * b * sig * (1.0 + a * (1.0 - sig))).astype(BF16)
                g_b[e, s, r, :] = (gh * act).astype(BF16)
            parts.append((nt(g_a[e, s], w_gate[layer, e]) + nt(g_b[e, s], w_up[layer, e])).astype(BF16))
        back_out[n_back, s] = tn(pick, jnp.concatenate(parts, axis=0)).astype(BF16)

    def send_back(s):
        @pl.when(s != z)
        def _():
            ret_copy(s).start()

    def gather_back():
        acc[...] = jnp.zeros_like(acc)

        def body(k, carry):
            s = order(k)

            @pl.when(k > 0)
            def _():
                with scope('retw'):
                    ret_wait(s)

            for e in range(2):
                here = lane == s * 2 + e
                pos = jnp.sum(jnp.where(here, posc[0], 0.0), axis=1, keepdims=True)
                weight = jnp.sum(jnp.where(here, gatec[0], 0.0), axis=1, keepdims=True)
                acc[...] += nn((pos == slot_lane).astype(F32).astype(BF16), ret[1, s, e]) * weight
            return carry
        lax.fori_loop(0, N_EP, body, 0)

    inner = jnp.logical_or(z == 1, z == 2)
    outer = jnp.logical_not(inner)
    beside = jnp.where(z < 2, 1, 2)
    near_end = jnp.where(z < 2, 0, 3)

    def back_copy(n, s, slot_in, to):
        return col_copy(back_out.at[n, s], back_in.at[n, slot_in], back_send.at[n, s], back_recv.at[n, slot_in], to)

    def back_plan(s):
        dist = jnp.abs(z - s)
        slot_in = jnp.where(inner, 0, jnp.where(dist == 1, 2, jnp.where(dist == 2, 1, 3)))
        to = jnp.where(inner, 3 - z, jnp.where(dist == 2, beside, s))
        go = jnp.where(inner, dist == 2, dist > 0)
        return slot_in, to, go

    def back_start(n, s):
        slot_in, to, go = back_plan(s)

        @pl.when(go)
        def _():
            back_copy(n, s, slot_in, to).start()

    def back_wait(n, slot_in):
        with scope('bk%d%d' % (n, slot_in)):
            back_copy(n, 0, slot_in, z).wait_recv()

    def back_merge(n):
        @pl.when(inner)
        def _():
            for slot_in, s, slot_out in ((0, near_end, 2), (1, 3 - z, 3)):
                back_wait(n, slot_in)
                back_out[n, s] = (back_out[n, s].astype(F32) + back_in[n, slot_in].astype(F32)).astype(BF16)
                back_copy(n, s, slot_out, s).start()

    def back_sum(n):
        back_wait(n, 2)
        back_wait(n, 3)
        return back_out[n, z].astype(F32) + back_in[n, 2].astype(F32) + back_in[n, 3].astype(F32)

    def back_drain(n):
        for k in range(1, N_EP):
            back_copy(n, (z + k) % N_EP, 0, z).wait_send()

    flip_x = chip + 1 - 2 * (chip % 2)
    flip_y = (chip + 2) % n_chip
    first = jnp.where(core == 0, flip_x, flip_y)
    second = jnp.where(core == 0, flip_y, flip_x)
    across = n_chip - 1 - chip

    def pair_copy(layer, j):
        return row_copy(gs.at[1 - core, j], gr.at[layer, j], pair_send.at[layer, j], pair_recv.at[layer, j], chip * 2 + 1 - core)

    def one_copy(layer, j, k):
        piece_of = (first, across)[k]
        return row_copy(gr.at[layer, j, piece_of], g2.at[layer, j, k], plane_send.at[layer, j, k], plane_recv.at[layer, j, k], first * 2 + core)

    def two_copy(layer, j):
        return row_copy(gr.at[layer, j, second], g2.at[layer, j, 2], plane_send.at[layer, j, 2], plane_recv.at[layer, j, 2], second * 2 + core)

    def pair_finish(layer, j):
        pair_copy(layer, j).wait()
        for c in range(n_chip):
            gr[layer, j, c] = (gr[layer, j, c].astype(F32) + gs[core, j, c].astype(F32)).astype(BF16)
        for k in (1, 0):
            one_copy(layer, j, k).start()

    def one_finish(layer):
        def body(j, carry):
            for k, mine in ((1, second), (0, chip)):
                one_copy(layer, j, k).wait_recv()
                gr[layer, j, mine] = (gr[layer, j, mine].astype(F32) + g2[layer, j, k].astype(F32)).astype(BF16)
                if k == 1:
                    two_copy(layer, j).start()
            return carry
        lax.fori_loop(0, 6, body, 0)

    def two_finish(layer):
        def body(j, carry):
            two_copy(layer, j).wait_recv()
            exp_v[layer, j] = (gr[layer, j, chip].astype(F32) + g2[layer, j, 2].astype(F32)).astype(BF16)
            for k in range(2):
                one_copy(layer, j, k).wait_send()
            two_copy(layer, j).wait_send()
            return carry
        lax.fori_loop(0, 6, body, 0)
        exp_copy(layer).start()

    def exp_copy(layer):
        return pltpu.make_async_copy(exp_v.at[layer], exp_out.at[layer], out_sem.at[layer])

    def operands(layer, e, at, n):
        rows = rows_in[layer, e, pl.ds(at, n)].reshape(n * CAP, d_model)
        outs = g_out[e, pl.ds(at, n)].reshape(n * CAP, d_model)
        for q, (left, right) in enumerate(((outs, hid), (rows, g_a), (rows, g_b))):
            yield q, (q + 2) % 3 * 2 + e, left, right[e, pl.ds(at, n)].reshape(n * CAP, d_ff)

    def weight_part(layer, at, n):
        def body(e, carry):
            for q, j, left, right in operands(layer, e, at, n):
                part[e, q] = tn(left, right)
            return carry
        lax.fori_loop(0, 2, body, 0)

    def weight_grads(layer, at, n, add):
        def body(e, carry):
            for q, j, left, right in operands(layer, e, at, n):
                grad = tn(left, right)
                if add:
                    grad = grad + part[e, q]
                for p in range(n_dp):
                    gs[p % 2, j, p // 2] = grad[p * piece:(p + 1) * piece].astype(BF16)
                pair_copy(layer, j).start()

                @pl.when(e > 0)
                def _():
                    pair_finish(layer, j - 1)
            return carry
        lax.fori_loop(0, 2, body, 0)
        for q in range(3):
            pair_finish(layer, (q + 2) % 3 * 2 + 1)

    sub = piece // N_EP

    def da_copy(layer, k):
        to = (z + k) % N_EP
        return col_copy(d_send.at[layer, to], d_a.at[layer, z], da_send.at[layer, k], da_recv.at[layer, z], to)

    def db_copy(layer, k):
        to = (dp + k) % n_dp
        return row_copy(d_bs.at[layer, to], d_b.at[layer, dp], db_send.at[layer, k], db_recv.at[layer, dp], to)

    def dense_start(layer, grad):
        for q in range(N_EP):
            for p in range(n_dp):
                at = p * piece + q * sub
                d_send[layer, q, p] = grad[at:at + sub].astype(BF16)
        for k in range(1, N_EP):
            da_copy(layer, k).start()

    def dense_middle(layer):
        total = d_send[layer, z].astype(F32)
        for k in range(1, N_EP):
            frm = (z + k) % N_EP
            col_copy(d_send.at[layer, frm], d_a.at[layer, frm], da_send.at[layer, k], da_recv.at[layer, frm], frm).wait_recv()
            total += d_a[layer, frm].astype(F32)
        d_bs[layer] = total.astype(BF16)
        for k in range(1, n_dp):
            db_copy(layer, k).start()

    def dense_end(layer):
        total = d_bs[layer, dp].astype(F32)
        for k in range(1, n_dp):
            frm = (dp + k) % n_dp
            row_copy(d_bs.at[layer, frm], d_b.at[layer, frm], db_send.at[layer, k], db_recv.at[layer, frm], frm).wait_recv()
            total += d_b[layer, frm].astype(F32)
        den_v[layer * sub:(layer + 1) * sub] = total.astype(BF16)
        for k in range(1, N_EP):
            da_copy(layer, k).wait_send()
        for k in range(1, n_dp):
            db_copy(layer, k).wait_send()

    def forward_step(k, carry):
        s = order(k)
        ag_step(0, k)
        with scope('f1'):
            forward(s)
        send_back(s)
        return carry
    lax.fori_loop(0, N_EP, forward_step, 0)
    gather_back()
    ag_pass(2, z)
    y = (ag[0, z].astype(F32) + acc[...]).astype(BF16)
    mid[...] = y
    ag[1, z] = (y.astype(F32) + nn(y, dense2[...])).astype(BF16)
    ag_pass(1, z)

    def second_step(k, carry):
        s = order(k)
        ag_step(2, k)
        ag_step(1, k)
        with scope('fb2'):
            backward(1, s, 2, 0, 1)
        back_start(0, s)
        return carry
    lax.fori_loop(0, N_EP, second_step, 0)
    with scope('wg1'):
        weight_grads(1, 0, N_EP, False)
    back_merge(0)
    gm = (dy_ref[...].astype(F32) + back_sum(0)).astype(BF16)
    gx = (gm.astype(F32) + nt(gm, dense2[...])).astype(BF16)
    g_mid[...] = gx
    ag[3, z] = gx
    ag_pass(3, z)
    dense_start(1, tn(mid[...], gm))
    with scope('one1'):
        one_finish(1)

    three = jnp.where(z < 2, 0, 1)
    last = jnp.where(z < 2, 3, 0)

    def first_step(k, carry):
        s = order(k)

        @pl.when(k == 2)
        def _():
            with scope('dmid1'):
                dense_middle(1)
            with scope('two1'):
                two_finish(1)

        @pl.when(jnp.logical_and(k == 3, outer))
        def _():
            with scope('wpart'):
                weight_part(0, three, 3)
        ag_step(3, k)
        with scope('b1'):
            backward(0, s, 3, 1, None)
        back_start(1, s)
        return carry
    lax.fori_loop(0, N_EP, first_step, 0)

    @pl.when(inner)
    def _():
        weight_part(0, three, 3)
    with scope('wg0'):
        weight_grads(0, last, 1, True)
    back_merge(1)
    with scope('dend1'):
        dense_end(1)
    with scope('one0'):
        one_finish(0)
    gm1 = (g_mid[...].astype(F32) + back_sum(1)).astype(BF16)
    dense_start(0, tn(x_ref[...], gm1))
    dx_v[...] = (gm1.astype(F32) + nt(gm1, dense1[...])).astype(BF16)
    dx_copy = pltpu.make_async_copy(dx_v, tok_out.at[pl.ds(0, n_tok)], out_sem.at[2])
    dx_copy.start()
    with scope('dmid0'):
        dense_middle(0)
    with scope('two0'):
        two_finish(0)
    with scope('dend0'):
        dense_end(0)
    den_copy = pltpu.make_async_copy(den_v, tok_out.at[pl.ds(n_tok, 2 * sub)], out_sem.at[3])
    den_copy.start()
    for n in range(4):
        ag_drain(n)
    ret_drain()
    for n in range(2):
        back_drain(n)
    for k in range(1, N_EP):
        aux_copy(k).wait_send()
    exp_copy(1).wait()
    exp_copy(0).wait()
    dx_copy.wait()
    den_copy.wait()


def solution(mesh):
    n_dp = mesh.shape['dp']
    n_chip = n_dp // 2
    tok_spec = P(('dp', 'ep'), None)
    exp_spec = P('ep', None, None)
    layer_specs = (P(None, None), tok_spec, tok_spec, exp_spec, exp_spec, exp_spec)
    grad_specs = (P(('dp', 'ep'), None), P('ep', 'dp', None), P('ep', 'dp', None), P('ep', None, 'dp'))

    def local_step(tokens, dy_out, dense_w1, idx1, gate1, wg1, wu1, wd1, dense_w2, idx2, gate2, wg2, wu2, wd2):
        n_tok, d_model = tokens.shape
        d_ff = wg1.shape[2]
        piece = d_model // n_dp
        sub = piece // N_EP
        vmem = pl.BlockSpec(memory_space=pltpu.VMEM)
        hbm = pl.BlockSpec(memory_space=pl.ANY)
        dma = pltpu.SemaphoreType.DMA
        outs = pl.pallas_call(
            functools.partial(kernel, n_dp),
            out_shape=(jax.ShapeDtypeStruct((n_tok + 2 * sub, d_model), BF16), jax.ShapeDtypeStruct((2, 6, piece, d_ff), BF16)),
            in_specs=[vmem] * 8 + [hbm] * 6,
            out_specs=[hbm] * 2,
            scratch_shapes=[
                pltpu.VMEM((2, 2, d_model, d_ff), BF16), pltpu.VMEM((2, 2, d_model, d_ff), BF16), pltpu.VMEM((2, 2, d_ff, d_model), BF16),
                pltpu.VMEM((8, n_tok), F32), pltpu.VMEM((N_EP, 8, n_tok), F32), pltpu.VMEM((4 * N_EP, 1, n_tok), F32), pltpu.VMEM((4 * N_EP, 1, n_tok), F32),
                pltpu.VMEM((2, n_tok, N_EXP), F32), pltpu.VMEM((2, n_tok, N_EXP), F32), pltpu.VMEM((n_tok, n_tok), BF16),
                pltpu.VMEM((4, N_EP, n_tok, d_model), BF16), pltpu.VMEM((2, N_EP, 2, CAP, d_model), BF16),
                pltpu.VMEM((2, N_EP, n_tok, d_model), BF16), pltpu.VMEM((2, N_EP, n_tok, d_model), BF16),
                pltpu.VMEM((2, 2, N_EP, CAP, d_model), BF16), pltpu.VMEM((2, CAP, d_ff), F32), pltpu.VMEM((2, CAP, d_ff), F32),
                pltpu.VMEM((2, CAP, d_ff), BF16), pltpu.VMEM((2, N_EP, CAP, d_ff), BF16), pltpu.VMEM((2, N_EP, CAP, d_ff), BF16),
                pltpu.VMEM((2, N_EP, CAP, d_ff), BF16), pltpu.VMEM((2, N_EP, CAP, d_model), BF16),
                pltpu.VMEM((n_tok, d_model), F32), pltpu.VMEM((n_tok, d_model), BF16), pltpu.VMEM((n_tok, d_model), BF16),
                pltpu.VMEM((2, 3, d_model, d_ff), F32),
                pltpu.VMEM((2, 6, n_chip, piece, d_ff), BF16), pltpu.VMEM((2, 6, n_chip, piece, d_ff), BF16),
                pltpu.VMEM((2, 6, 3, piece, d_ff), BF16),
                pltpu.VMEM((2, N_EP, n_dp, sub, d_model), BF16), pltpu.VMEM((2, N_EP, n_dp, sub, d_model), BF16),
                pltpu.VMEM((2, n_dp, sub, d_model), BF16), pltpu.VMEM((2, n_dp, sub, d_model), BF16),
                pltpu.VMEM((2, 6, piece, d_ff), BF16), pltpu.VMEM((n_tok, d_model), BF16), pltpu.VMEM((2 * sub, d_model), BF16),
                dma((6,)), dma((N_EP,)), dma((N_EP,)), dma((4, N_EP)), dma((4, N_EP)), dma((4, N_EP)), dma((N_EP,)), dma((N_EP,)),
                dma((2, N_EP)), dma((2, N_EP)), dma((2, 6)), dma((2, 6)), dma((2, 6, 3)), dma((2, 6, 3)),
                dma((2, N_EP)), dma((2, N_EP)), dma((2, n_dp)), dma((2, n_dp)), dma((4,)),
            ],
            compiler_params=pltpu.CompilerParams(collective_id=0, has_side_effects=True, vmem_limit_bytes=67043328),
        )(tokens, dy_out, dense_w1, dense_w2, idx1.T, gate1.T, idx2.T, gate2.T, wg1, wu1, wd1, wg2, wu2, wd2)
        tok, exp = outs
        res = [tok[:n_tok]]
        for layer in range(2):
            res += [tok[n_tok + layer * sub:n_tok + (layer + 1) * sub], exp[layer, 0:2], exp[layer, 2:4], jnp.swapaxes(exp[layer, 4:6], 1, 2)]
        return tuple(res)

    return jax.shard_map(local_step, mesh=mesh, in_specs=(tok_spec, tok_spec) + layer_specs + layer_specs,
                         out_specs=(tok_spec,) + grad_specs + grad_specs, check_vma=False)
```

```python
import functools

import jax
import jax.numpy as jnp
from jax import lax
from jax.experimental import pallas as pl
from jax.experimental.pallas import tpu as pltpu
from jax.sharding import PartitionSpec as P

MESH = pl.DeviceIdType.MESH
F32, BF16 = jnp.float32, jnp.bfloat16
N_EP = 4
scope = jax.named_scope
N_EXP = 8
CAP = 256


def nn(a, b):
    return lax.dot_general(a, b, (((1,), (0,)), ((), ())), preferred_element_type=F32)


def nt(a, b):
    return lax.dot_general(a, b, (((1,), (1,)), ((), ())), preferred_element_type=F32)


def tn(a, b):
    return lax.dot_general(a, b, (((0,), (0,)), ((), ())), preferred_element_type=F32)


def kernel(n_dp, x_ref, dy_ref, dense1, dense2, idx1, gate1, idx2, gate2,
           wg1_hbm, wu1_hbm, wd1_hbm, wg2_hbm, wu2_hbm, wd2_hbm,
           tok_out, exp_out,
           w_gate, w_up, w_down, auxs, auxb, posr, gater, posc, gatec, tri, ag, ret, back_out, back_in, rows_in, t_a, t_b, t_gh, hid, g_a, g_b, g_out,
           acc, mid, g_mid, part, gs, gr, g2, g3, d_send, d_a, d_bs, d_b, exp_v, dx_v, den_v,
           w_sem, aux_send, aux_recv, ag_right, ag_left, ag_recv, ret_send, ret_recv, back_send, back_recv, pair_send, pair_recv,
           one_send, one_recv, two_send, two_recv, da_send, da_recv, db_send, db_recv, out_sem):
    z = lax.axis_index('ep')
    dp = lax.axis_index('dp')
    n_chip = n_dp // 2
    core = dp % 2
    chip = dp // 2
    n_tok, d_model = x_ref.shape
    d_ff = t_a.shape[2]
    piece = d_model // n_dp

    def order(k):
        near_low = jnp.where(z == 1, jnp.where(k == 0, 1, jnp.where(k == 1, 0, k)), k)
        near_high = 3 - jnp.where(z == 2, jnp.where(k == 0, 1, jnp.where(k == 1, 0, k)), k)
        return jnp.where(z < 2, near_low, near_high)

    barrier = pltpu.get_barrier_semaphore()
    for k in range(1, N_EP):
        pl.semaphore_signal(barrier, inc=1, device_id={'ep': (z + k) % N_EP, 'dp': dp}, device_id_type=MESH)
    for k in range(1, n_dp):
        pl.semaphore_signal(barrier, inc=1, device_id={'ep': z, 'dp': (dp + k) % n_dp}, device_id_type=MESH)

    w_copies = []
    for n, (hbm, dst) in enumerate(((wg1_hbm, w_gate.at[0]), (wu1_hbm, w_up.at[0]), (wd1_hbm, w_down.at[0]),
                                    (wg2_hbm, w_gate.at[1]), (wu2_hbm, w_up.at[1]), (wd2_hbm, w_down.at[1]))):
        w_copies.append(pltpu.make_async_copy(hbm, dst, w_sem.at[n]))
        w_copies[-1].start()

    auxs[0:2] = idx1[...].astype(F32)
    auxs[2:4] = gate1[...]
    auxs[4:6] = idx2[...].astype(F32)
    auxs[6:8] = gate2[...]
    x = x_ref[...]
    ag[0, z] = (x.astype(F32) + nn(x, dense1[...])).astype(BF16)
    ag[2, z] = dy_ref[...]
    auxb[z] = auxs[...]

    with scope('barrier'):
        pl.semaphore_wait(barrier, N_EP - 1 + n_dp - 1)

    def col_copy(src, dst, send, recv, to):
        return pltpu.make_async_remote_copy(src_ref=src, dst_ref=dst, send_sem=send, recv_sem=recv,
                                            device_id={'ep': to, 'dp': dp}, device_id_type=MESH)

    def row_copy(src, dst, send, recv, to):
        return pltpu.make_async_remote_copy(src_ref=src, dst_ref=dst, send_sem=send, recv_sem=recv,
                                            device_id={'ep': z, 'dp': to}, device_id_type=MESH)

    def aux_copy(k):
        return col_copy(auxs, auxb.at[z], aux_send.at[k], aux_recv.at[z], (z + k) % N_EP)

    for k in range(1, N_EP):
        aux_copy(k).start()

    def ag_to_right(n, s):
        return col_copy(ag.at[n, s], ag.at[n, s], ag_right.at[n, s], ag_recv.at[n, s], jnp.minimum(z + 1, N_EP - 1))

    def ag_to_left(n, s):
        return col_copy(ag.at[n, s], ag.at[n, s], ag_left.at[n, s], ag_recv.at[n, s], jnp.maximum(z - 1, 0))

    def ag_pass(n, s):
        @pl.when(jnp.logical_and(s <= z, z < N_EP - 1))
        def _():
            ag_to_right(n, s).start()

        @pl.when(jnp.logical_and(s >= z, z > 0))
        def _():
            ag_to_left(n, s).start()

    def ag_take(n, s):
        with scope('agw%d' % n):
            ag_to_right(n, s).wait_recv()
        ag_pass(n, s)

    def ag_step(n, k):
        inner = jnp.logical_or(z == 1, z == 2)
        outer = jnp.logical_not(inner)

        @pl.when(k == 1)
        def _():
            ag_take(n, order(1))

        @pl.when(jnp.logical_or(jnp.logical_and(k == 1, inner), jnp.logical_and(k == 2, outer)))
        def _():
            ag_take(n, order(2))

        @pl.when(k == 3)
        def _():
            ag_take(n, order(3))

    def ag_drain(n):
        def body(s, carry):
            @pl.when(jnp.logical_and(s <= z, z < N_EP - 1))
            def _():
                ag_to_right(n, s).wait_send()

            @pl.when(jnp.logical_and(s >= z, z > 0))
            def _():
                ag_to_left(n, s).wait_send()
            return carry
        lax.fori_loop(0, N_EP, body, 0)

    def ret_copy(s):
        return col_copy(ret.at[0, s], ret.at[1, z], ret_send.at[s], ret_recv.at[z], s)

    def ret_wait(s):
        col_copy(ret.at[0, s], ret.at[1, s], ret_send.at[s], ret_recv.at[s], s).wait_recv()

    def ret_drain():
        for k in range(1, N_EP):
            ret_copy((z + k) % N_EP).wait_send()

    ag_pass(0, z)

    r_io = lax.broadcasted_iota(jnp.int32, (n_tok, n_tok), 0)
    c_io = lax.broadcasted_iota(jnp.int32, (n_tok, n_tok), 1)
    tri[...] = (c_io < r_io).astype(F32).astype(BF16)
    lane = lax.broadcasted_iota(jnp.int32, (n_tok, N_EXP), 1)
    cols = auxs[...].T
    for layer in range(2):
        hit0 = cols[:, 4 * layer:4 * layer + 1] == lane.astype(F32)
        hit1 = cols[:, 4 * layer + 1:4 * layer + 2] == lane.astype(F32)
        hit = jnp.logical_or(hit0, hit1)
        rank = nn(tri[...], hit.astype(F32).astype(BF16))
        posc[layer] = jnp.where(hit, rank, -1.0)
        gatec[layer] = jnp.where(hit0, cols[:, 4 * layer + 2:4 * layer + 3], 0.0) + jnp.where(hit1, cols[:, 4 * layer + 3:4 * layer + 4], 0.0)
    for k in range(1, N_EP):
        s = (z + k) % N_EP
        col_copy(auxs, auxb.at[s], aux_send.at[k], aux_recv.at[s], s).wait_recv()
    hits = []
    for layer in range(2):
        for s in range(N_EP):
            for e in range(2):
                a = auxb[s]
                expert = (z * 2 + e).astype(F32)
                hit0 = a[4 * layer:4 * layer + 1] == expert
                hit1 = a[4 * layer + 1:4 * layer + 2] == expert
                hits.append(jnp.logical_or(hit0, hit1).astype(F32))
                gater[(layer * N_EP + s) * 2 + e] = (jnp.where(hit0, a[4 * layer + 2:4 * layer + 3], 0.0)
                                                     + jnp.where(hit1, a[4 * layer + 3:4 * layer + 4], 0.0))
    stack = jnp.concatenate(hits, axis=0)
    ranks = jnp.where(stack > 0.5, nt(stack.astype(BF16), tri[...]), -1.0)
    for n in range(4 * N_EP):
        posr[n] = ranks[n:n + 1]

    for copy in w_copies:
        copy.wait()

    slot = lax.broadcasted_iota(jnp.int32, (CAP, n_tok), 0).astype(F32)
    slot_lane = lax.broadcasted_iota(jnp.int32, (n_tok, CAP), 1).astype(F32)
    step = 32

    def select(layer, s):
        at = (layer * N_EP + s) * 2
        return [posr[at + e] == slot for e in range(2)]

    def as_bf16(picks):
        return jnp.concatenate([p.astype(F32).astype(BF16) for p in picks], axis=0)

    def take_rows(layer, s, n, pick):
        rows = nn(pick, ag[n, s]).astype(BF16)
        for e in range(2):
            rows_in[layer, e, s] = rows[e * CAP:(e + 1) * CAP]

    def up_project(layer, s, e):
        rows = rows_in[layer, e, s]
        t_a[e] = nn(rows, w_gate[layer, e])
        t_b[e] = nn(rows, w_up[layer, e])

    def forward(s):
        take_rows(0, s, 0, as_bf16(select(0, s)))
        for e in range(2):
            up_project(0, s, e)
        for e in range(2):
            for i in range(CAP // step):
                r = pl.ds(i * step, step)
                a = t_a[e, r, :]
                hid[e, s, r, :] = (a * jax.nn.sigmoid(a) * t_b[e, r, :]).astype(BF16)
            ret[jnp.where(s == z, 1, 0), s, e] = nn(hid[e, s], w_down[0, e]).astype(BF16)

    def backward(layer, s, n_dy, n_back, n_u):
        picks = select(layer, s)
        pick = as_bf16(picks)
        at = (layer * N_EP + s) * 2
        if n_u is not None:
            take_rows(layer, s, n_u, pick)
        got = nn(pick, ag[n_dy, s])
        for e in range(2):
            gate = jnp.sum(jnp.where(picks[e], gater[at + e], 0.0), axis=1, keepdims=True)
            g_out[e, s] = (got[e * CAP:(e + 1) * CAP] * gate).astype(BF16)
        for e in range(2):
            up_project(layer, s, e)
            t_gh[e] = nt(g_out[e, s], w_down[layer, e]).astype(BF16)
        parts = []
        for e in range(2):
            for i in range(CAP // step):
                r = pl.ds(i * step, step)
                a = t_a[e, r, :]
                b = t_b[e, r, :]
                gh = t_gh[e, r, :].astype(F32)
                sig = jax.nn.sigmoid(a)
                act = a * sig
                hid[e, s, r, :] = (act * b).astype(BF16)
                g_a[e, s, r, :] = (gh * b * sig * (1.0 + a * (1.0 - sig))).astype(BF16)
                g_b[e, s, r, :] = (gh * act).astype(BF16)
            parts.append((nt(g_a[e, s], w_gate[layer, e]) + nt(g_b[e, s], w_up[layer, e])).astype(BF16))
        back_out[n_back, s] = tn(pick, jnp.concatenate(parts, axis=0)).astype(BF16)

    def send_back(s):
        @pl.when(s != z)
        def _():
            ret_copy(s).start()

    def gather_back():
        acc[...] = jnp.zeros_like(acc)

        def body(k, carry):
            s = order(k)

            @pl.when(k > 0)
            def _():
                with scope('retw'):
                    ret_wait(s)

            for e in range(2):
                here = lane == s * 2 + e
                pos = jnp.sum(jnp.where(here, posc[0], 0.0), axis=1, keepdims=True)
                weight = jnp.sum(jnp.where(here, gatec[0], 0.0), axis=1, keepdims=True)
                acc[...] += nn((pos == slot_lane).astype(F32).astype(BF16), ret[1, s, e]) * weight
            return carry
        lax.fori_loop(0, N_EP, body, 0)

    inner = jnp.logical_or(z == 1, z == 2)
    outer = jnp.logical_not(inner)
    beside = jnp.where(z < 2, 1, 2)
    near_end = jnp.where(z < 2, 0, 3)

    def back_copy(n, s, slot_in, to):
        return col_copy(back_out.at[n, s], back_in.at[n, slot_in], back_send.at[n, s], back_recv.at[n, slot_in], to)

    def back_plan(s):
        dist = jnp.abs(z - s)
        slot_in = jnp.where(inner, 0, jnp.where(dist == 1, 2, jnp.where(dist == 2, 1, 3)))
        to = jnp.where(inner, 3 - z, jnp.where(dist == 2, beside, s))
        go = jnp.where(inner, dist == 2, dist > 0)
        return slot_in, to, go

    def back_start(n, s):
        slot_in, to, go = back_plan(s)

        @pl.when(go)
        def _():
            back_copy(n, s, slot_in, to).start()

    def back_wait(n, slot_in):
        with scope('bk%d%d' % (n, slot_in)):
            back_copy(n, 0, slot_in, z).wait_recv()

    def back_merge(n):
        @pl.when(inner)
        def _():
            for slot_in, s, slot_out in ((0, near_end, 2), (1, 3 - z, 3)):
                back_wait(n, slot_in)
                back_out[n, s] = (back_out[n, s].astype(F32) + back_in[n, slot_in].astype(F32)).astype(BF16)
                back_copy(n, s, slot_out, s).start()

    def back_sum(n):
        back_wait(n, 2)
        back_wait(n, 3)
        return back_out[n, z].astype(F32) + back_in[n, 2].astype(F32) + back_in[n, 3].astype(F32)

    def back_drain(n):
        for k in range(1, N_EP):
            back_copy(n, (z + k) % N_EP, 0, z).wait_send()

    chip_x = chip % 2
    chip_y = chip // 2
    group = jnp.where(core == 0, chip_x, chip_y)
    place = jnp.where(core == 0, chip_y, chip_x)
    first = jnp.where(core == 0, chip + 1 - 2 * chip_x, (chip + 2) % n_chip)
    second = jnp.where(core == 0, (chip + 2) % n_chip, chip + 1 - 2 * chip_x)

    def pair_copy(layer, e):
        return row_copy(gs.at[1 - core, e], gr.at[layer, e], pair_send.at[layer, e], pair_recv.at[layer, e], chip * 2 + 1 - core)

    def one_copy(layer, e):
        return row_copy(gr.at[layer, e, 1 - group], g2.at[layer, e], one_send.at[layer, e], one_recv.at[layer, e], first * 2 + core)

    def two_copy(layer, e):
        return row_copy(gr.at[layer, e, group, 1 - place], g3.at[layer, e], two_send.at[layer, e], two_recv.at[layer, e], second * 2 + core)

    def pair_finish(layer, e):
        pair_copy(layer, e).wait()

        def body(q, carry):
            for g in range(2):
                for p in range(2):
                    gr[layer, e, g, p, q] = (gr[layer, e, g, p, q].astype(F32) + gs[core, e, g, p, q].astype(F32)).astype(BF16)
            return carry
        lax.fori_loop(0, 3, body, 0)
        one_copy(layer, e).start()

    def one_finish(layer):
        def body(e, carry):
            one_copy(layer, e).wait_recv()
            for p in range(2):
                for q in range(3):
                    gr[layer, e, group, p, q] = (gr[layer, e, group, p, q].astype(F32) + g2[layer, e, p, q].astype(F32)).astype(BF16)
            two_copy(layer, e).start()
            return carry
        lax.fori_loop(0, 2, body, 0)

    def two_finish(layer):
        def body(e, carry):
            two_copy(layer, e).wait_recv()
            for q in range(3):
                exp_v[layer, q * 2 + e] = (gr[layer, e, group, place, q].astype(F32) + g3[layer, e, q].astype(F32)).astype(BF16)
            one_copy(layer, e).wait_send()
            two_copy(layer, e).wait_send()
            return carry
        lax.fori_loop(0, 2, body, 0)
        exp_copy(layer).start()

    def exp_copy(layer):
        return pltpu.make_async_copy(exp_v.at[layer], exp_out.at[layer], out_sem.at[layer])

    def operands(layer, e, at, n):
        rows = rows_in[layer, e, pl.ds(at, n)].reshape(n * CAP, d_model)
        outs = g_out[e, pl.ds(at, n)].reshape(n * CAP, d_model)
        for q, (left, right) in enumerate(((outs, hid), (rows, g_a), (rows, g_b))):
            yield q, (q + 2) % 3, left, right[e, pl.ds(at, n)].reshape(n * CAP, d_ff)

    def weight_part(layer, at, n):
        def body(e, carry):
            for q, j, left, right in operands(layer, e, at, n):
                part[e, q] = tn(left, right)
            return carry
        lax.fori_loop(0, 2, body, 0)

    def weight_grads(layer, at, n, add):
        def body(e, carry):
            for q, j, left, right in operands(layer, e, at, n):
                grad = tn(left, right)
                if add:
                    grad = grad + part[e, q]
                for p in range(n_dp):
                    y, x = p // 4, p // 2 % 2
                    g = (x, y) if p % 2 == 0 else (y, x)
                    gs[p % 2, e, g[0], g[1], j] = grad[p * piece:(p + 1) * piece].astype(BF16)
            pair_copy(layer, e).start()
            return carry
        lax.fori_loop(0, 2, body, 0)
        pair_finish(layer, 0)
        pair_finish(layer, 1)

    sub = piece // N_EP

    def da_copy(layer, k):
        to = (z + k) % N_EP
        return col_copy(d_send.at[layer, to], d_a.at[layer, z], da_send.at[layer, k], da_recv.at[layer, z], to)

    def db_copy(layer, k):
        to = (dp + k) % n_dp
        return row_copy(d_bs.at[layer, to], d_b.at[layer, dp], db_send.at[layer, k], db_recv.at[layer, dp], to)

    def dense_start(layer, grad):
        for q in range(N_EP):
            for p in range(n_dp):
                at = p * piece + q * sub
                d_send[layer, q, p] = grad[at:at + sub].astype(BF16)
        for k in range(1, N_EP):
            da_copy(layer, k).start()

    def dense_middle(layer):
        total = d_send[layer, z].astype(F32)
        for k in range(1, N_EP):
            frm = (z + k) % N_EP
            col_copy(d_send.at[layer, frm], d_a.at[layer, frm], da_send.at[layer, k], da_recv.at[layer, frm], frm).wait_recv()
            total += d_a[layer, frm].astype(F32)
        d_bs[layer] = total.astype(BF16)
        for k in range(1, n_dp):
            db_copy(layer, k).start()

    def dense_end(layer):
        total = d_bs[layer, dp].astype(F32)
        for k in range(1, n_dp):
            frm = (dp + k) % n_dp
            row_copy(d_bs.at[layer, frm], d_b.at[layer, frm], db_send.at[layer, k], db_recv.at[layer, frm], frm).wait_recv()
            total += d_b[layer, frm].astype(F32)
        den_v[layer * sub:(layer + 1) * sub] = total.astype(BF16)
        for k in range(1, N_EP):
            da_copy(layer, k).wait_send()
        for k in range(1, n_dp):
            db_copy(layer, k).wait_send()

    def forward_step(k, carry):
        s = order(k)
        ag_step(0, k)
        with scope('f1'):
            forward(s)
        send_back(s)
        return carry
    lax.fori_loop(0, N_EP, forward_step, 0)
    gather_back()
    ag_pass(2, z)
    y = (ag[0, z].astype(F32) + acc[...]).astype(BF16)
    mid[...] = y
    ag[1, z] = (y.astype(F32) + nn(y, dense2[...])).astype(BF16)
    ag_pass(1, z)

    def second_step(k, carry):
        s = order(k)
        ag_step(2, k)
        ag_step(1, k)
        with scope('fb2'):
            backward(1, s, 2, 0, 1)
        back_start(0, s)
        return carry
    lax.fori_loop(0, N_EP, second_step, 0)
    with scope('wg1'):
        weight_grads(1, 0, N_EP, False)
    back_merge(0)
    gm = (dy_ref[...].astype(F32) + back_sum(0)).astype(BF16)
    gx = (gm.astype(F32) + nt(gm, dense2[...])).astype(BF16)
    g_mid[...] = gx
    ag[3, z] = gx
    ag_pass(3, z)
    dense_start(1, tn(mid[...], gm))
    with scope('one1'):
        one_finish(1)

    three = jnp.where(z < 2, 0, 1)
    last = jnp.where(z < 2, 3, 0)

    def first_step(k, carry):
        s = order(k)

        @pl.when(k == 2)
        def _():
            with scope('dmid1'):
                dense_middle(1)
            with scope('two1'):
                two_finish(1)

        @pl.when(jnp.logical_and(k == 3, outer))
        def _():
            with scope('wpart'):
                weight_part(0, three, 3)
        ag_step(3, k)
        with scope('b1'):
            backward(0, s, 3, 1, None)
        back_start(1, s)
        return carry
    lax.fori_loop(0, N_EP, first_step, 0)

    @pl.when(inner)
    def _():
        weight_part(0, three, 3)
    with scope('wg0'):
        weight_grads(0, last, 1, True)
    back_merge(1)
    with scope('dend1'):
        dense_end(1)
    with scope('one0'):
        one_finish(0)
    gm1 = (g_mid[...].astype(F32) + back_sum(1)).astype(BF16)
    dense_start(0, tn(x_ref[...], gm1))
    dx_v[...] = (gm1.astype(F32) + nt(gm1, dense1[...])).astype(BF16)
    dx_copy = pltpu.make_async_copy(dx_v, tok_out.at[pl.ds(0, n_tok)], out_sem.at[2])
    dx_copy.start()
    with scope('dmid0'):
        dense_middle(0)
    with scope('two0'):
        two_finish(0)
    with scope('dend0'):
        dense_end(0)
    den_copy = pltpu.make_async_copy(den_v, tok_out.at[pl.ds(n_tok, 2 * sub)], out_sem.at[3])
    den_copy.start()
    for n in range(4):
        ag_drain(n)
    ret_drain()
    for n in range(2):
        back_drain(n)
    for k in range(1, N_EP):
        aux_copy(k).wait_send()
    exp_copy(1).wait()
    exp_copy(0).wait()
    dx_copy.wait()
    den_copy.wait()


def solution(mesh):
    n_dp = mesh.shape['dp']
    n_chip = n_dp // 2
    tok_spec = P(('dp', 'ep'), None)
    exp_spec = P('ep', None, None)
    layer_specs = (P(None, None), tok_spec, tok_spec, exp_spec, exp_spec, exp_spec)
    grad_specs = (P(('dp', 'ep'), None), P('ep', 'dp', None), P('ep', 'dp', None), P('ep', None, 'dp'))

    def local_step(tokens, dy_out, dense_w1, idx1, gate1, wg1, wu1, wd1, dense_w2, idx2, gate2, wg2, wu2, wd2):
        n_tok, d_model = tokens.shape
        d_ff = wg1.shape[2]
        piece = d_model // n_dp
        sub = piece // N_EP
        vmem = pl.BlockSpec(memory_space=pltpu.VMEM)
        hbm = pl.BlockSpec(memory_space=pl.ANY)
        dma = pltpu.SemaphoreType.DMA
        outs = pl.pallas_call(
            functools.partial(kernel, n_dp),
            out_shape=(jax.ShapeDtypeStruct((n_tok + 2 * sub, d_model), BF16), jax.ShapeDtypeStruct((2, 6, piece, d_ff), BF16)),
            in_specs=[vmem] * 8 + [hbm] * 6,
            out_specs=[hbm] * 2,
            scratch_shapes=[
                pltpu.VMEM((2, 2, d_model, d_ff), BF16), pltpu.VMEM((2, 2, d_model, d_ff), BF16), pltpu.VMEM((2, 2, d_ff, d_model), BF16),
                pltpu.VMEM((8, n_tok), F32), pltpu.VMEM((N_EP, 8, n_tok), F32), pltpu.VMEM((4 * N_EP, 1, n_tok), F32), pltpu.VMEM((4 * N_EP, 1, n_tok), F32),
                pltpu.VMEM((2, n_tok, N_EXP), F32), pltpu.VMEM((2, n_tok, N_EXP), F32), pltpu.VMEM((n_tok, n_tok), BF16),
                pltpu.VMEM((4, N_EP, n_tok, d_model), BF16), pltpu.VMEM((2, N_EP, 2, CAP, d_model), BF16),
                pltpu.VMEM((2, N_EP, n_tok, d_model), BF16), pltpu.VMEM((2, N_EP, n_tok, d_model), BF16),
                pltpu.VMEM((2, 2, N_EP, CAP, d_model), BF16), pltpu.VMEM((2, CAP, d_ff), F32), pltpu.VMEM((2, CAP, d_ff), F32),
                pltpu.VMEM((2, CAP, d_ff), BF16), pltpu.VMEM((2, N_EP, CAP, d_ff), BF16), pltpu.VMEM((2, N_EP, CAP, d_ff), BF16),
                pltpu.VMEM((2, N_EP, CAP, d_ff), BF16), pltpu.VMEM((2, N_EP, CAP, d_model), BF16),
                pltpu.VMEM((n_tok, d_model), F32), pltpu.VMEM((n_tok, d_model), BF16), pltpu.VMEM((n_tok, d_model), BF16),
                pltpu.VMEM((2, 3, d_model, d_ff), F32),
                pltpu.VMEM((2, 2, 2, 2, 3, piece, d_ff), BF16), pltpu.VMEM((2, 2, 2, 2, 3, piece, d_ff), BF16),
                pltpu.VMEM((2, 2, 2, 3, piece, d_ff), BF16), pltpu.VMEM((2, 2, 3, piece, d_ff), BF16),
                pltpu.VMEM((2, N_EP, n_dp, sub, d_model), BF16), pltpu.VMEM((2, N_EP, n_dp, sub, d_model), BF16),
                pltpu.VMEM((2, n_dp, sub, d_model), BF16), pltpu.VMEM((2, n_dp, sub, d_model), BF16),
                pltpu.VMEM((2, 6, piece, d_ff), BF16), pltpu.VMEM((n_tok, d_model), BF16), pltpu.VMEM((2 * sub, d_model), BF16),
                dma((6,)), dma((N_EP,)), dma((N_EP,)), dma((4, N_EP)), dma((4, N_EP)), dma((4, N_EP)), dma((N_EP,)), dma((N_EP,)),
                dma((2, N_EP)), dma((2, N_EP)), dma((2, 2)), dma((2, 2)), dma((2, 2)), dma((2, 2)), dma((2, 2)), dma((2, 2)),
                dma((2, N_EP)), dma((2, N_EP)), dma((2, n_dp)), dma((2, n_dp)), dma((4,)),
            ],
            compiler_params=pltpu.CompilerParams(collective_id=0, has_side_effects=True, vmem_limit_bytes=67043328),
        )(tokens, dy_out, dense_w1, dense_w2, idx1.T, gate1.T, idx2.T, gate2.T, wg1, wu1, wd1, wg2, wu2, wd2)
        tok, exp = outs
        res = [tok[:n_tok]]
        for layer in range(2):
            res += [tok[n_tok + layer * sub:n_tok + (layer + 1) * sub], exp[layer, 0:2], exp[layer, 2:4], jnp.swapaxes(exp[layer, 4:6], 1, 2)]
        return tuple(res)

    return jax.shard_map(local_step, mesh=mesh, in_specs=(tok_spec, tok_spec) + layer_specs + layer_specs,
                         out_specs=(tok_spec,) + grad_specs + grad_specs, check_vma=False)
```

```python
import functools

import jax
import jax.numpy as jnp
from jax import lax
from jax.experimental import pallas as pl
from jax.experimental.pallas import tpu as pltpu
from jax.sharding import PartitionSpec as P

MESH = pl.DeviceIdType.MESH
F32, BF16 = jnp.float32, jnp.bfloat16
N_EP = 4
scope = jax.named_scope
N_EXP = 8
CAP = 256


def nn(a, b):
    return lax.dot_general(a, b, (((1,), (0,)), ((), ())), preferred_element_type=F32)


def nt(a, b):
    return lax.dot_general(a, b, (((1,), (1,)), ((), ())), preferred_element_type=F32)


def tn(a, b):
    return lax.dot_general(a, b, (((0,), (0,)), ((), ())), preferred_element_type=F32)


def kernel(n_dp, x_ref, dy_ref, dense1, dense2, idx1, gate1, idx2, gate2,
           wg1_hbm, wu1_hbm, wd1_hbm, wg2_hbm, wu2_hbm, wd2_hbm,
           tok_out, exp_out,
           w_gate, w_up, w_down, auxs, auxb, posr, gater, posc, gatec, tri, ag, ret, back_out, back_in, rows_in, t_a, t_b, t_gh, hid, g_a, g_b, g_out,
           acc, mid, g_mid, part, gs, gr, g2, g3, d_send, d_a, d_bs, d_b, exp_v, dx_v, den_v,
           w_sem, aux_send, aux_recv, ag_right, ag_left, ag_recv, ret_send, ret_recv, back_send, back_recv, pair_send, pair_recv,
           one_send, one_recv, two_send, two_recv, da_send, da_recv, db_send, db_recv, out_sem):
    z = lax.axis_index('ep')
    dp = lax.axis_index('dp')
    n_chip = n_dp // 2
    core = dp % 2
    chip = dp // 2
    n_tok, d_model = x_ref.shape
    d_ff = t_a.shape[2]
    piece = d_model // n_dp

    def order(k):
        near_low = jnp.where(z == 1, jnp.where(k == 0, 1, jnp.where(k == 1, 0, k)), k)
        near_high = 3 - jnp.where(z == 2, jnp.where(k == 0, 1, jnp.where(k == 1, 0, k)), k)
        return jnp.where(z < 2, near_low, near_high)

    barrier = pltpu.get_barrier_semaphore()
    for k in range(1, N_EP):
        pl.semaphore_signal(barrier, inc=1, device_id={'ep': (z + k) % N_EP, 'dp': dp}, device_id_type=MESH)
    for k in range(1, n_dp):
        pl.semaphore_signal(barrier, inc=1, device_id={'ep': z, 'dp': (dp + k) % n_dp}, device_id_type=MESH)

    w_copies = []
    for n, (hbm, dst) in enumerate(((wg1_hbm, w_gate.at[0]), (wu1_hbm, w_up.at[0]), (wd1_hbm, w_down.at[0]),
                                    (wg2_hbm, w_gate.at[1]), (wu2_hbm, w_up.at[1]), (wd2_hbm, w_down.at[1]))):
        w_copies.append(pltpu.make_async_copy(hbm, dst, w_sem.at[n]))
        w_copies[-1].start()

    auxs[0:2] = idx1[...].astype(F32)
    auxs[2:4] = gate1[...]
    auxs[4:6] = idx2[...].astype(F32)
    auxs[6:8] = gate2[...]
    x = x_ref[...]
    ag[0, z] = (x.astype(F32) + nn(x, dense1[...])).astype(BF16)
    ag[2, z] = dy_ref[...]
    auxb[z] = auxs[...]

    with scope('barrier'):
        pl.semaphore_wait(barrier, N_EP - 1 + n_dp - 1)

    def col_copy(src, dst, send, recv, to):
        return pltpu.make_async_remote_copy(src_ref=src, dst_ref=dst, send_sem=send, recv_sem=recv,
                                            device_id={'ep': to, 'dp': dp}, device_id_type=MESH)

    def row_copy(src, dst, send, recv, to):
        return pltpu.make_async_remote_copy(src_ref=src, dst_ref=dst, send_sem=send, recv_sem=recv,
                                            device_id={'ep': z, 'dp': to}, device_id_type=MESH)

    def aux_copy(k):
        return col_copy(auxs, auxb.at[z], aux_send.at[k], aux_recv.at[z], (z + k) % N_EP)

    for k in range(1, N_EP):
        aux_copy(k).start()

    def ag_to_right(n, s):
        return col_copy(ag.at[n, s], ag.at[n, s], ag_right.at[n, s], ag_recv.at[n, s], jnp.minimum(z + 1, N_EP - 1))

    def ag_to_left(n, s):
        return col_copy(ag.at[n, s], ag.at[n, s], ag_left.at[n, s], ag_recv.at[n, s], jnp.maximum(z - 1, 0))

    def ag_pass(n, s):
        @pl.when(jnp.logical_and(s <= z, z < N_EP - 1))
        def _():
            ag_to_right(n, s).start()

        @pl.when(jnp.logical_and(s >= z, z > 0))
        def _():
            ag_to_left(n, s).start()

    def ag_take(n, s):
        with scope('agw%d' % n):
            ag_to_right(n, s).wait_recv()
        ag_pass(n, s)

    def ag_step(n, k):
        inner = jnp.logical_or(z == 1, z == 2)
        outer = jnp.logical_not(inner)

        @pl.when(k == 1)
        def _():
            ag_take(n, order(1))

        @pl.when(jnp.logical_or(jnp.logical_and(k == 1, inner), jnp.logical_and(k == 2, outer)))
        def _():
            ag_take(n, order(2))

        @pl.when(k == 3)
        def _():
            ag_take(n, order(3))

    def ag_drain(n):
        def body(s, carry):
            @pl.when(jnp.logical_and(s <= z, z < N_EP - 1))
            def _():
                ag_to_right(n, s).wait_send()

            @pl.when(jnp.logical_and(s >= z, z > 0))
            def _():
                ag_to_left(n, s).wait_send()
            return carry
        lax.fori_loop(0, N_EP, body, 0)

    def ret_copy(s):
        return col_copy(ret.at[0, s], ret.at[1, z], ret_send.at[s], ret_recv.at[z], s)

    def ret_wait(s):
        col_copy(ret.at[0, s], ret.at[1, s], ret_send.at[s], ret_recv.at[s], s).wait_recv()

    def ret_drain():
        for k in range(1, N_EP):
            ret_copy((z + k) % N_EP).wait_send()

    ag_pass(0, z)

    r_io = lax.broadcasted_iota(jnp.int32, (n_tok, n_tok), 0)
    c_io = lax.broadcasted_iota(jnp.int32, (n_tok, n_tok), 1)
    tri[...] = (c_io < r_io).astype(F32).astype(BF16)
    lane = lax.broadcasted_iota(jnp.int32, (n_tok, N_EXP), 1)
    cols = auxs[...].T
    for layer in range(2):
        hit0 = cols[:, 4 * layer:4 * layer + 1] == lane.astype(F32)
        hit1 = cols[:, 4 * layer + 1:4 * layer + 2] == lane.astype(F32)
        hit = jnp.logical_or(hit0, hit1)
        rank = nn(tri[...], hit.astype(F32).astype(BF16))
        posc[layer] = jnp.where(hit, rank, -1.0)
        gatec[layer] = jnp.where(hit0, cols[:, 4 * layer + 2:4 * layer + 3], 0.0) + jnp.where(hit1, cols[:, 4 * layer + 3:4 * layer + 4], 0.0)
    for k in range(1, N_EP):
        s = (z + k) % N_EP
        col_copy(auxs, auxb.at[s], aux_send.at[k], aux_recv.at[s], s).wait_recv()
    hits = []
    for layer in range(2):
        for s in range(N_EP):
            for e in range(2):
                a = auxb[s]
                expert = (z * 2 + e).astype(F32)
                hit0 = a[4 * layer:4 * layer + 1] == expert
                hit1 = a[4 * layer + 1:4 * layer + 2] == expert
                hits.append(jnp.logical_or(hit0, hit1).astype(F32))
                gater[(layer * N_EP + s) * 2 + e] = (jnp.where(hit0, a[4 * layer + 2:4 * layer + 3], 0.0)
                                                     + jnp.where(hit1, a[4 * layer + 3:4 * layer + 4], 0.0))
    stack = jnp.concatenate(hits, axis=0)
    ranks = jnp.where(stack > 0.5, nt(stack.astype(BF16), tri[...]), -1.0)
    for n in range(4 * N_EP):
        posr[n] = ranks[n:n + 1]

    for copy in w_copies:
        copy.wait()

    slot = lax.broadcasted_iota(jnp.int32, (CAP, n_tok), 0).astype(F32)
    slot_lane = lax.broadcasted_iota(jnp.int32, (n_tok, CAP), 1).astype(F32)
    step = 32

    def select(layer, s):
        at = (layer * N_EP + s) * 2
        return [posr[at + e] == slot for e in range(2)]

    def as_bf16(picks):
        return jnp.concatenate([p.astype(F32).astype(BF16) for p in picks], axis=0)

    def take_rows(layer, s, n, pick):
        rows = nn(pick, ag[n, s]).astype(BF16)
        for e in range(2):
            rows_in[layer, e, s] = rows[e * CAP:(e + 1) * CAP]

    def up_project(layer, s, e):
        rows = rows_in[layer, e, s]
        t_a[e] = nn(rows, w_gate[layer, e])
        t_b[e] = nn(rows, w_up[layer, e])

    def forward(s):
        take_rows(0, s, 0, as_bf16(select(0, s)))
        for e in range(2):
            up_project(0, s, e)
        for e in range(2):
            for i in range(CAP // step):
                r = pl.ds(i * step, step)
                a = t_a[e, r, :]
                hid[e, s, r, :] = (a * jax.nn.sigmoid(a) * t_b[e, r, :]).astype(BF16)
            ret[jnp.where(s == z, 1, 0), s, e] = nn(hid[e, s], w_down[0, e]).astype(BF16)

    def backward(layer, s, n_dy, n_back, n_u):
        picks = select(layer, s)
        pick = as_bf16(picks)
        at = (layer * N_EP + s) * 2
        if n_u is not None:
            take_rows(layer, s, n_u, pick)
        got = nn(pick, ag[n_dy, s])
        for e in range(2):
            gate = jnp.sum(jnp.where(picks[e], gater[at + e], 0.0), axis=1, keepdims=True)
            g_out[e, s] = (got[e * CAP:(e + 1) * CAP] * gate).astype(BF16)
        for e in range(2):
            up_project(layer, s, e)
            t_gh[e] = nt(g_out[e, s], w_down[layer, e]).astype(BF16)
        parts = []
        for e in range(2):
            for i in range(CAP // step):
                r = pl.ds(i * step, step)
                a = t_a[e, r, :]
                b = t_b[e, r, :]
                gh = t_gh[e, r, :].astype(F32)
                sig = jax.nn.sigmoid(a)
                act = a * sig
                hid[e, s, r, :] = (act * b).astype(BF16)
                g_a[e, s, r, :] = (gh * b * sig * (1.0 + a * (1.0 - sig))).astype(BF16)
                g_b[e, s, r, :] = (gh * act).astype(BF16)
            parts.append((nt(g_a[e, s], w_gate[layer, e]) + nt(g_b[e, s], w_up[layer, e])).astype(BF16))
        back_out[n_back, s] = tn(pick, jnp.concatenate(parts, axis=0)).astype(BF16)

    def send_back(s):
        @pl.when(s != z)
        def _():
            ret_copy(s).start()

    def gather_back():
        acc[...] = jnp.zeros_like(acc)

        def body(k, carry):
            s = order(k)

            @pl.when(k > 0)
            def _():
                with scope('retw'):
                    ret_wait(s)

            for e in range(2):
                here = lane == s * 2 + e
                pos = jnp.sum(jnp.where(here, posc[0], 0.0), axis=1, keepdims=True)
                weight = jnp.sum(jnp.where(here, gatec[0], 0.0), axis=1, keepdims=True)
                acc[...] += nn((pos == slot_lane).astype(F32).astype(BF16), ret[1, s, e]) * weight
            return carry
        lax.fori_loop(0, N_EP, body, 0)

    inner = jnp.logical_or(z == 1, z == 2)
    outer = jnp.logical_not(inner)
    beside = jnp.where(z < 2, 1, 2)
    near_end = jnp.where(z < 2, 0, 3)

    def back_copy(n, s, slot_in, to):
        return col_copy(back_out.at[n, s], back_in.at[n, slot_in], back_send.at[n, s], back_recv.at[n, slot_in], to)

    def back_plan(s):
        dist = jnp.abs(z - s)
        slot_in = jnp.where(inner, 0, jnp.where(dist == 1, 2, jnp.where(dist == 2, 1, 3)))
        to = jnp.where(inner, 3 - z, jnp.where(dist == 2, beside, s))
        go = jnp.where(inner, dist == 2, dist > 0)
        return slot_in, to, go

    def back_start(n, s):
        slot_in, to, go = back_plan(s)

        @pl.when(go)
        def _():
            back_copy(n, s, slot_in, to).start()

    def back_wait(n, slot_in):
        with scope('bk%d%d' % (n, slot_in)):
            back_copy(n, 0, slot_in, z).wait_recv()

    def back_merge(n):
        @pl.when(inner)
        def _():
            for slot_in, s, slot_out in ((0, near_end, 2), (1, 3 - z, 3)):
                back_wait(n, slot_in)
                back_out[n, s] = (back_out[n, s].astype(F32) + back_in[n, slot_in].astype(F32)).astype(BF16)
                back_copy(n, s, slot_out, s).start()

    def back_sum(n):
        back_wait(n, 2)
        back_wait(n, 3)
        return back_out[n, z].astype(F32) + back_in[n, 2].astype(F32) + back_in[n, 3].astype(F32)

    def back_drain(n):
        for k in range(1, N_EP):
            back_copy(n, (z + k) % N_EP, 0, z).wait_send()

    chip_x = chip % 2
    chip_y = chip // 2
    over_x = chip + 1 - 2 * chip_x
    over_y = (chip + 2) % n_chip

    def group(e):
        return jnp.where(e == 0, chip_x, chip_y)

    def place(e):
        return jnp.where(e == 0, chip_y, chip_x)

    def pair_copy(layer, e):
        return row_copy(gs.at[1 - core, e], gr.at[layer, e], pair_send.at[layer, e], pair_recv.at[layer, e], chip * 2 + 1 - core)

    def one_copy(layer, e):
        return row_copy(gr.at[layer, e, 1 - group(e)], g2.at[layer, e], one_send.at[layer, e], one_recv.at[layer, e],
                        jnp.where(e == 0, over_x, over_y) * 2 + core)

    def two_copy(layer, e):
        return row_copy(gr.at[layer, e, group(e), 1 - place(e)], g3.at[layer, e], two_send.at[layer, e], two_recv.at[layer, e],
                        jnp.where(e == 0, over_y, over_x) * 2 + core)

    def pair_finish(layer, e):
        pair_copy(layer, e).wait()

        def body(q, carry):
            for g in range(2):
                for p in range(2):
                    gr[layer, e, g, p, q] = (gr[layer, e, g, p, q].astype(F32) + gs[core, e, g, p, q].astype(F32)).astype(BF16)
            return carry
        lax.fori_loop(0, 3, body, 0)
        one_copy(layer, e).start()

    def one_finish(layer):
        def body(e, carry):
            one_copy(layer, e).wait_recv()
            for p in range(2):
                for q in range(3):
                    gr[layer, e, group(e), p, q] = (gr[layer, e, group(e), p, q].astype(F32) + g2[layer, e, p, q].astype(F32)).astype(BF16)
            two_copy(layer, e).start()
            return carry
        lax.fori_loop(0, 2, body, 0)

    def two_finish(layer):
        def body(e, carry):
            two_copy(layer, e).wait_recv()
            for q in range(3):
                exp_v[layer, q * 2 + e] = (gr[layer, e, group(e), place(e), q].astype(F32) + g3[layer, e, q].astype(F32)).astype(BF16)
            one_copy(layer, e).wait_send()
            two_copy(layer, e).wait_send()
            return carry
        lax.fori_loop(0, 2, body, 0)
        exp_copy(layer).start()

    def exp_copy(layer):
        return pltpu.make_async_copy(exp_v.at[layer], exp_out.at[layer], out_sem.at[layer])

    def operands(layer, e, at, n):
        rows = rows_in[layer, e, pl.ds(at, n)].reshape(n * CAP, d_model)
        outs = g_out[e, pl.ds(at, n)].reshape(n * CAP, d_model)
        for q, (left, right) in enumerate(((outs, hid), (rows, g_a), (rows, g_b))):
            yield q, (q + 2) % 3, left, right[e, pl.ds(at, n)].reshape(n * CAP, d_ff)

    def weight_part(layer, at, n):
        def body(e, carry):
            for q, j, left, right in operands(layer, e, at, n):
                part[e, q] = tn(left, right)
            return carry
        lax.fori_loop(0, 2, body, 0)

    def weight_grads(layer, at, n, add):
        def body(e, carry):
            for q, j, left, right in operands(layer, e, at, n):
                grad = tn(left, right)
                if add:
                    grad = grad + part[e, q]
                for p in range(n_dp):
                    y, x = p // 4, p // 2 % 2
                    gs[p % 2, e, jnp.where(e == 0, x, y), jnp.where(e == 0, y, x), j] = grad[p * piece:(p + 1) * piece].astype(BF16)
            pair_copy(layer, e).start()
            return carry
        lax.fori_loop(0, 2, body, 0)
        pair_finish(layer, 0)
        pair_finish(layer, 1)

    sub = piece // N_EP

    def da_copy(layer, k):
        to = (z + k) % N_EP
        return col_copy(d_send.at[layer, to], d_a.at[layer, z], da_send.at[layer, k], da_recv.at[layer, z], to)

    def db_copy(layer, k):
        to = (dp + k) % n_dp
        return row_copy(d_bs.at[layer, to], d_b.at[layer, dp], db_send.at[layer, k], db_recv.at[layer, dp], to)

    def dense_start(layer, grad):
        for q in range(N_EP):
            for p in range(n_dp):
                at = p * piece + q * sub
                d_send[layer, q, p] = grad[at:at + sub].astype(BF16)
        for k in range(1, N_EP):
            da_copy(layer, k).start()

    def dense_middle(layer):
        total = d_send[layer, z].astype(F32)
        for k in range(1, N_EP):
            frm = (z + k) % N_EP
            col_copy(d_send.at[layer, frm], d_a.at[layer, frm], da_send.at[layer, k], da_recv.at[layer, frm], frm).wait_recv()
            total += d_a[layer, frm].astype(F32)
        d_bs[layer] = total.astype(BF16)
        for k in range(1, n_dp):
            db_copy(layer, k).start()

    def dense_end(layer):
        total = d_bs[layer, dp].astype(F32)
        for k in range(1, n_dp):
            frm = (dp + k) % n_dp
            row_copy(d_bs.at[layer, frm], d_b.at[layer, frm], db_send.at[layer, k], db_recv.at[layer, frm], frm).wait_recv()
            total += d_b[layer, frm].astype(F32)
        den_v[layer * sub:(layer + 1) * sub] = total.astype(BF16)
        for k in range(1, N_EP):
            da_copy(layer, k).wait_send()
        for k in range(1, n_dp):
            db_copy(layer, k).wait_send()

    def forward_step(k, carry):
        s = order(k)
        ag_step(0, k)
        with scope('f1'):
            forward(s)
        send_back(s)
        return carry
    lax.fori_loop(0, N_EP, forward_step, 0)
    gather_back()
    ag_pass(2, z)
    y = (ag[0, z].astype(F32) + acc[...]).astype(BF16)
    mid[...] = y
    ag[1, z] = (y.astype(F32) + nn(y, dense2[...])).astype(BF16)
    ag_pass(1, z)

    def second_step(k, carry):
        s = order(k)
        ag_step(2, k)
        ag_step(1, k)
        with scope('fb2'):
            backward(1, s, 2, 0, 1)
        back_start(0, s)
        return carry
    lax.fori_loop(0, N_EP, second_step, 0)
    with scope('wg1'):
        weight_grads(1, 0, N_EP, False)
    back_merge(0)
    gm = (dy_ref[...].astype(F32) + back_sum(0)).astype(BF16)
    gx = (gm.astype(F32) + nt(gm, dense2[...])).astype(BF16)
    g_mid[...] = gx
    ag[3, z] = gx
    ag_pass(3, z)
    dense_start(1, tn(mid[...], gm))
    three = jnp.where(z < 2, 0, 1)
    last = jnp.where(z < 2, 3, 0)

    def first_step(k, carry):
        s = order(k)

        @pl.when(k == 2)
        def _():
            with scope('dmid1'):
                dense_middle(1)
            with scope('one1'):
                one_finish(1)

        @pl.when(k == 3)
        def _():
            with scope('two1'):
                two_finish(1)

        @pl.when(jnp.logical_and(k == 3, outer))
        def _():
            with scope('wpart'):
                weight_part(0, three, 3)
        ag_step(3, k)
        with scope('b1'):
            backward(0, s, 3, 1, None)
        back_start(1, s)
        return carry
    lax.fori_loop(0, N_EP, first_step, 0)

    @pl.when(inner)
    def _():
        weight_part(0, three, 3)
    with scope('wg0'):
        weight_grads(0, last, 1, True)
    back_merge(1)
    with scope('dend1'):
        dense_end(1)
    with scope('one0'):
        one_finish(0)
    gm1 = (g_mid[...].astype(F32) + back_sum(1)).astype(BF16)
    dense_start(0, tn(x_ref[...], gm1))
    dx_v[...] = (gm1.astype(F32) + nt(gm1, dense1[...])).astype(BF16)
    dx_copy = pltpu.make_async_copy(dx_v, tok_out.at[pl.ds(0, n_tok)], out_sem.at[2])
    dx_copy.start()
    with scope('dmid0'):
        dense_middle(0)
    with scope('two0'):
        two_finish(0)
    with scope('dend0'):
        dense_end(0)
    den_copy = pltpu.make_async_copy(den_v, tok_out.at[pl.ds(n_tok, 2 * sub)], out_sem.at[3])
    den_copy.start()
    for n in range(4):
        ag_drain(n)
    ret_drain()
    for n in range(2):
        back_drain(n)
    for k in range(1, N_EP):
        aux_copy(k).wait_send()
    exp_copy(1).wait()
    exp_copy(0).wait()
    dx_copy.wait()
    den_copy.wait()


def solution(mesh):
    n_dp = mesh.shape['dp']
    n_chip = n_dp // 2
    tok_spec = P(('dp', 'ep'), None)
    exp_spec = P('ep', None, None)
    layer_specs = (P(None, None), tok_spec, tok_spec, exp_spec, exp_spec, exp_spec)
    grad_specs = (P(('dp', 'ep'), None), P('ep', 'dp', None), P('ep', 'dp', None), P('ep', None, 'dp'))

    def local_step(tokens, dy_out, dense_w1, idx1, gate1, wg1, wu1, wd1, dense_w2, idx2, gate2, wg2, wu2, wd2):
        n_tok, d_model = tokens.shape
        d_ff = wg1.shape[2]
        piece = d_model // n_dp
        sub = piece // N_EP
        vmem = pl.BlockSpec(memory_space=pltpu.VMEM)
        hbm = pl.BlockSpec(memory_space=pl.ANY)
        dma = pltpu.SemaphoreType.DMA
        outs = pl.pallas_call(
            functools.partial(kernel, n_dp),
            out_shape=(jax.ShapeDtypeStruct((n_tok + 2 * sub, d_model), BF16), jax.ShapeDtypeStruct((2, 6, piece, d_ff), BF16)),
            in_specs=[vmem] * 8 + [hbm] * 6,
            out_specs=[hbm] * 2,
            scratch_shapes=[
                pltpu.VMEM((2, 2, d_model, d_ff), BF16), pltpu.VMEM((2, 2, d_model, d_ff), BF16), pltpu.VMEM((2, 2, d_ff, d_model), BF16),
                pltpu.VMEM((8, n_tok), F32), pltpu.VMEM((N_EP, 8, n_tok), F32), pltpu.VMEM((4 * N_EP, 1, n_tok), F32), pltpu.VMEM((4 * N_EP, 1, n_tok), F32),
                pltpu.VMEM((2, n_tok, N_EXP), F32), pltpu.VMEM((2, n_tok, N_EXP), F32), pltpu.VMEM((n_tok, n_tok), BF16),
                pltpu.VMEM((4, N_EP, n_tok, d_model), BF16), pltpu.VMEM((2, N_EP, 2, CAP, d_model), BF16),
                pltpu.VMEM((2, N_EP, n_tok, d_model), BF16), pltpu.VMEM((2, N_EP, n_tok, d_model), BF16),
                pltpu.VMEM((2, 2, N_EP, CAP, d_model), BF16), pltpu.VMEM((2, CAP, d_ff), F32), pltpu.VMEM((2, CAP, d_ff), F32),
                pltpu.VMEM((2, CAP, d_ff), BF16), pltpu.VMEM((2, N_EP, CAP, d_ff), BF16), pltpu.VMEM((2, N_EP, CAP, d_ff), BF16),
                pltpu.VMEM((2, N_EP, CAP, d_ff), BF16), pltpu.VMEM((2, N_EP, CAP, d_model), BF16),
                pltpu.VMEM((n_tok, d_model), F32), pltpu.VMEM((n_tok, d_model), BF16), pltpu.VMEM((n_tok, d_model), BF16),
                pltpu.VMEM((2, 3, d_model, d_ff), F32),
                pltpu.VMEM((2, 2, 2, 2, 3, piece, d_ff), BF16), pltpu.VMEM((2, 2, 2, 2, 3, piece, d_ff), BF16),
                pltpu.VMEM((2, 2, 2, 3, piece, d_ff), BF16), pltpu.VMEM((2, 2, 3, piece, d_ff), BF16),
                pltpu.VMEM((2, N_EP, n_dp, sub, d_model), BF16), pltpu.VMEM((2, N_EP, n_dp, sub, d_model), BF16),
                pltpu.VMEM((2, n_dp, sub, d_model), BF16), pltpu.VMEM((2, n_dp, sub, d_model), BF16),
                pltpu.VMEM((2, 6, piece, d_ff), BF16), pltpu.VMEM((n_tok, d_model), BF16), pltpu.VMEM((2 * sub, d_model), BF16),
                dma((6,)), dma((N_EP,)), dma((N_EP,)), dma((4, N_EP)), dma((4, N_EP)), dma((4, N_EP)), dma((N_EP,)), dma((N_EP,)),
                dma((2, N_EP)), dma((2, N_EP)), dma((2, 2)), dma((2, 2)), dma((2, 2)), dma((2, 2)), dma((2, 2)), dma((2, 2)),
                dma((2, N_EP)), dma((2, N_EP)), dma((2, n_dp)), dma((2, n_dp)), dma((4,)),
            ],
            compiler_params=pltpu.CompilerParams(collective_id=0, has_side_effects=True, vmem_limit_bytes=67043328),
        )(tokens, dy_out, dense_w1, dense_w2, idx1.T, gate1.T, idx2.T, gate2.T, wg1, wu1, wd1, wg2, wu2, wd2)
        tok, exp = outs
        res = [tok[:n_tok]]
        for layer in range(2):
            res += [tok[n_tok + layer * sub:n_tok + (layer + 1) * sub], exp[layer, 0:2], exp[layer, 2:4], jnp.swapaxes(exp[layer, 4:6], 1, 2)]
        return tuple(res)

    return jax.shard_map(local_step, mesh=mesh, in_specs=(tok_spec, tok_spec) + layer_specs + layer_specs,
                         out_specs=(tok_spec,) + grad_specs + grad_specs, check_vma=False)
```

```python
import functools

import jax
import jax.numpy as jnp
from jax import lax
from jax.experimental import pallas as pl
from jax.experimental.pallas import tpu as pltpu
from jax.sharding import PartitionSpec as P

MESH = pl.DeviceIdType.MESH
F32, BF16 = jnp.float32, jnp.bfloat16
N_EP = 4
scope = jax.named_scope
N_EXP = 8
CAP = 256


def nn(a, b):
    return lax.dot_general(a, b, (((1,), (0,)), ((), ())), preferred_element_type=F32)


def nt(a, b):
    return lax.dot_general(a, b, (((1,), (1,)), ((), ())), preferred_element_type=F32)


def tn(a, b):
    return lax.dot_general(a, b, (((0,), (0,)), ((), ())), preferred_element_type=F32)


def kernel(n_dp, x_ref, dy_ref, dense1, dense2, idx1, gate1, idx2, gate2,
           wg1_hbm, wu1_hbm, wd1_hbm, wg2_hbm, wu2_hbm, wd2_hbm,
           tok_out, exp_out,
           w_gate, w_up, w_down, auxs, auxb, posr, gater, posc, gatec, tri, ag, ret, x_end, rows_in, t_a, t_b, t_gh, hid, g_a, g_b, g_out,
           acc, g_mix, part, gs, gr, g2, g3, d_send, d_a, d_bs, d_b, exp_v, dx_v, den_v,
           w_sem, aux_send, aux_recv, ag_right, ag_left, ag_recv, ret_send, ret_recv, end_send, end_recv, pair_send, pair_recv,
           one_send, one_recv, two_send, two_recv, da_send, da_recv, db_send, db_recv, out_sem):
    z = lax.axis_index('ep')
    dp = lax.axis_index('dp')
    n_chip = n_dp // 2
    core = dp % 2
    chip = dp // 2
    n_tok, d_model = x_ref.shape
    d_ff = t_a.shape[2]
    piece = d_model // n_dp

    def order(k):
        near_low = jnp.where(z == 1, jnp.where(k == 0, 1, jnp.where(k == 1, 0, k)), k)
        near_high = 3 - jnp.where(z == 2, jnp.where(k == 0, 1, jnp.where(k == 1, 0, k)), k)
        return jnp.where(z < 2, near_low, near_high)

    def order_owned(k):
        low = jnp.where(k == 0, 1, jnp.where(k == 1, 0, k))
        return jnp.where(z < 2, low, 3 - low)

    def owner(s):
        return jnp.where(s < 2, 1, 2)

    inner = jnp.logical_or(z == 1, z == 2)
    outer = jnp.logical_not(inner)
    near_mid = jnp.where(z < 2, 1, 2)
    near_end = jnp.where(z < 2, 0, 3)

    barrier = pltpu.get_barrier_semaphore()
    for k in range(1, N_EP):
        pl.semaphore_signal(barrier, inc=1, device_id={'ep': (z + k) % N_EP, 'dp': dp}, device_id_type=MESH)
    for k in range(1, n_dp):
        pl.semaphore_signal(barrier, inc=1, device_id={'ep': z, 'dp': (dp + k) % n_dp}, device_id_type=MESH)

    w_copies = []
    for n, (hbm, dst) in enumerate(((wg1_hbm, w_gate.at[0]), (wu1_hbm, w_up.at[0]), (wd1_hbm, w_down.at[0]),
                                    (wg2_hbm, w_gate.at[1]), (wu2_hbm, w_up.at[1]), (wd2_hbm, w_down.at[1]))):
        w_copies.append(pltpu.make_async_copy(hbm, dst, w_sem.at[n]))
        w_copies[-1].start()

    auxs[0:2] = idx1[...].astype(F32)
    auxs[2:4] = gate1[...]
    auxs[4:6] = idx2[...].astype(F32)
    auxs[6:8] = gate2[...]
    x = x_ref[...]
    ag[0, z] = (x.astype(F32) + nn(x, dense1[...])).astype(BF16)
    ag[2, z] = dy_ref[...]
    auxb[z] = auxs[...]

    with scope('barrier'):
        pl.semaphore_wait(barrier, N_EP - 1 + n_dp - 1)

    def col_copy(src, dst, send, recv, to):
        return pltpu.make_async_remote_copy(src_ref=src, dst_ref=dst, send_sem=send, recv_sem=recv,
                                            device_id={'ep': to, 'dp': dp}, device_id_type=MESH)

    def row_copy(src, dst, send, recv, to):
        return pltpu.make_async_remote_copy(src_ref=src, dst_ref=dst, send_sem=send, recv_sem=recv,
                                            device_id={'ep': z, 'dp': to}, device_id_type=MESH)

    def aux_copy(k):
        return col_copy(auxs, auxb.at[z], aux_send.at[k], aux_recv.at[z], (z + k) % N_EP)

    for k in range(1, N_EP):
        aux_copy(k).start()

    def ag_to_right(n, s):
        return col_copy(ag.at[n, s], ag.at[n, s], ag_right.at[n, s], ag_recv.at[n, s], jnp.minimum(z + 1, N_EP - 1))

    def ag_to_left(n, s):
        return col_copy(ag.at[n, s], ag.at[n, s], ag_left.at[n, s], ag_recv.at[n, s], jnp.maximum(z - 1, 0))

    def rightward(n, s):
        return jnp.logical_and((owner(s) if n % 2 else s) <= z, z < N_EP - 1)

    def leftward(n, s):
        return jnp.logical_and((owner(s) if n % 2 else s) >= z, z > 0)

    def ag_pass(n, s, right=True, left=True):
        if right is not False:
            @pl.when(jnp.logical_and(rightward(n, s), right))
            def _():
                ag_to_right(n, s).start()

        if left is not False:
            @pl.when(jnp.logical_and(leftward(n, s), left))
            def _():
                ag_to_left(n, s).start()

    def ag_take(n, s):
        with scope('agw%d' % n):
            ag_to_right(n, s).wait_recv()
        ag_pass(n, s)

    def ag_step(n, k):
        @pl.when(k == 1)
        def _():
            ag_take(n, order(1))

        @pl.when(jnp.logical_or(jnp.logical_and(k == 1, inner), jnp.logical_and(k == 2, outer)))
        def _():
            ag_take(n, order(2))

        @pl.when(k == 3)
        def _():
            ag_take(n, order(3))

    def owned_step(n, k, s):
        @pl.when(jnp.logical_or(k > 1, outer))
        def _():
            ag_take(n, s)

    def ag_drain(n):
        def body(s, carry):
            @pl.when(rightward(n, s))
            def _():
                ag_to_right(n, s).wait_send()

            @pl.when(leftward(n, s))
            def _():
                ag_to_left(n, s).wait_send()
            return carry
        lax.fori_loop(0, N_EP, body, 0)

    def ret_at(s):
        return jnp.where(owner(s) == z, N_EP + s % 2 * N_EP + z, s)

    def ret_copy(n, s):
        return col_copy(ret.at[n, s], ret.at[n, N_EP + s % 2 * N_EP + z], ret_send.at[n, s], ret_recv.at[n, s % 2 * N_EP + z], owner(s))

    def ret_start(n, s):
        @pl.when(owner(s) != z)
        def _():
            ret_copy(n, s).start()

    def ret_wait(n, p, frm):
        with scope('retw%d' % n):
            at = p * N_EP + frm
            col_copy(ret.at[n, 0], ret.at[n, N_EP + at], ret_send.at[n, 0], ret_recv.at[n, at], z).wait_recv()

    def ret_drain(n):
        def body(s, carry):
            @pl.when(owner(s) != z)
            def _():
                ret_copy(n, s).wait_send()
            return carry
        lax.fori_loop(0, N_EP, body, 0)

    def x_copy():
        return col_copy(x_ref, x_end, end_send.at[0], end_recv.at[0], near_mid)

    def dx_back():
        return col_copy(g_mix.at[0], dx_v, end_send.at[1], end_recv.at[1], near_end)

    ag_pass(0, z)

    r_io = lax.broadcasted_iota(jnp.int32, (n_tok, n_tok), 0)
    c_io = lax.broadcasted_iota(jnp.int32, (n_tok, n_tok), 1)
    tri[...] = (c_io < r_io).astype(F32).astype(BF16)
    lane = lax.broadcasted_iota(jnp.int32, (n_tok, N_EXP), 1)
    for k in range(1, N_EP):
        s = (z + k) % N_EP
        col_copy(auxs, auxb.at[s], aux_send.at[k], aux_recv.at[s], s).wait_recv()
    for p in range(2):
        cols = auxb[jnp.where(z < 2, 0, 2) + p].T
        hit0 = cols[:, 0:1] == lane.astype(F32)
        hit1 = cols[:, 1:2] == lane.astype(F32)
        hit = jnp.logical_or(hit0, hit1)
        rank = nn(tri[...], hit.astype(F32).astype(BF16))
        posc[p] = jnp.where(hit, rank, -1.0)
        gatec[p] = jnp.where(hit0, cols[:, 2:3], 0.0) + jnp.where(hit1, cols[:, 3:4], 0.0)
    hits = []
    for layer in range(2):
        for s in range(N_EP):
            for e in range(2):
                a = auxb[s]
                expert = (z * 2 + e).astype(F32)
                hit0 = a[4 * layer:4 * layer + 1] == expert
                hit1 = a[4 * layer + 1:4 * layer + 2] == expert
                hits.append(jnp.logical_or(hit0, hit1).astype(F32))
                gater[(layer * N_EP + s) * 2 + e] = (jnp.where(hit0, a[4 * layer + 2:4 * layer + 3], 0.0)
                                                     + jnp.where(hit1, a[4 * layer + 3:4 * layer + 4], 0.0))
    stack = jnp.concatenate(hits, axis=0)
    ranks = jnp.where(stack > 0.5, nt(stack.astype(BF16), tri[...]), -1.0)
    for n in range(4 * N_EP):
        posr[n] = ranks[n:n + 1]

    for copy in w_copies:
        copy.wait()

    slot = lax.broadcasted_iota(jnp.int32, (CAP, n_tok), 0).astype(F32)
    slot_lane = lax.broadcasted_iota(jnp.int32, (n_tok, CAP), 1).astype(F32)
    step = 32

    def select(layer, s):
        at = (layer * N_EP + s) * 2
        return [posr[at + e] == slot for e in range(2)]

    def as_bf16(picks):
        return jnp.concatenate([p.astype(F32).astype(BF16) for p in picks], axis=0)

    def take_rows(layer, s, n, pick):
        u = ag[n, s]
        if n == 1:
            u = (u.astype(F32) + nn(u, dense2[...])).astype(BF16)
        rows = nn(pick, u).astype(BF16)
        for e in range(2):
            rows_in[layer, e, s] = rows[e * CAP:(e + 1) * CAP]

    def up_project(layer, s, e):
        rows = rows_in[layer, e, s]
        t_a[e] = nn(rows, w_gate[layer, e])
        t_b[e] = nn(rows, w_up[layer, e])

    def forward(s):
        take_rows(0, s, 0, as_bf16(select(0, s)))
        for e in range(2):
            up_project(0, s, e)
        for e in range(2):
            for i in range(CAP // step):
                r = pl.ds(i * step, step)
                a = t_a[e, r, :]
                hid[e, s, r, :] = (a * jax.nn.sigmoid(a) * t_b[e, r, :]).astype(BF16)
            ret[0, ret_at(s), e * CAP:(e + 1) * CAP] = nn(hid[e, s], w_down[0, e]).astype(BF16)

    def backward(layer, s, n_dy, n_ret, n_u):
        picks = select(layer, s)
        pick = as_bf16(picks)
        at = (layer * N_EP + s) * 2
        if n_u is not None:
            take_rows(layer, s, n_u, pick)
        got = nn(pick, ag[n_dy, s])
        for e in range(2):
            gate = jnp.sum(jnp.where(picks[e], gater[at + e], 0.0), axis=1, keepdims=True)
            g_out[e, s] = (got[e * CAP:(e + 1) * CAP] * gate).astype(BF16)
        for e in range(2):
            up_project(layer, s, e)
            t_gh[e] = nt(g_out[e, s], w_down[layer, e]).astype(BF16)
        parts = []
        for e in range(2):
            for i in range(CAP // step):
                r = pl.ds(i * step, step)
                a = t_a[e, r, :]
                b = t_b[e, r, :]
                gh = t_gh[e, r, :].astype(F32)
                sig = jax.nn.sigmoid(a)
                act = a * sig
                hid[e, s, r, :] = (act * b).astype(BF16)
                g_a[e, s, r, :] = (gh * b * sig * (1.0 + a * (1.0 - sig))).astype(BF16)
                g_b[e, s, r, :] = (gh * act).astype(BF16)
            parts.append((nt(g_a[e, s], w_gate[layer, e]) + nt(g_b[e, s], w_up[layer, e])).astype(BF16))
        ret[n_ret, ret_at(s)] = tn(pick, jnp.concatenate(parts, axis=0)).astype(BF16)

    def mix(p, base):
        acc[...] = base.astype(F32)

        def body(k, carry):
            s = order(k)

            @pl.when(k > 0)
            def _():
                ret_wait(0, p, s)

            for e in range(2):
                here = lane == s * 2 + e
                pos = jnp.sum(jnp.where(here, posc[p], 0.0), axis=1, keepdims=True)
                weight = jnp.sum(jnp.where(here, gatec[p], 0.0), axis=1, keepdims=True)
                hot = (pos == slot_lane).astype(F32).astype(BF16)
                acc[...] += nn(hot, ret[0, N_EP + p * N_EP + s, e * CAP:(e + 1) * CAP]) * weight
            return carry
        lax.fori_loop(0, N_EP, body, 0)
        return acc[...].astype(BF16)

    def add_up(n, p, base):
        total = base.astype(F32) + ret[n, N_EP + p * N_EP + z].astype(F32)
        for k in range(1, N_EP):
            ret_wait(n, p, order(k))
            total += ret[n, N_EP + p * N_EP + order(k)].astype(F32)
        return total.astype(BF16)

    chip_x = chip % 2
    chip_y = chip // 2
    over_x = chip + 1 - 2 * chip_x
    over_y = (chip + 2) % n_chip

    def group(e):
        return jnp.where(e == 0, chip_x, chip_y)

    def place(e):
        return jnp.where(e == 0, chip_y, chip_x)

    def pair_copy(layer, e):
        return row_copy(gs.at[1 - core, e], gr.at[layer, e], pair_send.at[layer, e], pair_recv.at[layer, e], chip * 2 + 1 - core)

    def one_copy(layer, e):
        return row_copy(gr.at[layer, e, 1 - group(e)], g2.at[layer, e], one_send.at[layer, e], one_recv.at[layer, e],
                        jnp.where(e == 0, over_x, over_y) * 2 + core)

    def two_copy(layer, e):
        return row_copy(gr.at[layer, e, group(e), 1 - place(e)], g3.at[layer, e], two_send.at[layer, e], two_recv.at[layer, e],
                        jnp.where(e == 0, over_y, over_x) * 2 + core)

    def pair_finish(layer, e):
        pair_copy(layer, e).wait()

        def body(q, carry):
            for g in range(2):
                for p in range(2):
                    gr[layer, e, g, p, q] = (gr[layer, e, g, p, q].astype(F32) + gs[core, e, g, p, q].astype(F32)).astype(BF16)
            return carry
        lax.fori_loop(0, 3, body, 0)
        one_copy(layer, e).start()

    def one_finish(layer):
        def body(e, carry):
            one_copy(layer, e).wait_recv()
            for p in range(2):
                for q in range(3):
                    gr[layer, e, group(e), p, q] = (gr[layer, e, group(e), p, q].astype(F32) + g2[layer, e, p, q].astype(F32)).astype(BF16)
            two_copy(layer, e).start()
            return carry
        lax.fori_loop(0, 2, body, 0)

    def two_finish(layer):
        def body(e, carry):
            two_copy(layer, e).wait_recv()
            for q in range(3):
                exp_v[layer, q * 2 + e] = (gr[layer, e, group(e), place(e), q].astype(F32) + g3[layer, e, q].astype(F32)).astype(BF16)
            one_copy(layer, e).wait_send()
            two_copy(layer, e).wait_send()
            return carry
        lax.fori_loop(0, 2, body, 0)
        exp_copy(layer).start()

    def exp_copy(layer):
        return pltpu.make_async_copy(exp_v.at[layer], exp_out.at[layer], out_sem.at[layer])

    def operands(layer, e, at, n):
        rows = rows_in[layer, e, pl.ds(at, n)].reshape(n * CAP, d_model)
        outs = g_out[e, pl.ds(at, n)].reshape(n * CAP, d_model)
        for q, (left, right) in enumerate(((outs, hid), (rows, g_a), (rows, g_b))):
            yield q, (q + 2) % 3, left, right[e, pl.ds(at, n)].reshape(n * CAP, d_ff)

    def weight_part(layer, at, n):
        def body(e, carry):
            for q, j, left, right in operands(layer, e, at, n):
                part[e, q] = tn(left, right)
            return carry
        lax.fori_loop(0, 2, body, 0)

    def weight_grads(layer, at, n, add):
        def body(e, carry):
            for q, j, left, right in operands(layer, e, at, n):
                grad = tn(left, right)
                if add:
                    grad = grad + part[e, q]
                for p in range(n_dp):
                    y, x = p // 4, p // 2 % 2
                    gs[p % 2, e, jnp.where(e == 0, x, y), jnp.where(e == 0, y, x), j] = grad[p * piece:(p + 1) * piece].astype(BF16)
            pair_copy(layer, e).start()
            return carry
        lax.fori_loop(0, 2, body, 0)
        pair_finish(layer, 0)
        pair_finish(layer, 1)

    sub = piece // N_EP

    def da_copy(layer, k):
        to = (z + k) % N_EP
        return col_copy(d_send.at[layer, to], d_a.at[layer, z], da_send.at[layer, k], da_recv.at[layer, z], to)

    def db_copy(layer, k):
        to = (dp + k) % n_dp
        return row_copy(d_bs.at[layer, to], d_b.at[layer, dp], db_send.at[layer, k], db_recv.at[layer, dp], to)

    def dense_start(layer, grad):
        for q in range(N_EP):
            for p in range(n_dp):
                at = p * piece + q * sub
                d_send[layer, q, p] = grad[at:at + sub].astype(BF16)
        for k in range(1, N_EP):
            da_copy(layer, k).start()
        d_a[layer, z] = d_send[layer, z]

    def dense_middle(layer):
        for m in (1, 2):
            @pl.when(z != m)
            def _():
                col_copy(d_send.at[layer, m], d_a.at[layer, m], da_send.at[layer, 0], da_recv.at[layer, m], m).wait_recv()
        d_bs[layer] = (d_a[layer, 1].astype(F32) + d_a[layer, 2].astype(F32)).astype(BF16)
        for k in range(1, n_dp):
            db_copy(layer, k).start()

    def dense_end(layer):
        total = d_bs[layer, dp].astype(F32)
        for k in range(1, n_dp):
            frm = (dp + k) % n_dp
            row_copy(d_bs.at[layer, frm], d_b.at[layer, frm], db_send.at[layer, k], db_recv.at[layer, frm], frm).wait_recv()
            total += d_b[layer, frm].astype(F32)
        den_v[layer * sub:(layer + 1) * sub] = total.astype(BF16)
        @pl.when(inner)
        def _():
            for k in range(1, N_EP):
                da_copy(layer, k).wait_send()
        for k in range(1, n_dp):
            db_copy(layer, k).wait_send()

    def forward_step(k, carry):
        s = order(k)
        ag_step(0, k)
        with scope('f1'):
            forward(s)
        ret_start(0, s)
        return carry
    lax.fori_loop(0, N_EP, forward_step, 0)

    ag_pass(2, z, right=z != 1, left=z != 2)

    @pl.when(outer)
    def _():
        x_copy().start()

    @pl.when(inner)
    def _():
        def body(n, carry):
            s = jnp.where(n == 0, z, near_end)
            ag[1, s] = mix(s % 2, ag[0, s])
            ag_pass(1, s)

            @pl.when(n == 1)
            def _():
                with scope('dyw'):
                    ag_to_right(2, s).wait_recv()
            ag_pass(2, s, right=z == 1, left=z == 2)
            return carry
        lax.fori_loop(0, 2, body, 0)

    def second_step(k, carry):
        s = order_owned(k)

        @pl.when(jnp.logical_or(k > 1, jnp.logical_and(outer, s != z)))
        def _():
            ag_take(2, s)
        owned_step(1, k, s)
        with scope('fb2'):
            backward(1, s, 2, 1, 1)
        ret_start(1, s)
        return carry
    lax.fori_loop(0, N_EP, second_step, 0)
    with scope('wg1'):
        weight_grads(1, 0, N_EP, False)

    @pl.when(inner)
    def _():
        def body(n, carry):
            s = jnp.where(n == 0, z, near_end)
            gm = add_up(1, s % 2, ag[2, s])
            g_mix[n] = gm
            ag[3, s] = (gm.astype(F32) + nt(gm, dense2[...])).astype(BF16)
            ag_pass(3, s)
            return carry
        lax.fori_loop(0, 2, body, 0)
        dense_start(1, tn(ag[1, z], g_mix[0]) + tn(ag[1, near_end], g_mix[1]))

    three = jnp.where(z < 2, 0, 1)
    last = jnp.where(z < 2, 3, 0)

    def first_step(k, carry):
        s = order_owned(k)

        @pl.when(k == 2)
        def _():
            with scope('dmid1'):
                dense_middle(1)
            with scope('one1'):
                one_finish(1)

        @pl.when(jnp.logical_and(k == 3, outer))
        def _():
            with scope('wpart'):
                weight_part(0, three, 3)
        owned_step(3, k, s)
        with scope('b1'):
            backward(0, s, 3, 2, None)
        ret_start(2, s)
        return carry
    lax.fori_loop(0, N_EP, first_step, 0)

    @pl.when(inner)
    def _():
        weight_part(0, three, 3)
    with scope('wg0'):
        weight_grads(0, last, 1, True)
    with scope('two1'):
        two_finish(1)
    with scope('dend1'):
        dense_end(1)

    def dx_copy():
        return pltpu.make_async_copy(dx_v, tok_out.at[pl.ds(0, n_tok)], out_sem.at[2])

    @pl.when(inner)
    def _():
        gm = add_up(2, z % 2, ag[3, z])
        dx_v[...] = (gm.astype(F32) + nt(gm, dense1[...])).astype(BF16)
        dx_copy().start()
        ge = add_up(2, near_end % 2, ag[3, near_end])
        g_mix[0] = (ge.astype(F32) + nt(ge, dense1[...])).astype(BF16)
        dx_back().start()
        x_copy().wait_recv()
        dense_start(0, tn(x_ref[...], gm) + tn(x_end[...], ge))
    with scope('one0'):
        one_finish(0)
    with scope('dmid0'):
        dense_middle(0)
    with scope('two0'):
        two_finish(0)

    @pl.when(outer)
    def _():
        with scope('dxw'):
            dx_back().wait_recv()
        dx_copy().start()
        x_copy().wait_send()
    with scope('dend0'):
        dense_end(0)
    den_copy = pltpu.make_async_copy(den_v, tok_out.at[pl.ds(n_tok, 2 * sub)], out_sem.at[3])
    den_copy.start()
    for n in range(4):
        ag_drain(n)
    for n in range(3):
        ret_drain(n)

    @pl.when(inner)
    def _():
        dx_back().wait_send()
    for k in range(1, N_EP):
        aux_copy(k).wait_send()
    exp_copy(1).wait()
    exp_copy(0).wait()
    dx_copy().wait()
    den_copy.wait()


def solution(mesh):
    n_dp = mesh.shape['dp']
    n_chip = n_dp // 2
    tok_spec = P(('dp', 'ep'), None)
    exp_spec = P('ep', None, None)
    layer_specs = (P(None, None), tok_spec, tok_spec, exp_spec, exp_spec, exp_spec)
    grad_specs = (P(('dp', 'ep'), None), P('ep', 'dp', None), P('ep', 'dp', None), P('ep', None, 'dp'))

    def local_step(tokens, dy_out, dense_w1, idx1, gate1, wg1, wu1, wd1, dense_w2, idx2, gate2, wg2, wu2, wd2):
        n_tok, d_model = tokens.shape
        d_ff = wg1.shape[2]
        piece = d_model // n_dp
        sub = piece // N_EP
        vmem = pl.BlockSpec(memory_space=pltpu.VMEM)
        hbm = pl.BlockSpec(memory_space=pl.ANY)
        dma = pltpu.SemaphoreType.DMA
        outs = pl.pallas_call(
            functools.partial(kernel, n_dp),
            out_shape=(jax.ShapeDtypeStruct((n_tok + 2 * sub, d_model), BF16), jax.ShapeDtypeStruct((2, 6, piece, d_ff), BF16)),
            in_specs=[vmem] * 8 + [hbm] * 6,
            out_specs=[hbm] * 2,
            scratch_shapes=[
                pltpu.VMEM((2, 2, d_model, d_ff), BF16), pltpu.VMEM((2, 2, d_model, d_ff), BF16), pltpu.VMEM((2, 2, d_ff, d_model), BF16),
                pltpu.VMEM((8, n_tok), F32), pltpu.VMEM((N_EP, 8, n_tok), F32), pltpu.VMEM((4 * N_EP, 1, n_tok), F32), pltpu.VMEM((4 * N_EP, 1, n_tok), F32),
                pltpu.VMEM((2, n_tok, N_EXP), F32), pltpu.VMEM((2, n_tok, N_EXP), F32), pltpu.VMEM((n_tok, n_tok), BF16),
                pltpu.VMEM((4, N_EP, n_tok, d_model), BF16), pltpu.VMEM((3, 3 * N_EP, n_tok, d_model), BF16),
                pltpu.VMEM((n_tok, d_model), BF16),
                pltpu.VMEM((2, 2, N_EP, CAP, d_model), BF16), pltpu.VMEM((2, CAP, d_ff), F32), pltpu.VMEM((2, CAP, d_ff), F32),
                pltpu.VMEM((2, CAP, d_ff), BF16), pltpu.VMEM((2, N_EP, CAP, d_ff), BF16), pltpu.VMEM((2, N_EP, CAP, d_ff), BF16),
                pltpu.VMEM((2, N_EP, CAP, d_ff), BF16), pltpu.VMEM((2, N_EP, CAP, d_model), BF16),
                pltpu.VMEM((n_tok, d_model), F32), pltpu.VMEM((2, n_tok, d_model), BF16),
                pltpu.VMEM((2, 3, d_model, d_ff), F32),
                pltpu.VMEM((2, 2, 2, 2, 3, piece, d_ff), BF16), pltpu.VMEM((2, 2, 2, 2, 3, piece, d_ff), BF16),
                pltpu.VMEM((2, 2, 2, 3, piece, d_ff), BF16), pltpu.VMEM((2, 2, 3, piece, d_ff), BF16),
                pltpu.VMEM((2, N_EP, n_dp, sub, d_model), BF16), pltpu.VMEM((2, N_EP, n_dp, sub, d_model), BF16),
                pltpu.VMEM((2, n_dp, sub, d_model), BF16), pltpu.VMEM((2, n_dp, sub, d_model), BF16),
                pltpu.VMEM((2, 6, piece, d_ff), BF16), pltpu.VMEM((n_tok, d_model), BF16), pltpu.VMEM((2 * sub, d_model), BF16),
                dma((6,)), dma((N_EP,)), dma((N_EP,)), dma((4, N_EP)), dma((4, N_EP)), dma((4, N_EP)), dma((3, N_EP)), dma((3, 2 * N_EP)),
                dma((2,)), dma((2,)), dma((2, 2)), dma((2, 2)), dma((2, 2)), dma((2, 2)), dma((2, 2)), dma((2, 2)),
                dma((2, N_EP)), dma((2, N_EP)), dma((2, n_dp)), dma((2, n_dp)), dma((4,)),
            ],
            compiler_params=pltpu.CompilerParams(collective_id=0, has_side_effects=True, vmem_limit_bytes=67043328),
        )(tokens, dy_out, dense_w1, dense_w2, idx1.T, gate1.T, idx2.T, gate2.T, wg1, wu1, wd1, wg2, wu2, wd2)
        tok, exp = outs
        res = [tok[:n_tok]]
        for layer in range(2):
            res += [tok[n_tok + layer * sub:n_tok + (layer + 1) * sub], exp[layer, 0:2], exp[layer, 2:4], jnp.swapaxes(exp[layer, 4:6], 1, 2)]
        return tuple(res)

    return jax.shard_map(local_step, mesh=mesh, in_specs=(tok_spec, tok_spec) + layer_specs + layer_specs,
                         out_specs=(tok_spec,) + grad_specs + grad_specs, check_vma=False)
```

```python
import functools

import jax
import jax.numpy as jnp
from jax import lax
from jax.experimental import pallas as pl
from jax.experimental.pallas import tpu as pltpu
from jax.sharding import PartitionSpec as P

MESH = pl.DeviceIdType.MESH
F32, BF16 = jnp.float32, jnp.bfloat16
N_EP = 4
scope = jax.named_scope
N_EXP = 8
CAP = 256


def nn(a, b):
    return lax.dot_general(a, b, (((1,), (0,)), ((), ())), preferred_element_type=F32)


def nt(a, b):
    return lax.dot_general(a, b, (((1,), (1,)), ((), ())), preferred_element_type=F32)


def tn(a, b):
    return lax.dot_general(a, b, (((0,), (0,)), ((), ())), preferred_element_type=F32)


def kernel(n_dp, x_ref, dy_ref, dense1, dense2, idx1, gate1, idx2, gate2,
           wg1_hbm, wu1_hbm, wd1_hbm, wg2_hbm, wu2_hbm, wd2_hbm,
           tok_out, exp_out,
           w_gate, w_up, w_down, auxs, auxb, posr, gater, posc, gatec, tri, ag, ret, x_end, rows_in, t_a, t_b, t_gh, hid, g_a, g_b, g_out,
           acc, g_mix, part, gs, gr, g2, g3, d_send, d_a, d_bs, d_b, exp_v, dx_v, den_v,
           w_sem, aux_send, aux_recv, ag_right, ag_left, ag_recv, ret_send, ret_recv, end_send, end_recv, pair_send, pair_recv,
           one_send, one_recv, two_send, two_recv, da_send, da_recv, db_send, db_recv, out_sem):
    z = lax.axis_index('ep')
    dp = lax.axis_index('dp')
    n_chip = n_dp // 2
    core = dp % 2
    chip = dp // 2
    n_tok, d_model = x_ref.shape
    d_ff = t_a.shape[2]
    piece = d_model // n_dp

    def order(k):
        near_low = jnp.where(z == 1, jnp.where(k == 0, 1, jnp.where(k == 1, 0, k)), k)
        near_high = 3 - jnp.where(z == 2, jnp.where(k == 0, 1, jnp.where(k == 1, 0, k)), k)
        return jnp.where(z < 2, near_low, near_high)

    def order_owned(k):
        low = jnp.where(k == 0, 1, jnp.where(k == 1, 0, k))
        return jnp.where(z < 2, low, 3 - low)

    def owner(s):
        return jnp.where(s < 2, 1, 2)

    inner = jnp.logical_or(z == 1, z == 2)
    outer = jnp.logical_not(inner)
    near_mid = jnp.where(z < 2, 1, 2)
    near_end = jnp.where(z < 2, 0, 3)

    barrier = pltpu.get_barrier_semaphore()
    for k in range(1, N_EP):
        pl.semaphore_signal(barrier, inc=1, device_id={'ep': (z + k) % N_EP, 'dp': dp}, device_id_type=MESH)
    for k in range(1, n_dp):
        pl.semaphore_signal(barrier, inc=1, device_id={'ep': z, 'dp': (dp + k) % n_dp}, device_id_type=MESH)

    w_copies = []
    for n, (hbm, dst) in enumerate(((wg1_hbm, w_gate.at[0]), (wu1_hbm, w_up.at[0]), (wd1_hbm, w_down.at[0]),
                                    (wg2_hbm, w_gate.at[1]), (wu2_hbm, w_up.at[1]), (wd2_hbm, w_down.at[1]))):
        w_copies.append(pltpu.make_async_copy(hbm, dst, w_sem.at[n]))
        w_copies[-1].start()

    auxs[0:2] = idx1[...].astype(F32)
    auxs[2:4] = gate1[...]
    auxs[4:6] = idx2[...].astype(F32)
    auxs[6:8] = gate2[...]
    x = x_ref[...]
    ag[0, z] = (x.astype(F32) + nn(x, dense1[...])).astype(BF16)
    ag[2, z] = dy_ref[...]
    auxb[z] = auxs[...]

    with scope('barrier'):
        pl.semaphore_wait(barrier, N_EP - 1 + n_dp - 1)

    def col_copy(src, dst, send, recv, to):
        return pltpu.make_async_remote_copy(src_ref=src, dst_ref=dst, send_sem=send, recv_sem=recv,
                                            device_id={'ep': to, 'dp': dp}, device_id_type=MESH)

    def row_copy(src, dst, send, recv, to):
        return pltpu.make_async_remote_copy(src_ref=src, dst_ref=dst, send_sem=send, recv_sem=recv,
                                            device_id={'ep': z, 'dp': to}, device_id_type=MESH)

    def aux_copy(k):
        return col_copy(auxs, auxb.at[z], aux_send.at[k], aux_recv.at[z], (z + k) % N_EP)

    for k in range(1, N_EP):
        aux_copy(k).start()

    def ag_to_right(n, s):
        return col_copy(ag.at[n, s], ag.at[n, s], ag_right.at[n, s], ag_recv.at[n, s], jnp.minimum(z + 1, N_EP - 1))

    def ag_to_left(n, s):
        return col_copy(ag.at[n, s], ag.at[n, s], ag_left.at[n, s], ag_recv.at[n, s], jnp.maximum(z - 1, 0))

    def rightward(n, s):
        return jnp.logical_and((owner(s) if n % 2 else s) <= z, z < N_EP - 1)

    def leftward(n, s):
        return jnp.logical_and((owner(s) if n % 2 else s) >= z, z > 0)

    def ag_pass(n, s, right=True, left=True):
        if right is not False:
            @pl.when(jnp.logical_and(rightward(n, s), right))
            def _():
                ag_to_right(n, s).start()

        if left is not False:
            @pl.when(jnp.logical_and(leftward(n, s), left))
            def _():
                ag_to_left(n, s).start()

    def ag_take(n, s):
        with scope('agw%d' % n):
            ag_to_right(n, s).wait_recv()
        ag_pass(n, s)

    def ag_step(n, k):
        @pl.when(k == 1)
        def _():
            ag_take(n, order(1))

        @pl.when(jnp.logical_or(jnp.logical_and(k == 1, inner), jnp.logical_and(k == 2, outer)))
        def _():
            ag_take(n, order(2))

        @pl.when(k == 3)
        def _():
            ag_take(n, order(3))

    def owned_step(n, k, s, early):
        if early:
            @pl.when(jnp.logical_and(k == 0, inner))
            def _():
                ag_take(n, order_owned(2))

        @pl.when(jnp.logical_or(k > (2 if early else 1), outer))
        def _():
            ag_take(n, s)

    def ag_drain(n):
        def body(s, carry):
            @pl.when(rightward(n, s))
            def _():
                ag_to_right(n, s).wait_send()

            @pl.when(leftward(n, s))
            def _():
                ag_to_left(n, s).wait_send()
            return carry
        lax.fori_loop(0, N_EP, body, 0)

    def ret_at(s):
        return jnp.where(owner(s) == z, N_EP + s % 2 * N_EP + z, s)

    def ret_copy(n, s):
        return col_copy(ret.at[n, s], ret.at[n, N_EP + s % 2 * N_EP + z], ret_send.at[n, s], ret_recv.at[n, s % 2 * N_EP + z], owner(s))

    def ret_start(n, s):
        @pl.when(owner(s) != z)
        def _():
            ret_copy(n, s).start()

    def ret_wait(n, p, frm):
        with scope('retw%d' % n):
            at = p * N_EP + frm
            col_copy(ret.at[n, 0], ret.at[n, N_EP + at], ret_send.at[n, 0], ret_recv.at[n, at], z).wait_recv()

    def ret_drain(n):
        def body(s, carry):
            @pl.when(owner(s) != z)
            def _():
                ret_copy(n, s).wait_send()
            return carry
        lax.fori_loop(0, N_EP, body, 0)

    def x_copy():
        return col_copy(x_ref, x_end, end_send.at[0], end_recv.at[0], near_mid)

    def dx_back():
        return col_copy(g_mix.at[0], dx_v, end_send.at[1], end_recv.at[1], near_end)

    ag_pass(0, z)

    r_io = lax.broadcasted_iota(jnp.int32, (n_tok, n_tok), 0)
    c_io = lax.broadcasted_iota(jnp.int32, (n_tok, n_tok), 1)
    tri[...] = (c_io < r_io).astype(F32).astype(BF16)
    lane = lax.broadcasted_iota(jnp.int32, (n_tok, N_EXP), 1)
    for k in range(1, N_EP):
        s = (z + k) % N_EP
        col_copy(auxs, auxb.at[s], aux_send.at[k], aux_recv.at[s], s).wait_recv()
    for p in range(2):
        cols = auxb[jnp.where(z < 2, 0, 2) + p].T
        hit0 = cols[:, 0:1] == lane.astype(F32)
        hit1 = cols[:, 1:2] == lane.astype(F32)
        hit = jnp.logical_or(hit0, hit1)
        rank = nn(tri[...], hit.astype(F32).astype(BF16))
        posc[p] = jnp.where(hit, rank, -1.0)
        gatec[p] = jnp.where(hit0, cols[:, 2:3], 0.0) + jnp.where(hit1, cols[:, 3:4], 0.0)
    hits = []
    for layer in range(2):
        for s in range(N_EP):
            for e in range(2):
                a = auxb[s]
                expert = (z * 2 + e).astype(F32)
                hit0 = a[4 * layer:4 * layer + 1] == expert
                hit1 = a[4 * layer + 1:4 * layer + 2] == expert
                hits.append(jnp.logical_or(hit0, hit1).astype(F32))
                gater[(layer * N_EP + s) * 2 + e] = (jnp.where(hit0, a[4 * layer + 2:4 * layer + 3], 0.0)
                                                     + jnp.where(hit1, a[4 * layer + 3:4 * layer + 4], 0.0))
    stack = jnp.concatenate(hits, axis=0)
    ranks = jnp.where(stack > 0.5, nt(stack.astype(BF16), tri[...]), -1.0)
    for n in range(4 * N_EP):
        posr[n] = ranks[n:n + 1]

    for copy in w_copies:
        copy.wait()

    slot = lax.broadcasted_iota(jnp.int32, (CAP, n_tok), 0).astype(F32)
    slot_lane = lax.broadcasted_iota(jnp.int32, (n_tok, CAP), 1).astype(F32)
    step = 32

    def select(layer, s):
        at = (layer * N_EP + s) * 2
        return [posr[at + e] == slot for e in range(2)]

    def as_bf16(picks):
        return jnp.concatenate([p.astype(F32).astype(BF16) for p in picks], axis=0)

    def take_rows(layer, s, n, pick):
        u = ag[n, s]
        if n == 1:
            u = (u.astype(F32) + nn(u, dense2[...])).astype(BF16)
        rows = nn(pick, u).astype(BF16)
        for e in range(2):
            rows_in[layer, e, s] = rows[e * CAP:(e + 1) * CAP]

    def up_project(layer, s, e):
        rows = rows_in[layer, e, s]
        t_a[e] = nn(rows, w_gate[layer, e])
        t_b[e] = nn(rows, w_up[layer, e])

    def forward(s):
        take_rows(0, s, 0, as_bf16(select(0, s)))
        for e in range(2):
            up_project(0, s, e)
        for e in range(2):
            for i in range(CAP // step):
                r = pl.ds(i * step, step)
                a = t_a[e, r, :]
                hid[e, s, r, :] = (a * jax.nn.sigmoid(a) * t_b[e, r, :]).astype(BF16)
            ret[0, ret_at(s), e * CAP:(e + 1) * CAP] = nn(hid[e, s], w_down[0, e]).astype(BF16)

    def backward(layer, s, n_dy, n_ret, n_u):
        picks = select(layer, s)
        pick = as_bf16(picks)
        at = (layer * N_EP + s) * 2
        if n_u is not None:
            take_rows(layer, s, n_u, pick)
        got = nn(pick, ag[n_dy, s])
        for e in range(2):
            gate = jnp.sum(jnp.where(picks[e], gater[at + e], 0.0), axis=1, keepdims=True)
            g_out[e, s] = (got[e * CAP:(e + 1) * CAP] * gate).astype(BF16)
        for e in range(2):
            up_project(layer, s, e)
            t_gh[e] = nt(g_out[e, s], w_down[layer, e]).astype(BF16)
        parts = []
        for e in range(2):
            for i in range(CAP // step):
                r = pl.ds(i * step, step)
                a = t_a[e, r, :]
                b = t_b[e, r, :]
                gh = t_gh[e, r, :].astype(F32)
                sig = jax.nn.sigmoid(a)
                act = a * sig
                hid[e, s, r, :] = (act * b).astype(BF16)
                g_a[e, s, r, :] = (gh * b * sig * (1.0 + a * (1.0 - sig))).astype(BF16)
                g_b[e, s, r, :] = (gh * act).astype(BF16)
            parts.append((nt(g_a[e, s], w_gate[layer, e]) + nt(g_b[e, s], w_up[layer, e])).astype(BF16))
        ret[n_ret, ret_at(s)] = tn(pick, jnp.concatenate(parts, axis=0)).astype(BF16)

    def mix(p, base):
        acc[...] = base.astype(F32)

        def body(k, carry):
            s = order(k)

            @pl.when(k > 0)
            def _():
                ret_wait(0, p, s)

            for e in range(2):
                here = lane == s * 2 + e
                pos = jnp.sum(jnp.where(here, posc[p], 0.0), axis=1, keepdims=True)
                weight = jnp.sum(jnp.where(here, gatec[p], 0.0), axis=1, keepdims=True)
                hot = (pos == slot_lane).astype(F32).astype(BF16)
                acc[...] += nn(hot, ret[0, N_EP + p * N_EP + s, e * CAP:(e + 1) * CAP]) * weight
            return carry
        lax.fori_loop(0, N_EP, body, 0)
        return acc[...].astype(BF16)

    def add_up(n, p, base):
        total = base.astype(F32) + ret[n, N_EP + p * N_EP + z].astype(F32)
        for k in range(1, N_EP):
            ret_wait(n, p, order(k))
            total += ret[n, N_EP + p * N_EP + order(k)].astype(F32)
        return total.astype(BF16)

    chip_x = chip % 2
    chip_y = chip // 2
    over_x = chip + 1 - 2 * chip_x
    over_y = (chip + 2) % n_chip

    def group(e):
        return jnp.where(e == 0, chip_x, chip_y)

    def place(e):
        return jnp.where(e == 0, chip_y, chip_x)

    def pair_copy(layer, e, q):
        return row_copy(gs.at[1 - core, e, q], gr.at[layer, e, q], pair_send.at[layer, e, q], pair_recv.at[layer, e, q], chip * 2 + 1 - core)

    def one_copy(layer, e, q):
        return row_copy(gr.at[layer, e, q, 1 - group(e)], g2.at[layer, e, q], one_send.at[layer, e, q], one_recv.at[layer, e, q],
                        jnp.where(e == 0, over_x, over_y) * 2 + core)

    def two_copy(layer, e, q):
        return row_copy(gr.at[layer, e, q, group(e), 1 - place(e)], g3.at[layer, e, q], two_send.at[layer, e, q], two_recv.at[layer, e, q],
                        jnp.where(e == 0, over_y, over_x) * 2 + core)

    def pair_finish(layer, e, q):
        pair_copy(layer, e, q).wait()
        for g in range(2):
            for p in range(2):
                gr[layer, e, q, g, p] = (gr[layer, e, q, g, p].astype(F32) + gs[core, e, q, g, p].astype(F32)).astype(BF16)
        one_copy(layer, e, q).start()

    def one_finish(layer):
        def body(n, carry):
            e, q = n % 2, (n // 2 + 2) % 3
            one_copy(layer, e, q).wait_recv()
            for p in range(2):
                gr[layer, e, q, group(e), p] = (gr[layer, e, q, group(e), p].astype(F32) + g2[layer, e, q, p].astype(F32)).astype(BF16)
            two_copy(layer, e, q).start()
            return carry
        lax.fori_loop(0, 6, body, 0)

    def two_finish(layer):
        def body(n, carry):
            e, q = n % 2, (n // 2 + 2) % 3
            two_copy(layer, e, q).wait_recv()
            exp_v[layer, q * 2 + e] = (gr[layer, e, q, group(e), place(e)].astype(F32) + g3[layer, e, q].astype(F32)).astype(BF16)
            one_copy(layer, e, q).wait_send()
            two_copy(layer, e, q).wait_send()
            return carry
        lax.fori_loop(0, 6, body, 0)
        exp_copy(layer).start()

    def exp_copy(layer):
        return pltpu.make_async_copy(exp_v.at[layer], exp_out.at[layer], out_sem.at[layer])

    def operands(layer, e, at, n):
        rows = rows_in[layer, e, pl.ds(at, n)].reshape(n * CAP, d_model)
        outs = g_out[e, pl.ds(at, n)].reshape(n * CAP, d_model)
        return [(j, left, right[e, pl.ds(at, n)].reshape(n * CAP, d_ff))
                for j, left, right in ((2, outs, hid), (0, rows, g_a), (1, rows, g_b))]

    def weight_part(layer, at, n):
        def body(e, carry):
            for j, left, right in operands(layer, e, at, n):
                part[e, j] = tn(left, right)
            return carry
        lax.fori_loop(0, 2, body, 0)

    def split_grad(layer, e, j, grad):
        for p in range(n_dp):
            y, x = p // 4, p // 2 % 2
            gs[p % 2, e, j, jnp.where(e == 0, x, y), jnp.where(e == 0, y, x)] = grad[p * piece:(p + 1) * piece].astype(BF16)
        pair_copy(layer, e, j).start()

    def weight_grads(layer):
        def body(e, carry):
            for j, left, right in operands(layer, e, 0, N_EP):
                split_grad(layer, e, j, tn(left, right))
            return carry
        lax.fori_loop(0, 2, body, 0)
        for j in (2, 0, 1):
            for e in range(2):
                pair_finish(layer, e, j)

    def weight_rest(layer, at):
        both = [operands(layer, e, at, 1) for e in range(2)]
        todo = [(e, both[e][q]) for q in range(3) for e in range(2)]
        for k, (e, (j, left, right)) in enumerate(todo):
            split_grad(layer, e, j, tn(left, right) + part[e, j])
            if k >= 2:
                pair_finish(layer, todo[k - 2][0], todo[k - 2][1][0])
        for e, (j, _, _) in todo[4:]:
            pair_finish(layer, e, j)

    sub = piece // N_EP

    def da_copy(layer, k):
        to = (z + k) % N_EP
        return col_copy(d_send.at[layer, to], d_a.at[layer, z], da_send.at[layer, k], da_recv.at[layer, z], to)

    def db_copy(layer, k):
        to = (dp + k) % n_dp
        return row_copy(d_bs.at[layer, to], d_b.at[layer, dp], db_send.at[layer, k], db_recv.at[layer, dp], to)

    def dense_start(layer, grad):
        for q in range(N_EP):
            for p in range(n_dp):
                at = p * piece + q * sub
                d_send[layer, q, p] = grad[at:at + sub].astype(BF16)
        for k in range(1, N_EP):
            da_copy(layer, k).start()
        d_a[layer, z] = d_send[layer, z]

    def dense_middle(layer):
        for m in (1, 2):
            @pl.when(z != m)
            def _():
                col_copy(d_send.at[layer, m], d_a.at[layer, m], da_send.at[layer, 0], da_recv.at[layer, m], m).wait_recv()
        d_bs[layer] = (d_a[layer, 1].astype(F32) + d_a[layer, 2].astype(F32)).astype(BF16)
        for k in range(1, n_dp):
            db_copy(layer, k).start()

    def dense_end(layer):
        total = d_bs[layer, dp].astype(F32)
        for k in range(1, n_dp):
            frm = (dp + k) % n_dp
            row_copy(d_bs.at[layer, frm], d_b.at[layer, frm], db_send.at[layer, k], db_recv.at[layer, frm], frm).wait_recv()
            total += d_b[layer, frm].astype(F32)
        den_v[layer * sub:(layer + 1) * sub] = total.astype(BF16)
        @pl.when(inner)
        def _():
            for k in range(1, N_EP):
                da_copy(layer, k).wait_send()
        for k in range(1, n_dp):
            db_copy(layer, k).wait_send()

    def forward_step(k, carry):
        s = order(k)
        ag_step(0, k)
        with scope('f1'):
            forward(s)
        ret_start(0, s)
        return carry
    lax.fori_loop(0, N_EP, forward_step, 0)

    ag_pass(2, z, right=z != 1, left=z != 2)

    @pl.when(outer)
    def _():
        x_copy().start()

    @pl.when(inner)
    def _():
        def body(n, carry):
            s = jnp.where(n == 0, z, near_end)
            ag[1, s] = mix(s % 2, ag[0, s])
            ag_pass(1, s)

            @pl.when(n == 1)
            def _():
                with scope('dyw'):
                    ag_to_right(2, s).wait_recv()
            ag_pass(2, s, right=z == 1, left=z == 2)
            return carry
        lax.fori_loop(0, 2, body, 0)

    def second_step(k, carry):
        s = order_owned(k)

        owned_step(1, k, s, False)

        @pl.when(jnp.logical_or(k > 1, jnp.logical_and(outer, s != z)))
        def _():
            ag_take(2, s)
        with scope('fb2'):
            backward(1, s, 2, 1, 1)
        ret_start(1, s)
        return carry
    lax.fori_loop(0, N_EP, second_step, 0)
    with scope('wg1'):
        weight_grads(1)

    @pl.when(inner)
    def _():
        def body(n, carry):
            s = jnp.where(n == 0, z, near_end)
            gm = add_up(1, s % 2, ag[2, s])
            g_mix[n] = gm
            ag[3, s] = (gm.astype(F32) + nt(gm, dense2[...])).astype(BF16)
            ag_pass(3, s)
            return carry
        lax.fori_loop(0, 2, body, 0)
        dense_start(1, tn(ag[1, z], g_mix[0]) + tn(ag[1, near_end], g_mix[1]))

    three = jnp.where(z < 2, 0, 1)
    last = jnp.where(z < 2, 3, 0)

    def first_step(k, carry):
        s = order_owned(k)

        @pl.when(jnp.logical_and(k == 3, outer))
        def _():
            with scope('dmid1'):
                dense_middle(1)
            with scope('one1'):
                one_finish(1)
            with scope('wpart'):
                weight_part(0, three, 3)
        owned_step(3, k, s, True)
        with scope('b1'):
            backward(0, s, 3, 2, None)
        ret_start(2, s)
        return carry
    lax.fori_loop(0, N_EP, first_step, 0)

    @pl.when(inner)
    def _():
        dense_middle(1)
        one_finish(1)
        weight_part(0, three, 3)
    with scope('wg0'):
        weight_rest(0, last)
    with scope('one0'):
        one_finish(0)
    with scope('two1'):
        two_finish(1)
    with scope('dend1'):
        dense_end(1)

    def dx_copy():
        return pltpu.make_async_copy(dx_v, tok_out.at[pl.ds(0, n_tok)], out_sem.at[2])

    @pl.when(inner)
    def _():
        gm = add_up(2, z % 2, ag[3, z])
        dx_v[...] = (gm.astype(F32) + nt(gm, dense1[...])).astype(BF16)
        dx_copy().start()
        ge = add_up(2, near_end % 2, ag[3, near_end])
        g_mix[0] = (ge.astype(F32) + nt(ge, dense1[...])).astype(BF16)
        dx_back().start()
        x_copy().wait_recv()
        dense_start(0, tn(x_ref[...], gm) + tn(x_end[...], ge))
    with scope('dmid0'):
        dense_middle(0)
    with scope('two0'):
        two_finish(0)

    @pl.when(outer)
    def _():
        with scope('dxw'):
            dx_back().wait_recv()
        dx_copy().start()
        x_copy().wait_send()
    with scope('dend0'):
        dense_end(0)
    den_copy = pltpu.make_async_copy(den_v, tok_out.at[pl.ds(n_tok, 2 * sub)], out_sem.at[3])
    den_copy.start()
    for n in range(4):
        ag_drain(n)
    for n in range(3):
        ret_drain(n)

    @pl.when(inner)
    def _():
        dx_back().wait_send()
    for k in range(1, N_EP):
        aux_copy(k).wait_send()
    exp_copy(1).wait()
    exp_copy(0).wait()
    dx_copy().wait()
    den_copy.wait()


def solution(mesh):
    n_dp = mesh.shape['dp']
    n_chip = n_dp // 2
    tok_spec = P(('dp', 'ep'), None)
    exp_spec = P('ep', None, None)
    layer_specs = (P(None, None), tok_spec, tok_spec, exp_spec, exp_spec, exp_spec)
    grad_specs = (P(('dp', 'ep'), None), P('ep', 'dp', None), P('ep', 'dp', None), P('ep', None, 'dp'))

    def local_step(tokens, dy_out, dense_w1, idx1, gate1, wg1, wu1, wd1, dense_w2, idx2, gate2, wg2, wu2, wd2):
        n_tok, d_model = tokens.shape
        d_ff = wg1.shape[2]
        piece = d_model // n_dp
        sub = piece // N_EP
        vmem = pl.BlockSpec(memory_space=pltpu.VMEM)
        hbm = pl.BlockSpec(memory_space=pl.ANY)
        dma = pltpu.SemaphoreType.DMA
        outs = pl.pallas_call(
            functools.partial(kernel, n_dp),
            out_shape=(jax.ShapeDtypeStruct((n_tok + 2 * sub, d_model), BF16), jax.ShapeDtypeStruct((2, 6, piece, d_ff), BF16)),
            in_specs=[vmem] * 8 + [hbm] * 6,
            out_specs=[hbm] * 2,
            scratch_shapes=[
                pltpu.VMEM((2, 2, d_model, d_ff), BF16), pltpu.VMEM((2, 2, d_model, d_ff), BF16), pltpu.VMEM((2, 2, d_ff, d_model), BF16),
                pltpu.VMEM((8, n_tok), F32), pltpu.VMEM((N_EP, 8, n_tok), F32), pltpu.VMEM((4 * N_EP, 1, n_tok), F32), pltpu.VMEM((4 * N_EP, 1, n_tok), F32),
                pltpu.VMEM((2, n_tok, N_EXP), F32), pltpu.VMEM((2, n_tok, N_EXP), F32), pltpu.VMEM((n_tok, n_tok), BF16),
                pltpu.VMEM((4, N_EP, n_tok, d_model), BF16), pltpu.VMEM((3, 3 * N_EP, n_tok, d_model), BF16),
                pltpu.VMEM((n_tok, d_model), BF16),
                pltpu.VMEM((2, 2, N_EP, CAP, d_model), BF16), pltpu.VMEM((2, CAP, d_ff), F32), pltpu.VMEM((2, CAP, d_ff), F32),
                pltpu.VMEM((2, CAP, d_ff), BF16), pltpu.VMEM((2, N_EP, CAP, d_ff), BF16), pltpu.VMEM((2, N_EP, CAP, d_ff), BF16),
                pltpu.VMEM((2, N_EP, CAP, d_ff), BF16), pltpu.VMEM((2, N_EP, CAP, d_model), BF16),
                pltpu.VMEM((n_tok, d_model), F32), pltpu.VMEM((2, n_tok, d_model), BF16),
                pltpu.VMEM((2, 3, d_model, d_ff), F32),
                pltpu.VMEM((2, 2, 3, 2, 2, piece, d_ff), BF16), pltpu.VMEM((2, 2, 3, 2, 2, piece, d_ff), BF16),
                pltpu.VMEM((2, 2, 3, 2, piece, d_ff), BF16), pltpu.VMEM((2, 2, 3, piece, d_ff), BF16),
                pltpu.VMEM((2, N_EP, n_dp, sub, d_model), BF16), pltpu.VMEM((2, N_EP, n_dp, sub, d_model), BF16),
                pltpu.VMEM((2, n_dp, sub, d_model), BF16), pltpu.VMEM((2, n_dp, sub, d_model), BF16),
                pltpu.VMEM((2, 6, piece, d_ff), BF16), pltpu.VMEM((n_tok, d_model), BF16), pltpu.VMEM((2 * sub, d_model), BF16),
                dma((6,)), dma((N_EP,)), dma((N_EP,)), dma((4, N_EP)), dma((4, N_EP)), dma((4, N_EP)), dma((3, N_EP)), dma((3, 2 * N_EP)),
                dma((2,)), dma((2,)), dma((2, 2, 3)), dma((2, 2, 3)), dma((2, 2, 3)), dma((2, 2, 3)), dma((2, 2, 3)), dma((2, 2, 3)),
                dma((2, N_EP)), dma((2, N_EP)), dma((2, n_dp)), dma((2, n_dp)), dma((4,)),
            ],
            compiler_params=pltpu.CompilerParams(collective_id=0, has_side_effects=True, vmem_limit_bytes=67043328),
        )(tokens, dy_out, dense_w1, dense_w2, idx1.T, gate1.T, idx2.T, gate2.T, wg1, wu1, wd1, wg2, wu2, wd2)
        tok, exp = outs
        res = [tok[:n_tok]]
        for layer in range(2):
            res += [tok[n_tok + layer * sub:n_tok + (layer + 1) * sub], exp[layer, 0:2], exp[layer, 2:4], jnp.swapaxes(exp[layer, 4:6], 1, 2)]
        return tuple(res)

    return jax.shard_map(local_step, mesh=mesh, in_specs=(tok_spec, tok_spec) + layer_specs + layer_specs,
                         out_specs=(tok_spec,) + grad_specs + grad_specs, check_vma=False)
```

```python
import functools

import jax
import jax.numpy as jnp
from jax import lax
from jax.experimental import pallas as pl
from jax.experimental.pallas import tpu as pltpu
from jax.sharding import PartitionSpec as P

MESH = pl.DeviceIdType.MESH
F32, BF16 = jnp.float32, jnp.bfloat16
N_EP = 4
scope = jax.named_scope
N_EXP = 8
CAP = 256


def nn(a, b):
    return lax.dot_general(a, b, (((1,), (0,)), ((), ())), preferred_element_type=F32)


def nt(a, b):
    return lax.dot_general(a, b, (((1,), (1,)), ((), ())), preferred_element_type=F32)


def tn(a, b):
    return lax.dot_general(a, b, (((0,), (0,)), ((), ())), preferred_element_type=F32)


def kernel(n_dp, x_ref, dy_ref, dense1, dense2, idx1, gate1, idx2, gate2,
           wg1_hbm, wu1_hbm, wd1_hbm, wg2_hbm, wu2_hbm, wd2_hbm,
           tok_out, exp_out,
           w_gate, w_up, w_down, auxs, auxb, posr, gater, posc, gatec, tri, ag, ret, x_end, rows_in, t_a, t_b, t_gh, hid, g_a, g_b, g_out,
           acc, g_mix, part, gs, gr, g2, g3, d_send, d_a, d_bs, d_b, exp_v, dx_v, den_v,
           w_sem, aux_send, aux_recv, ag_right, ag_left, ag_recv, ret_send, ret_recv, end_send, end_recv, pair_send, pair_recv,
           one_send, one_recv, two_send, two_recv, da_send, da_recv, db_send, db_recv, out_sem):
    z = lax.axis_index('ep')
    dp = lax.axis_index('dp')
    n_chip = n_dp // 2
    core = dp % 2
    chip = dp // 2
    n_tok, d_model = x_ref.shape
    d_ff = t_a.shape[2]
    piece = d_model // n_dp

    def order(k):
        near_low = jnp.where(z == 1, jnp.where(k == 0, 1, jnp.where(k == 1, 0, k)), k)
        near_high = 3 - jnp.where(z == 2, jnp.where(k == 0, 1, jnp.where(k == 1, 0, k)), k)
        return jnp.where(z < 2, near_low, near_high)

    def order_owned(k):
        low = jnp.where(k == 0, 1, jnp.where(k == 1, 0, k))
        return jnp.where(z < 2, low, 3 - low)

    def owner(s):
        return jnp.where(s < 2, 1, 2)

    inner = jnp.logical_or(z == 1, z == 2)
    outer = jnp.logical_not(inner)
    near_mid = jnp.where(z < 2, 1, 2)
    near_end = jnp.where(z < 2, 0, 3)

    barrier = pltpu.get_barrier_semaphore()
    for k in range(1, N_EP):
        pl.semaphore_signal(barrier, inc=1, device_id={'ep': (z + k) % N_EP, 'dp': dp}, device_id_type=MESH)
    for k in range(1, n_dp):
        pl.semaphore_signal(barrier, inc=1, device_id={'ep': z, 'dp': (dp + k) % n_dp}, device_id_type=MESH)

    w_copies = []
    for n, (hbm, dst) in enumerate(((wg1_hbm, w_gate.at[0]), (wu1_hbm, w_up.at[0]), (wd1_hbm, w_down.at[0]),
                                    (wg2_hbm, w_gate.at[1]), (wu2_hbm, w_up.at[1]), (wd2_hbm, w_down.at[1]))):
        w_copies.append(pltpu.make_async_copy(hbm, dst, w_sem.at[n]))
        w_copies[-1].start()

    auxs[0:2] = idx1[...].astype(F32)
    auxs[2:4] = gate1[...]
    auxs[4:6] = idx2[...].astype(F32)
    auxs[6:8] = gate2[...]
    x = x_ref[...]
    ag[0, z] = (x.astype(F32) + nn(x, dense1[...])).astype(BF16)
    ag[2, z] = dy_ref[...]
    auxb[z] = auxs[...]

    with scope('barrier'):
        pl.semaphore_wait(barrier, N_EP - 1 + n_dp - 1)

    def col_copy(src, dst, send, recv, to):
        return pltpu.make_async_remote_copy(src_ref=src, dst_ref=dst, send_sem=send, recv_sem=recv,
                                            device_id={'ep': to, 'dp': dp}, device_id_type=MESH)

    def row_copy(src, dst, send, recv, to):
        return pltpu.make_async_remote_copy(src_ref=src, dst_ref=dst, send_sem=send, recv_sem=recv,
                                            device_id={'ep': z, 'dp': to}, device_id_type=MESH)

    def aux_copy(k):
        return col_copy(auxs, auxb.at[z], aux_send.at[k], aux_recv.at[z], (z + k) % N_EP)

    for k in range(1, N_EP):
        aux_copy(k).start()

    def ag_to_right(n, s):
        return col_copy(ag.at[n, s], ag.at[n, s], ag_right.at[n, s], ag_recv.at[n, s], jnp.minimum(z + 1, N_EP - 1))

    def ag_to_left(n, s):
        return col_copy(ag.at[n, s], ag.at[n, s], ag_left.at[n, s], ag_recv.at[n, s], jnp.maximum(z - 1, 0))

    def rightward(n, s):
        return jnp.logical_and((owner(s) if n % 2 else s) <= z, z < N_EP - 1)

    def leftward(n, s):
        return jnp.logical_and((owner(s) if n % 2 else s) >= z, z > 0)

    def ag_pass(n, s, right=True, left=True):
        if right is not False:
            @pl.when(jnp.logical_and(rightward(n, s), right))
            def _():
                ag_to_right(n, s).start()

        if left is not False:
            @pl.when(jnp.logical_and(leftward(n, s), left))
            def _():
                ag_to_left(n, s).start()

    def ag_take(n, s):
        with scope('agw%d' % n):
            ag_to_right(n, s).wait_recv()
        ag_pass(n, s)

    def ag_step(n, k):
        @pl.when(k == 1)
        def _():
            ag_take(n, order(1))

        @pl.when(jnp.logical_or(jnp.logical_and(k == 1, inner), jnp.logical_and(k == 2, outer)))
        def _():
            ag_take(n, order(2))

        @pl.when(k == 3)
        def _():
            ag_take(n, order(3))

    def owned_step(n, k, s, early):
        if early:
            @pl.when(jnp.logical_and(k == 0, inner))
            def _():
                ag_take(n, order_owned(2))

            @pl.when(jnp.logical_and(k == 2, inner))
            def _():
                ag_take(n, order_owned(3))

        @pl.when(outer if early else jnp.logical_or(k > 1, outer))
        def _():
            ag_take(n, s)

    def ag_drain(n):
        def body(s, carry):
            @pl.when(rightward(n, s))
            def _():
                ag_to_right(n, s).wait_send()

            @pl.when(leftward(n, s))
            def _():
                ag_to_left(n, s).wait_send()
            return carry
        lax.fori_loop(0, N_EP, body, 0)

    def ret_at(s):
        return jnp.where(owner(s) == z, N_EP + s % 2 * N_EP + z, s)

    def ret_copy(n, s):
        return col_copy(ret.at[n, s], ret.at[n, N_EP + s % 2 * N_EP + z], ret_send.at[n, s], ret_recv.at[n, s % 2 * N_EP + z], owner(s))

    def ret_start(n, s):
        @pl.when(owner(s) != z)
        def _():
            ret_copy(n, s).start()

    def ret_wait(n, p, frm):
        with scope('retw%d' % n):
            at = p * N_EP + frm
            col_copy(ret.at[n, 0], ret.at[n, N_EP + at], ret_send.at[n, 0], ret_recv.at[n, at], z).wait_recv()

    def ret_drain(n):
        def body(s, carry):
            @pl.when(owner(s) != z)
            def _():
                ret_copy(n, s).wait_send()
            return carry
        lax.fori_loop(0, N_EP, body, 0)

    def x_copy():
        return col_copy(x_ref, x_end, end_send.at[0], end_recv.at[0], near_mid)

    def dx_back():
        return col_copy(g_mix.at[0], dx_v, end_send.at[1], end_recv.at[1], near_end)

    ag_pass(0, z)
    ag_pass(2, z, right=z == 1, left=z == 2)

    r_io = lax.broadcasted_iota(jnp.int32, (n_tok, n_tok), 0)
    c_io = lax.broadcasted_iota(jnp.int32, (n_tok, n_tok), 1)
    tri[...] = (c_io < r_io).astype(F32).astype(BF16)
    lane = lax.broadcasted_iota(jnp.int32, (n_tok, N_EXP), 1)
    for k in range(1, N_EP):
        s = (z + k) % N_EP
        col_copy(auxs, auxb.at[s], aux_send.at[k], aux_recv.at[s], s).wait_recv()
    for p in range(2):
        cols = auxb[jnp.where(z < 2, 0, 2) + p].T
        hit0 = cols[:, 0:1] == lane.astype(F32)
        hit1 = cols[:, 1:2] == lane.astype(F32)
        hit = jnp.logical_or(hit0, hit1)
        rank = nn(tri[...], hit.astype(F32).astype(BF16))
        posc[p] = jnp.where(hit, rank, -1.0)
        gatec[p] = jnp.where(hit0, cols[:, 2:3], 0.0) + jnp.where(hit1, cols[:, 3:4], 0.0)
    hits = []
    for layer in range(2):
        for s in range(N_EP):
            for e in range(2):
                a = auxb[s]
                expert = (z * 2 + e).astype(F32)
                hit0 = a[4 * layer:4 * layer + 1] == expert
                hit1 = a[4 * layer + 1:4 * layer + 2] == expert
                hits.append(jnp.logical_or(hit0, hit1).astype(F32))
                gater[(layer * N_EP + s) * 2 + e] = (jnp.where(hit0, a[4 * layer + 2:4 * layer + 3], 0.0)
                                                     + jnp.where(hit1, a[4 * layer + 3:4 * layer + 4], 0.0))
    stack = jnp.concatenate(hits, axis=0)
    ranks = jnp.where(stack > 0.5, nt(stack.astype(BF16), tri[...]), -1.0)
    for n in range(4 * N_EP):
        posr[n] = ranks[n:n + 1]

    for copy in w_copies:
        copy.wait()

    slot = lax.broadcasted_iota(jnp.int32, (CAP, n_tok), 0).astype(F32)
    slot_lane = lax.broadcasted_iota(jnp.int32, (n_tok, CAP), 1).astype(F32)
    step = 32

    def select(layer, s):
        at = (layer * N_EP + s) * 2
        return [posr[at + e] == slot for e in range(2)]

    def as_bf16(picks):
        return jnp.concatenate([p.astype(F32).astype(BF16) for p in picks], axis=0)

    def take_rows(layer, s, n, pick):
        u = ag[n, s]
        if n == 1:
            u = (u.astype(F32) + nn(u, dense2[...])).astype(BF16)
        rows = nn(pick, u).astype(BF16)
        for e in range(2):
            rows_in[layer, e, s] = rows[e * CAP:(e + 1) * CAP]

    def up_project(layer, s, e):
        rows = rows_in[layer, e, s]
        t_a[e] = nn(rows, w_gate[layer, e])
        t_b[e] = nn(rows, w_up[layer, e])

    def forward(s):
        take_rows(0, s, 0, as_bf16(select(0, s)))
        for e in range(2):
            up_project(0, s, e)
        for e in range(2):
            for i in range(CAP // step):
                r = pl.ds(i * step, step)
                a = t_a[e, r, :]
                hid[e, s, r, :] = (a * jax.nn.sigmoid(a) * t_b[e, r, :]).astype(BF16)
            ret[0, ret_at(s), e * CAP:(e + 1) * CAP] = nn(hid[e, s], w_down[0, e]).astype(BF16)

    def backward(layer, s, n_dy, n_ret, n_u):
        picks = select(layer, s)
        pick = as_bf16(picks)
        at = (layer * N_EP + s) * 2
        if n_u is not None:
            take_rows(layer, s, n_u, pick)
        got = nn(pick, ag[n_dy, s])
        for e in range(2):
            gate = jnp.sum(jnp.where(picks[e], gater[at + e], 0.0), axis=1, keepdims=True)
            g_out[e, s] = (got[e * CAP:(e + 1) * CAP] * gate).astype(BF16)
        for e in range(2):
            up_project(layer, s, e)
            t_gh[e] = nt(g_out[e, s], w_down[layer, e]).astype(BF16)
        parts = []
        for e in range(2):
            for i in range(CAP // step):
                r = pl.ds(i * step, step)
                a = t_a[e, r, :]
                b = t_b[e, r, :]
                gh = t_gh[e, r, :].astype(F32)
                sig = jax.nn.sigmoid(a)
                act = a * sig
                hid[e, s, r, :] = (act * b).astype(BF16)
                g_a[e, s, r, :] = (gh * b * sig * (1.0 + a * (1.0 - sig))).astype(BF16)
                g_b[e, s, r, :] = (gh * act).astype(BF16)
            parts.append((nt(g_a[e, s], w_gate[layer, e]) + nt(g_b[e, s], w_up[layer, e])).astype(BF16))
        ret[n_ret, ret_at(s)] = tn(pick, jnp.concatenate(parts, axis=0)).astype(BF16)

    def mix(p, base):
        acc[...] = base.astype(F32)

        def body(k, carry):
            s = order(k)

            @pl.when(k > 0)
            def _():
                ret_wait(0, p, s)

            for e in range(2):
                here = lane == s * 2 + e
                pos = jnp.sum(jnp.where(here, posc[p], 0.0), axis=1, keepdims=True)
                weight = jnp.sum(jnp.where(here, gatec[p], 0.0), axis=1, keepdims=True)
                hot = (pos == slot_lane).astype(F32).astype(BF16)
                acc[...] += nn(hot, ret[0, N_EP + p * N_EP + s, e * CAP:(e + 1) * CAP]) * weight
            return carry
        lax.fori_loop(0, N_EP, body, 0)
        return acc[...].astype(BF16)

    def add_up(n, p, base):
        total = base.astype(F32) + ret[n, N_EP + p * N_EP + z].astype(F32)
        for k in range(1, N_EP):
            ret_wait(n, p, order(k))
            total += ret[n, N_EP + p * N_EP + order(k)].astype(F32)
        return total.astype(BF16)

    chip_x = chip % 2
    chip_y = chip // 2
    over_x = chip + 1 - 2 * chip_x
    over_y = (chip + 2) % n_chip

    def group(e):
        return jnp.where(e == 0, chip_x, chip_y)

    def place(e):
        return jnp.where(e == 0, chip_y, chip_x)

    def pair_copy(layer, e, q):
        return row_copy(gs.at[1 - core, e, q], gr.at[layer, e, q], pair_send.at[layer, e, q], pair_recv.at[layer, e, q], chip * 2 + 1 - core)

    def one_copy(layer, e, q):
        return row_copy(gr.at[layer, e, q, 1 - group(e)], g2.at[layer, e, q], one_send.at[layer, e, q], one_recv.at[layer, e, q],
                        jnp.where(e == 0, over_x, over_y) * 2 + core)

    def two_copy(layer, e, q):
        return row_copy(gr.at[layer, e, q, group(e), 1 - place(e)], g3.at[layer, e, q], two_send.at[layer, e, q], two_recv.at[layer, e, q],
                        jnp.where(e == 0, over_y, over_x) * 2 + core)

    def pair_finish(layer, e, q):
        pair_copy(layer, e, q).wait()
        for g in range(2):
            for p in range(2):
                gr[layer, e, q, g, p] = (gr[layer, e, q, g, p].astype(F32) + gs[core, e, q, g, p].astype(F32)).astype(BF16)
        one_copy(layer, e, q).start()

    def one_finish(layer):
        def body(n, carry):
            e, q = n % 2, (n // 2 + 2) % 3
            one_copy(layer, e, q).wait_recv()
            for p in range(2):
                gr[layer, e, q, group(e), p] = (gr[layer, e, q, group(e), p].astype(F32) + g2[layer, e, q, p].astype(F32)).astype(BF16)
            two_copy(layer, e, q).start()
            return carry
        lax.fori_loop(0, 6, body, 0)

    def two_finish(layer):
        def body(n, carry):
            e, q = n % 2, (n // 2 + 2) % 3
            two_copy(layer, e, q).wait_recv()
            exp_v[layer, q * 2 + e] = (gr[layer, e, q, group(e), place(e)].astype(F32) + g3[layer, e, q].astype(F32)).astype(BF16)
            one_copy(layer, e, q).wait_send()
            two_copy(layer, e, q).wait_send()
            return carry
        lax.fori_loop(0, 6, body, 0)
        exp_copy(layer).start()

    def exp_copy(layer):
        return pltpu.make_async_copy(exp_v.at[layer], exp_out.at[layer], out_sem.at[layer])

    def operands(layer, e, at, n):
        rows = rows_in[layer, e, pl.ds(at, n)].reshape(n * CAP, d_model)
        outs = g_out[e, pl.ds(at, n)].reshape(n * CAP, d_model)
        return [(j, left, right[e, pl.ds(at, n)].reshape(n * CAP, d_ff))
                for j, left, right in ((2, outs, hid), (0, rows, g_a), (1, rows, g_b))]

    def weight_part(layer, at, n):
        def body(e, carry):
            for j, left, right in operands(layer, e, at, n):
                part[e, j] = tn(left, right)
            return carry
        lax.fori_loop(0, 2, body, 0)

    def split_grad(layer, e, j, grad):
        for p in range(n_dp):
            y, x = p // 4, p // 2 % 2
            gs[p % 2, e, j, jnp.where(e == 0, x, y), jnp.where(e == 0, y, x)] = grad[p * piece:(p + 1) * piece].astype(BF16)
        pair_copy(layer, e, j).start()

    def weight_grads(layer):
        def body(e, carry):
            for j, left, right in operands(layer, e, 0, N_EP):
                split_grad(layer, e, j, tn(left, right))
            return carry
        lax.fori_loop(0, 2, body, 0)
        for j in (2, 0, 1):
            for e in range(2):
                pair_finish(layer, e, j)

    def weight_rest(layer, at):
        both = [operands(layer, e, at, 1) for e in range(2)]
        todo = [(e, both[e][q]) for q in range(3) for e in range(2)]
        for k, (e, (j, left, right)) in enumerate(todo):
            split_grad(layer, e, j, tn(left, right) + part[e, j])
            if k >= 2:
                pair_finish(layer, todo[k - 2][0], todo[k - 2][1][0])
        for e, (j, _, _) in todo[4:]:
            pair_finish(layer, e, j)

    sub = piece // N_EP

    def da_copy(layer, k):
        to = (z + k) % N_EP
        return col_copy(d_send.at[layer, to], d_a.at[layer, z], da_send.at[layer, k], da_recv.at[layer, z], to)

    def db_copy(layer, k):
        to = (dp + k) % n_dp
        return row_copy(d_bs.at[layer, to], d_b.at[layer, dp], db_send.at[layer, k], db_recv.at[layer, dp], to)

    def dense_start(layer, grad):
        for q in range(N_EP):
            for p in range(n_dp):
                at = p * piece + q * sub
                d_send[layer, q, p] = grad[at:at + sub].astype(BF16)
        for k in range(1, N_EP):
            da_copy(layer, k).start()
        d_a[layer, z] = d_send[layer, z]

    def dense_middle(layer):
        for m in (1, 2):
            @pl.when(z != m)
            def _():
                col_copy(d_send.at[layer, m], d_a.at[layer, m], da_send.at[layer, 0], da_recv.at[layer, m], m).wait_recv()
        d_bs[layer] = (d_a[layer, 1].astype(F32) + d_a[layer, 2].astype(F32)).astype(BF16)
        for k in range(1, n_dp):
            db_copy(layer, k).start()

    def dense_end(layer):
        total = d_bs[layer, dp].astype(F32)
        for k in range(1, n_dp):
            frm = (dp + k) % n_dp
            row_copy(d_bs.at[layer, frm], d_b.at[layer, frm], db_send.at[layer, k], db_recv.at[layer, frm], frm).wait_recv()
            total += d_b[layer, frm].astype(F32)
        den_v[layer * sub:(layer + 1) * sub] = total.astype(BF16)
        @pl.when(inner)
        def _():
            for k in range(1, N_EP):
                da_copy(layer, k).wait_send()
        for k in range(1, n_dp):
            db_copy(layer, k).wait_send()

    def forward_step(k, carry):
        s = order(k)
        ag_step(0, k)
        with scope('f1'):
            forward(s)
        ret_start(0, s)
        return carry
    lax.fori_loop(0, N_EP, forward_step, 0)

    ag_pass(2, z, right=z != 1, left=z != 2)

    @pl.when(outer)
    def _():
        x_copy().start()

    @pl.when(inner)
    def _():
        ag_take(2, 3 - z)

        def body(n, carry):
            s = jnp.where(n == 0, z, near_end)
            ag[1, s] = mix(s % 2, ag[0, s])
            ag_pass(1, s)

            @pl.when(n == 1)
            def _():
                with scope('dyw'):
                    ag_to_right(2, s).wait_recv()
                ag_pass(2, s, right=z == 1, left=z == 2)
            return carry
        lax.fori_loop(0, 2, body, 0)

    def second_step(k, carry):
        s = order_owned(k)

        owned_step(1, k, s, False)

        @pl.when(jnp.logical_or(k > 2, jnp.logical_and(outer, s != z)))
        def _():
            ag_take(2, s)
        with scope('fb2'):
            backward(1, s, 2, 1, 1)
        ret_start(1, s)
        return carry
    lax.fori_loop(0, N_EP, second_step, 0)
    with scope('wg1'):
        weight_grads(1)

    @pl.when(inner)
    def _():
        def body(n, carry):
            s = jnp.where(n == 0, z, near_end)
            gm = add_up(1, s % 2, ag[2, s])
            g_mix[n] = gm
            ag[3, s] = (gm.astype(F32) + nt(gm, dense2[...])).astype(BF16)
            ag_pass(3, s)
            return carry
        lax.fori_loop(0, 2, body, 0)
        dense_start(1, tn(ag[1, z], g_mix[0]) + tn(ag[1, near_end], g_mix[1]))

    three = jnp.where(z < 2, 0, 1)
    last = jnp.where(z < 2, 3, 0)

    def first_step(k, carry):
        s = order_owned(k)

        @pl.when(jnp.logical_and(k == 3, outer))
        def _():
            with scope('dmid1'):
                dense_middle(1)
            with scope('one1'):
                one_finish(1)
            with scope('wpart'):
                weight_part(0, three, 3)
        owned_step(3, k, s, True)
        with scope('b1'):
            backward(0, s, 3, 2, None)
        ret_start(2, s)
        return carry
    lax.fori_loop(0, N_EP, first_step, 0)

    @pl.when(inner)
    def _():
        dense_middle(1)
        one_finish(1)
        weight_part(0, three, 3)
    with scope('wg0'):
        weight_rest(0, last)
    with scope('one0'):
        one_finish(0)
    with scope('two1'):
        two_finish(1)
    with scope('dend1'):
        dense_end(1)

    def dx_copy():
        return pltpu.make_async_copy(dx_v, tok_out.at[pl.ds(0, n_tok)], out_sem.at[2])

    @pl.when(inner)
    def _():
        gm = add_up(2, z % 2, ag[3, z])
        dx_v[...] = (gm.astype(F32) + nt(gm, dense1[...])).astype(BF16)
        dx_copy().start()
        ge = add_up(2, near_end % 2, ag[3, near_end])
        g_mix[0] = (ge.astype(F32) + nt(ge, dense1[...])).astype(BF16)
        x_copy().wait_recv()
        dense_start(0, tn(x_ref[...], gm) + tn(x_end[...], ge))
        dx_back().start()
    with scope('dmid0'):
        dense_middle(0)
    with scope('two0'):
        two_finish(0)

    @pl.when(outer)
    def _():
        with scope('dxw'):
            dx_back().wait_recv()
        dx_copy().start()
        x_copy().wait_send()
    with scope('dend0'):
        dense_end(0)
    den_copy = pltpu.make_async_copy(den_v, tok_out.at[pl.ds(n_tok, 2 * sub)], out_sem.at[3])
    den_copy.start()
    for n in range(4):
        ag_drain(n)
    for n in range(3):
        ret_drain(n)

    @pl.when(inner)
    def _():
        dx_back().wait_send()
    for k in range(1, N_EP):
        aux_copy(k).wait_send()
    exp_copy(1).wait()
    exp_copy(0).wait()
    dx_copy().wait()
    den_copy.wait()


def solution(mesh):
    n_dp = mesh.shape['dp']
    n_chip = n_dp // 2
    tok_spec = P(('dp', 'ep'), None)
    exp_spec = P('ep', None, None)
    layer_specs = (P(None, None), tok_spec, tok_spec, exp_spec, exp_spec, exp_spec)
    grad_specs = (P(('dp', 'ep'), None), P('ep', 'dp', None), P('ep', 'dp', None), P('ep', None, 'dp'))

    def local_step(tokens, dy_out, dense_w1, idx1, gate1, wg1, wu1, wd1, dense_w2, idx2, gate2, wg2, wu2, wd2):
        n_tok, d_model = tokens.shape
        d_ff = wg1.shape[2]
        piece = d_model // n_dp
        sub = piece // N_EP
        vmem = pl.BlockSpec(memory_space=pltpu.VMEM)
        hbm = pl.BlockSpec(memory_space=pl.ANY)
        dma = pltpu.SemaphoreType.DMA
        outs = pl.pallas_call(
            functools.partial(kernel, n_dp),
            out_shape=(jax.ShapeDtypeStruct((n_tok + 2 * sub, d_model), BF16), jax.ShapeDtypeStruct((2, 6, piece, d_ff), BF16)),
            in_specs=[vmem] * 8 + [hbm] * 6,
            out_specs=[hbm] * 2,
            scratch_shapes=[
                pltpu.VMEM((2, 2, d_model, d_ff), BF16), pltpu.VMEM((2, 2, d_model, d_ff), BF16), pltpu.VMEM((2, 2, d_ff, d_model), BF16),
                pltpu.VMEM((8, n_tok), F32), pltpu.VMEM((N_EP, 8, n_tok), F32), pltpu.VMEM((4 * N_EP, 1, n_tok), F32), pltpu.VMEM((4 * N_EP, 1, n_tok), F32),
                pltpu.VMEM((2, n_tok, N_EXP), F32), pltpu.VMEM((2, n_tok, N_EXP), F32), pltpu.VMEM((n_tok, n_tok), BF16),
                pltpu.VMEM((4, N_EP, n_tok, d_model), BF16), pltpu.VMEM((3, 3 * N_EP, n_tok, d_model), BF16),
                pltpu.VMEM((n_tok, d_model), BF16),
                pltpu.VMEM((2, 2, N_EP, CAP, d_model), BF16), pltpu.VMEM((2, CAP, d_ff), F32), pltpu.VMEM((2, CAP, d_ff), F32),
                pltpu.VMEM((2, CAP, d_ff), BF16), pltpu.VMEM((2, N_EP, CAP, d_ff), BF16), pltpu.VMEM((2, N_EP, CAP, d_ff), BF16),
                pltpu.VMEM((2, N_EP, CAP, d_ff), BF16), pltpu.VMEM((2, N_EP, CAP, d_model), BF16),
                pltpu.VMEM((n_tok, d_model), F32), pltpu.VMEM((2, n_tok, d_model), BF16),
                pltpu.VMEM((2, 3, d_model, d_ff), F32),
                pltpu.VMEM((2, 2, 3, 2, 2, piece, d_ff), BF16), pltpu.VMEM((2, 2, 3, 2, 2, piece, d_ff), BF16),
                pltpu.VMEM((2, 2, 3, 2, piece, d_ff), BF16), pltpu.VMEM((2, 2, 3, piece, d_ff), BF16),
                pltpu.VMEM((2, N_EP, n_dp, sub, d_model), BF16), pltpu.VMEM((2, N_EP, n_dp, sub, d_model), BF16),
                pltpu.VMEM((2, n_dp, sub, d_model), BF16), pltpu.VMEM((2, n_dp, sub, d_model), BF16),
                pltpu.VMEM((2, 6, piece, d_ff), BF16), pltpu.VMEM((n_tok, d_model), BF16), pltpu.VMEM((2 * sub, d_model), BF16),
                dma((6,)), dma((N_EP,)), dma((N_EP,)), dma((4, N_EP)), dma((4, N_EP)), dma((4, N_EP)), dma((3, N_EP)), dma((3, 2 * N_EP)),
                dma((2,)), dma((2,)), dma((2, 2, 3)), dma((2, 2, 3)), dma((2, 2, 3)), dma((2, 2, 3)), dma((2, 2, 3)), dma((2, 2, 3)),
                dma((2, N_EP)), dma((2, N_EP)), dma((2, n_dp)), dma((2, n_dp)), dma((4,)),
            ],
            compiler_params=pltpu.CompilerParams(collective_id=0, has_side_effects=True, vmem_limit_bytes=67043328),
        )(tokens, dy_out, dense_w1, dense_w2, idx1.T, gate1.T, idx2.T, gate2.T, wg1, wu1, wd1, wg2, wu2, wd2)
        tok, exp = outs
        res = [tok[:n_tok]]
        for layer in range(2):
            res += [tok[n_tok + layer * sub:n_tok + (layer + 1) * sub], exp[layer, 0:2], exp[layer, 2:4], jnp.swapaxes(exp[layer, 4:6], 1, 2)]
        return tuple(res)

    return jax.shard_map(local_step, mesh=mesh, in_specs=(tok_spec, tok_spec) + layer_specs + layer_specs,
                         out_specs=(tok_spec,) + grad_specs + grad_specs, check_vma=False)
```

```python
import functools

import jax
import jax.numpy as jnp
from jax import lax
from jax.experimental import pallas as pl
from jax.experimental.pallas import tpu as pltpu
from jax.sharding import PartitionSpec as P

MESH = pl.DeviceIdType.MESH
F32, BF16 = jnp.float32, jnp.bfloat16
N_EP = 4
scope = jax.named_scope
N_EXP = 8
CAP = 256


def nn(a, b):
    return lax.dot_general(a, b, (((1,), (0,)), ((), ())), preferred_element_type=F32)


def nt(a, b):
    return lax.dot_general(a, b, (((1,), (1,)), ((), ())), preferred_element_type=F32)


def tn(a, b):
    return lax.dot_general(a, b, (((0,), (0,)), ((), ())), preferred_element_type=F32)


def kernel(n_dp, x_ref, dy_ref, dense1, dense2, idx1, gate1, idx2, gate2,
           wg1_hbm, wu1_hbm, wd1_hbm, wg2_hbm, wu2_hbm, wd2_hbm,
           tok_out, exp_out,
           w_gate, w_up, w_down, auxs, auxb, posr, gater, posc, gatec, tri, ag, ret, x_end, rows_in, t_a, t_b, t_gh, hid, g_a, g_b, g_out,
           acc, g_mix, part, gs, gr, g2, g3, d_send, d_a, d_bs, d_b, exp_v, dx_v, den_v,
           w_sem, aux_send, aux_recv, ag_right, ag_left, ag_recv, ret_send, ret_recv, end_send, end_recv, pair_send, pair_recv,
           one_send, one_recv, two_send, two_recv, da_send, da_recv, db_send, db_recv, out_sem):
    z = lax.axis_index('ep')
    dp = lax.axis_index('dp')
    n_chip = n_dp // 2
    core = dp % 2
    chip = dp // 2
    n_tok, d_model = x_ref.shape
    d_ff = t_a.shape[2]
    piece = d_model // n_dp

    def swapped(k):
        return jnp.where(k < 2, 1 - k, k)

    def order(k):
        low = jnp.where(jnp.logical_or(z == 1, z == 2), swapped(k), k)
        return jnp.where(z < 2, low, 3 - low)

    def order_owned(k):
        low = swapped(k)
        return jnp.where(z < 2, low, 3 - low)

    def owner(s):
        return jnp.where(s < 2, 1, 2)

    inner = jnp.logical_or(z == 1, z == 2)
    outer = jnp.logical_not(inner)
    near_mid = jnp.where(z < 2, 1, 2)
    near_end = jnp.where(z < 2, 0, 3)

    barrier = pltpu.get_barrier_semaphore()
    for k in range(1, N_EP):
        pl.semaphore_signal(barrier, inc=1, device_id={'ep': (z + k) % N_EP, 'dp': dp}, device_id_type=MESH)
    for k in range(1, n_dp):
        pl.semaphore_signal(barrier, inc=1, device_id={'ep': z, 'dp': (dp + k) % n_dp}, device_id_type=MESH)

    w_copies = []
    for n, (hbm, dst) in enumerate(((wg1_hbm, w_gate.at[0]), (wu1_hbm, w_up.at[0]), (wd1_hbm, w_down.at[0]),
                                    (wg2_hbm, w_gate.at[1]), (wu2_hbm, w_up.at[1]), (wd2_hbm, w_down.at[1]))):
        w_copies.append(pltpu.make_async_copy(hbm, dst, w_sem.at[n]))
        w_copies[-1].start()

    auxs[0:2] = idx1[...].astype(F32)
    auxs[2:4] = gate1[...]
    auxs[4:6] = idx2[...].astype(F32)
    auxs[6:8] = gate2[...]
    x = x_ref[...]
    ag[0, z] = (x.astype(F32) + nn(x, dense1[...])).astype(BF16)
    ag[2, z] = dy_ref[...]
    auxb[z] = auxs[...]

    with scope('barrier'):
        pl.semaphore_wait(barrier, N_EP - 1 + n_dp - 1)

    def col_copy(src, dst, send, recv, to):
        return pltpu.make_async_remote_copy(src_ref=src, dst_ref=dst, send_sem=send, recv_sem=recv,
                                            device_id={'ep': to, 'dp': dp}, device_id_type=MESH)

    def row_copy(src, dst, send, recv, to):
        return pltpu.make_async_remote_copy(src_ref=src, dst_ref=dst, send_sem=send, recv_sem=recv,
                                            device_id={'ep': z, 'dp': to}, device_id_type=MESH)

    def aux_copy(k):
        return col_copy(auxs, auxb.at[z], aux_send.at[k], aux_recv.at[z], (z + k) % N_EP)

    for k in range(1, N_EP):
        aux_copy(k).start()

    def ag_to_right(n, s):
        return col_copy(ag.at[n, s], ag.at[n, s], ag_right.at[n, s], ag_recv.at[n, s], jnp.minimum(z + 1, N_EP - 1))

    def ag_to_left(n, s):
        return col_copy(ag.at[n, s], ag.at[n, s], ag_left.at[n, s], ag_recv.at[n, s], jnp.maximum(z - 1, 0))

    def rightward(n, s):
        return jnp.logical_and((owner(s) if n % 2 else s) <= z, z < N_EP - 1)

    def leftward(n, s):
        return jnp.logical_and((owner(s) if n % 2 else s) >= z, z > 0)

    def ag_pass(n, s, right=True, left=True):
        if right is not False:
            @pl.when(jnp.logical_and(rightward(n, s), right))
            def _():
                ag_to_right(n, s).start()

        if left is not False:
            @pl.when(jnp.logical_and(leftward(n, s), left))
            def _():
                ag_to_left(n, s).start()

    def ag_take(n, s):
        with scope('agw%d' % n):
            ag_to_right(n, s).wait_recv()
        ag_pass(n, s)

    def ag_step(n, k):
        @pl.when(k == 1)
        def _():
            ag_take(n, order(1))

        @pl.when(jnp.logical_or(jnp.logical_and(k == 1, inner), jnp.logical_and(k == 2, outer)))
        def _():
            ag_take(n, order(2))

        @pl.when(k == 3)
        def _():
            ag_take(n, order(3))

    def owned_step(n, k, s, early):
        if early:
            @pl.when(jnp.logical_and(k == 0, inner))
            def _():
                ag_take(n, order_owned(2))

            @pl.when(jnp.logical_and(k == 2, inner))
            def _():
                ag_take(n, order_owned(3))

        @pl.when(outer if early else jnp.logical_or(k > 1, outer))
        def _():
            ag_take(n, s)

    def ag_drain(n):
        def body(s, carry):
            @pl.when(rightward(n, s))
            def _():
                ag_to_right(n, s).wait_send()

            @pl.when(leftward(n, s))
            def _():
                ag_to_left(n, s).wait_send()
            return carry
        lax.fori_loop(0, N_EP, body, 0)

    def ret_at(s):
        return jnp.where(owner(s) == z, N_EP + s % 2 * N_EP + z, s)

    def ret_copy(n, s):
        return col_copy(ret.at[n, s], ret.at[n, N_EP + s % 2 * N_EP + z], ret_send.at[n, s], ret_recv.at[n, s % 2 * N_EP + z], owner(s))

    def ret_start(n, s):
        @pl.when(owner(s) != z)
        def _():
            ret_copy(n, s).start()

    def ret_wait(n, p, frm):
        with scope('retw%d' % n):
            at = p * N_EP + frm
            col_copy(ret.at[n, 0], ret.at[n, N_EP + at], ret_send.at[n, 0], ret_recv.at[n, at], z).wait_recv()

    def ret_drain(n):
        def body(s, carry):
            @pl.when(owner(s) != z)
            def _():
                ret_copy(n, s).wait_send()
            return carry
        lax.fori_loop(0, N_EP, body, 0)

    def x_copy():
        return col_copy(x_ref, x_end, end_send.at[0], end_recv.at[0], near_mid)

    def dx_back():
        return col_copy(g_mix.at[0], dx_v, end_send.at[1], end_recv.at[1], near_end)

    ag_pass(0, z)
    ag_pass(2, z, right=z == 1, left=z == 2)

    r_io = lax.broadcasted_iota(jnp.int32, (n_tok, n_tok), 0)
    c_io = lax.broadcasted_iota(jnp.int32, (n_tok, n_tok), 1)
    tri[...] = (c_io < r_io).astype(F32).astype(BF16)
    lane = lax.broadcasted_iota(jnp.int32, (n_tok, N_EXP), 1)
    for k in range(1, N_EP):
        s = (z + k) % N_EP
        col_copy(auxs, auxb.at[s], aux_send.at[k], aux_recv.at[s], s).wait_recv()
    for p in range(2):
        cols = auxb[jnp.where(z < 2, 0, 2) + p].T
        hit0 = cols[:, 0:1] == lane.astype(F32)
        hit1 = cols[:, 1:2] == lane.astype(F32)
        hit = jnp.logical_or(hit0, hit1)
        rank = nn(tri[...], hit.astype(F32).astype(BF16))
        posc[p] = jnp.where(hit, rank, -1.0)
        gatec[p] = jnp.where(hit0, cols[:, 2:3], 0.0) + jnp.where(hit1, cols[:, 3:4], 0.0)
    hits = []
    for layer in range(2):
        for s in range(N_EP):
            for e in range(2):
                a = auxb[s]
                expert = (z * 2 + e).astype(F32)
                hit0 = a[4 * layer:4 * layer + 1] == expert
                hit1 = a[4 * layer + 1:4 * layer + 2] == expert
                hits.append(jnp.logical_or(hit0, hit1).astype(F32))
                gater[(layer * N_EP + s) * 2 + e] = (jnp.where(hit0, a[4 * layer + 2:4 * layer + 3], 0.0)
                                                     + jnp.where(hit1, a[4 * layer + 3:4 * layer + 4], 0.0))
    stack = jnp.concatenate(hits, axis=0)
    ranks = jnp.where(stack > 0.5, nt(stack.astype(BF16), tri[...]), -1.0)
    for n in range(4 * N_EP):
        posr[n] = ranks[n:n + 1]

    for copy in w_copies:
        copy.wait()

    slot = lax.broadcasted_iota(jnp.int32, (CAP, n_tok), 0).astype(F32)
    slot_lane = lax.broadcasted_iota(jnp.int32, (n_tok, CAP), 1).astype(F32)
    step = 32

    def select(layer, s):
        at = (layer * N_EP + s) * 2
        return [posr[at + e] == slot for e in range(2)]

    def as_bf16(picks):
        return jnp.concatenate([p.astype(F32).astype(BF16) for p in picks], axis=0)

    def take_rows(layer, s, n, pick):
        u = ag[n, s]
        if n == 1:
            u = (u.astype(F32) + nn(u, dense2[...])).astype(BF16)
        rows = nn(pick, u).astype(BF16)
        for e in range(2):
            rows_in[layer, e, s] = rows[e * CAP:(e + 1) * CAP]

    def up_project(layer, s, e):
        rows = rows_in[layer, e, s]
        t_a[e] = nn(rows, w_gate[layer, e])
        t_b[e] = nn(rows, w_up[layer, e])

    def forward(s):
        take_rows(0, s, 0, as_bf16(select(0, s)))
        for e in range(2):
            up_project(0, s, e)
        for e in range(2):
            for i in range(CAP // step):
                r = pl.ds(i * step, step)
                a = t_a[e, r, :]
                hid[e, s, r, :] = (a * jax.nn.sigmoid(a) * t_b[e, r, :]).astype(BF16)
            ret[0, ret_at(s), e * CAP:(e + 1) * CAP] = nn(hid[e, s], w_down[0, e]).astype(BF16)

    def backward(layer, s, n_dy, n_ret, n_u):
        picks = select(layer, s)
        pick = as_bf16(picks)
        at = (layer * N_EP + s) * 2
        if n_u is not None:
            take_rows(layer, s, n_u, pick)
        got = nn(pick, ag[n_dy, s])
        for e in range(2):
            gate = jnp.sum(jnp.where(picks[e], gater[at + e], 0.0), axis=1, keepdims=True)
            g_out[e, s] = (got[e * CAP:(e + 1) * CAP] * gate).astype(BF16)
        for e in range(2):
            up_project(layer, s, e)
            t_gh[e] = nt(g_out[e, s], w_down[layer, e]).astype(BF16)
        parts = []
        for e in range(2):
            for i in range(CAP // step):
                r = pl.ds(i * step, step)
                a = t_a[e, r, :]
                b = t_b[e, r, :]
                gh = t_gh[e, r, :].astype(F32)
                sig = jax.nn.sigmoid(a)
                act = a * sig
                hid[e, s, r, :] = (act * b).astype(BF16)
                g_a[e, s, r, :] = (gh * b * sig * (1.0 + a * (1.0 - sig))).astype(BF16)
                g_b[e, s, r, :] = (gh * act).astype(BF16)
            parts.append((nt(g_a[e, s], w_gate[layer, e]) + nt(g_b[e, s], w_up[layer, e])).astype(BF16))
        ret[n_ret, ret_at(s)] = tn(pick, jnp.concatenate(parts, axis=0)).astype(BF16)

    def mix(p, base):
        acc[...] = base.astype(F32)

        def body(k, carry):
            s = order(k)

            @pl.when(k > 0)
            def _():
                ret_wait(0, p, s)

            for e in range(2):
                here = lane == s * 2 + e
                pos = jnp.sum(jnp.where(here, posc[p], 0.0), axis=1, keepdims=True)
                weight = jnp.sum(jnp.where(here, gatec[p], 0.0), axis=1, keepdims=True)
                hot = (pos == slot_lane).astype(F32).astype(BF16)
                acc[...] += nn(hot, ret[0, N_EP + p * N_EP + s, e * CAP:(e + 1) * CAP]) * weight
            return carry
        lax.fori_loop(0, N_EP, body, 0)
        return acc[...].astype(BF16)

    def add_up(n, p, base):
        total = base.astype(F32) + ret[n, N_EP + p * N_EP + z].astype(F32)
        for k in range(1, N_EP):
            ret_wait(n, p, order(k))
            total += ret[n, N_EP + p * N_EP + order(k)].astype(F32)
        return total.astype(BF16)

    chip_x = chip % 2
    chip_y = chip // 2
    over_x = chip + 1 - 2 * chip_x
    over_y = (chip + 2) % n_chip

    def group(e):
        return jnp.where(e == 0, chip_x, chip_y)

    def place(e):
        return jnp.where(e == 0, chip_y, chip_x)

    def pair_copy(layer, e, q):
        return row_copy(gs.at[1 - core, e, q], gr.at[layer, e, q], pair_send.at[layer, e, q], pair_recv.at[layer, e, q], chip * 2 + 1 - core)

    def one_copy(layer, e, q):
        return row_copy(gr.at[layer, e, q, 1 - group(e)], g2.at[layer, e, q], one_send.at[layer, e, q], one_recv.at[layer, e, q],
                        jnp.where(e == 0, over_x, over_y) * 2 + core)

    def two_copy(layer, e, q):
        return row_copy(gr.at[layer, e, q, group(e), 1 - place(e)], g3.at[layer, e, q], two_send.at[layer, e, q], two_recv.at[layer, e, q],
                        jnp.where(e == 0, over_y, over_x) * 2 + core)

    def pair_finish(layer, e, q):
        pair_copy(layer, e, q).wait()
        for g in range(2):
            for p in range(2):
                gr[layer, e, q, g, p] = (gr[layer, e, q, g, p].astype(F32) + gs[core, e, q, g, p].astype(F32)).astype(BF16)
        one_copy(layer, e, q).start()

    def one_finish(layer):
        def body(n, carry):
            e, q = n % 2, (n // 2 + 2) % 3
            one_copy(layer, e, q).wait_recv()
            for p in range(2):
                gr[layer, e, q, group(e), p] = (gr[layer, e, q, group(e), p].astype(F32) + g2[layer, e, q, p].astype(F32)).astype(BF16)
            two_copy(layer, e, q).start()
            return carry
        lax.fori_loop(0, 6, body, 0)

    def two_finish(layer):
        def body(n, carry):
            e, q = n % 2, (n // 2 + 2) % 3
            two_copy(layer, e, q).wait_recv()
            exp_v[layer, q * 2 + e] = (gr[layer, e, q, group(e), place(e)].astype(F32) + g3[layer, e, q].astype(F32)).astype(BF16)
            one_copy(layer, e, q).wait_send()
            two_copy(layer, e, q).wait_send()
            return carry
        lax.fori_loop(0, 6, body, 0)
        exp_copy(layer).start()

    def exp_copy(layer):
        return pltpu.make_async_copy(exp_v.at[layer], exp_out.at[layer], out_sem.at[layer])

    def operands(layer, e, at, n):
        rows = rows_in[layer, e, pl.ds(at, n)].reshape(n * CAP, d_model)
        outs = g_out[e, pl.ds(at, n)].reshape(n * CAP, d_model)
        return [(j, left, right[e, pl.ds(at, n)].reshape(n * CAP, d_ff))
                for j, left, right in ((2, outs, hid), (0, rows, g_a), (1, rows, g_b))]

    def weight_part(layer, at, n):
        def body(e, carry):
            for j, left, right in operands(layer, e, at, n):
                part[e, j] = tn(left, right)
            return carry
        lax.fori_loop(0, 2, body, 0)

    def split_grad(layer, e, j, grad):
        for p in range(n_dp):
            y, x = p // 4, p // 2 % 2
            gs[p % 2, e, j, jnp.where(e == 0, x, y), jnp.where(e == 0, y, x)] = grad[p * piece:(p + 1) * piece].astype(BF16)
        pair_copy(layer, e, j).start()

    def weight_grads(layer):
        def body(e, carry):
            for j, left, right in operands(layer, e, 0, N_EP):
                split_grad(layer, e, j, tn(left, right))
            return carry
        lax.fori_loop(0, 2, body, 0)
        for j in (2, 0, 1):
            for e in range(2):
                pair_finish(layer, e, j)

    def weight_rest(layer, at):
        both = [operands(layer, e, at, 2) for e in range(2)]
        todo = [(e, both[e][q]) for q in range(3) for e in range(2)]
        for k, (e, (j, left, right)) in enumerate(todo):
            split_grad(layer, e, j, tn(left, right) + part[e, j])
            if k >= 2:
                pair_finish(layer, todo[k - 2][0], todo[k - 2][1][0])
        for e, (j, _, _) in todo[4:]:
            pair_finish(layer, e, j)

    sub = piece // N_EP

    def da_copy(layer, k):
        to = (z + k) % N_EP
        return col_copy(d_send.at[layer, to], d_a.at[layer, z], da_send.at[layer, k], da_recv.at[layer, z], to)

    def db_copy(layer, k):
        to = (dp + k) % n_dp
        return row_copy(d_bs.at[layer, to], d_b.at[layer, dp], db_send.at[layer, k], db_recv.at[layer, dp], to)

    def dense_start(layer, grad):
        for q in range(N_EP):
            for p in range(n_dp):
                at = p * piece + q * sub
                d_send[layer, q, p] = grad[at:at + sub].astype(BF16)
        for k in range(1, N_EP):
            da_copy(layer, k).start()
        d_a[layer, z] = d_send[layer, z]

    def dense_middle(layer):
        for m in (1, 2):
            @pl.when(z != m)
            def _():
                col_copy(d_send.at[layer, m], d_a.at[layer, m], da_send.at[layer, 0], da_recv.at[layer, m], m).wait_recv()
        d_bs[layer] = (d_a[layer, 1].astype(F32) + d_a[layer, 2].astype(F32)).astype(BF16)
        for k in range(1, n_dp):
            db_copy(layer, k).start()

    def dense_end(layer):
        total = d_bs[layer, dp].astype(F32)
        for k in range(1, n_dp):
            frm = (dp + k) % n_dp
            row_copy(d_bs.at[layer, frm], d_b.at[layer, frm], db_send.at[layer, k], db_recv.at[layer, frm], frm).wait_recv()
            total += d_b[layer, frm].astype(F32)
        den_v[layer * sub:(layer + 1) * sub] = total.astype(BF16)
        @pl.when(inner)
        def _():
            for k in range(1, N_EP):
                da_copy(layer, k).wait_send()
        for k in range(1, n_dp):
            db_copy(layer, k).wait_send()

    def forward_step(k, carry):
        s = order(k)
        ag_step(0, k)
        with scope('f1'):
            forward(s)
        ret_start(0, s)
        return carry
    lax.fori_loop(0, N_EP, forward_step, 0)

    ag_pass(2, z, right=z != 1, left=z != 2)

    @pl.when(outer)
    def _():
        x_copy().start()

    @pl.when(inner)
    def _():
        ag_take(2, 3 - z)

        def body(n, carry):
            s = jnp.where(n == 0, z, near_end)
            ag[1, s] = mix(s % 2, ag[0, s])
            ag_pass(1, s)

            @pl.when(n == 1)
            def _():
                with scope('dyw'):
                    ag_to_right(2, s).wait_recv()
                ag_pass(2, s, right=z == 1, left=z == 2)
            return carry
        lax.fori_loop(0, 2, body, 0)

    def second_step(k, carry):
        s = order_owned(k)

        owned_step(1, k, s, False)

        @pl.when(jnp.logical_or(k > 2, jnp.logical_and(outer, s != z)))
        def _():
            ag_take(2, s)
        with scope('fb2'):
            backward(1, s, 2, 1, 1)
        ret_start(1, s)
        return carry
    lax.fori_loop(0, N_EP, second_step, 0)
    with scope('wg1'):
        weight_grads(1)

    @pl.when(inner)
    def _():
        def body(n, carry):
            s = jnp.where(n == 0, z, near_end)
            gm = add_up(1, s % 2, ag[2, s])
            g_mix[n] = gm
            ag[3, s] = (gm.astype(F32) + nt(gm, dense2[...])).astype(BF16)
            ag_pass(3, s)
            return carry
        lax.fori_loop(0, 2, body, 0)
        dense_start(1, tn(ag[1, z], g_mix[0]) + tn(ag[1, near_end], g_mix[1]))

    early_at = jnp.where(z < 2, 0, 2)
    late_at = 2 - early_at

    def first_step(k, carry):
        s = order_owned(k)

        @pl.when(jnp.logical_and(k == 2, outer))
        def _():
            with scope('wpart'):
                weight_part(0, early_at, 2)

        @pl.when(jnp.logical_and(k == 3, outer))
        def _():
            with scope('dmid1'):
                dense_middle(1)
            with scope('one1'):
                one_finish(1)
        owned_step(3, k, s, True)
        with scope('b1'):
            backward(0, s, 3, 2, None)
        ret_start(2, s)
        return carry
    lax.fori_loop(0, N_EP, first_step, 0)

    @pl.when(inner)
    def _():
        dense_middle(1)
        one_finish(1)
        weight_part(0, early_at, 2)
    with scope('wg0'):
        weight_rest(0, late_at)
    for n in range(3):
        ag_drain(n)
    for n in range(2):
        ret_drain(n)

    @pl.when(outer)
    def _():
        x_copy().wait_send()
    for k in range(1, N_EP):
        aux_copy(k).wait_send()
    with scope('one0'):
        one_finish(0)
    with scope('two1'):
        two_finish(1)
    with scope('dend1'):
        dense_end(1)

    def dx_copy():
        return pltpu.make_async_copy(dx_v, tok_out.at[pl.ds(0, n_tok)], out_sem.at[2])

    @pl.when(inner)
    def _():
        gm = add_up(2, z % 2, ag[3, z])
        dx_v[...] = (gm.astype(F32) + nt(gm, dense1[...])).astype(BF16)
        dx_copy().start()
        ge = add_up(2, near_end % 2, ag[3, near_end])
        g_mix[0] = (ge.astype(F32) + nt(ge, dense1[...])).astype(BF16)
        x_copy().wait_recv()
        dense_start(0, tn(x_ref[...], gm) + tn(x_end[...], ge))
        dx_back().start()
    with scope('dmid0'):
        dense_middle(0)
    with scope('two0'):
        two_finish(0)

    @pl.when(outer)
    def _():
        with scope('dxw'):
            dx_back().wait_recv()
        dx_copy().start()
    with scope('dend0'):
        dense_end(0)
    den_copy = pltpu.make_async_copy(den_v, tok_out.at[pl.ds(n_tok, 2 * sub)], out_sem.at[3])
    den_copy.start()
    ag_drain(3)
    ret_drain(2)

    @pl.when(inner)
    def _():
        dx_back().wait_send()
    exp_copy(1).wait()
    exp_copy(0).wait()
    dx_copy().wait()
    den_copy.wait()


def spread(n_tok, sub, tok, exp, *refs):
    outs, tok_v, exp_v, sem = refs[:9], refs[9], refs[10], refs[11]
    parts = [(tok, tok_v), (exp, exp_v)]
    for n, (src, dst) in enumerate(parts):
        pltpu.make_async_copy(src, dst, sem.at[n]).start()
    pltpu.make_async_copy(tok, tok_v, sem.at[0]).wait()
    copies = [(tok_v.at[pl.ds(0, n_tok)], outs[0])]
    for layer in range(2):
        copies.append((tok_v.at[pl.ds(n_tok + layer * sub, sub)], outs[1 + 4 * layer]))
    for layer in range(2):
        for q in range(3):
            copies.append((exp_v.at[layer, pl.ds(2 * q, 2)], outs[2 + 4 * layer + q]))
    for n, (src, dst) in enumerate(copies):
        if n == 3:
            pltpu.make_async_copy(exp, exp_v, sem.at[1]).wait()
        pltpu.make_async_copy(src, dst, sem.at[2 + n]).start()
    for n, (src, dst) in enumerate(copies):
        pltpu.make_async_copy(src, dst, sem.at[2 + n]).wait()


def solution(mesh):
    n_dp = mesh.shape['dp']
    n_chip = n_dp // 2
    tok_spec = P(('dp', 'ep'), None)
    exp_spec = P('ep', None, None)
    layer_specs = (P(None, None), tok_spec, tok_spec, exp_spec, exp_spec, exp_spec)
    grad_specs = (P(('dp', 'ep'), None), P('ep', 'dp', None), P('ep', 'dp', None), P('ep', None, 'dp'))

    def local_step(tokens, dy_out, dense_w1, idx1, gate1, wg1, wu1, wd1, dense_w2, idx2, gate2, wg2, wu2, wd2):
        n_tok, d_model = tokens.shape
        d_ff = wg1.shape[2]
        piece = d_model // n_dp
        sub = piece // N_EP
        vmem = pl.BlockSpec(memory_space=pltpu.VMEM)
        hbm = pl.BlockSpec(memory_space=pl.ANY)
        dma = pltpu.SemaphoreType.DMA
        six = (2, 2, 3)
        outs = pl.pallas_call(
            functools.partial(kernel, n_dp),
            out_shape=(jax.ShapeDtypeStruct((n_tok + 2 * sub, d_model), BF16), jax.ShapeDtypeStruct((2, 6, piece, d_ff), BF16)),
            in_specs=[vmem] * 8 + [hbm] * 6,
            out_specs=[hbm] * 2,
            scratch_shapes=[
                pltpu.VMEM((2, 2, d_model, d_ff), BF16), pltpu.VMEM((2, 2, d_model, d_ff), BF16), pltpu.VMEM((2, 2, d_ff, d_model), BF16),
                pltpu.VMEM((8, n_tok), F32), pltpu.VMEM((N_EP, 8, n_tok), F32), pltpu.VMEM((4 * N_EP, 1, n_tok), F32), pltpu.VMEM((4 * N_EP, 1, n_tok), F32),
                pltpu.VMEM((2, n_tok, N_EXP), F32), pltpu.VMEM((2, n_tok, N_EXP), F32), pltpu.VMEM((n_tok, n_tok), BF16),
                pltpu.VMEM((4, N_EP, n_tok, d_model), BF16), pltpu.VMEM((3, 3 * N_EP, n_tok, d_model), BF16),
                pltpu.VMEM((n_tok, d_model), BF16),
                pltpu.VMEM((2, 2, N_EP, CAP, d_model), BF16), pltpu.VMEM((2, CAP, d_ff), F32), pltpu.VMEM((2, CAP, d_ff), F32),
                pltpu.VMEM((2, CAP, d_ff), BF16), pltpu.VMEM((2, N_EP, CAP, d_ff), BF16), pltpu.VMEM((2, N_EP, CAP, d_ff), BF16),
                pltpu.VMEM((2, N_EP, CAP, d_ff), BF16), pltpu.VMEM((2, N_EP, CAP, d_model), BF16),
                pltpu.VMEM((n_tok, d_model), F32), pltpu.VMEM((2, n_tok, d_model), BF16),
                pltpu.VMEM((2, 3, d_model, d_ff), F32),
                *[pltpu.VMEM(six + (2, 2, piece, d_ff), BF16)] * 2, pltpu.VMEM(six + (2, piece, d_ff), BF16), pltpu.VMEM(six + (piece, d_ff), BF16),
                pltpu.VMEM((2, N_EP, n_dp, sub, d_model), BF16), pltpu.VMEM((2, N_EP, n_dp, sub, d_model), BF16),
                pltpu.VMEM((2, n_dp, sub, d_model), BF16), pltpu.VMEM((2, n_dp, sub, d_model), BF16),
                pltpu.VMEM((2, 6, piece, d_ff), BF16), pltpu.VMEM((n_tok, d_model), BF16), pltpu.VMEM((2 * sub, d_model), BF16),
                dma((6,)), dma((N_EP,)), dma((N_EP,)), *[dma((4, N_EP))] * 3, dma((3, N_EP)), dma((3, 2 * N_EP)),
                dma((2,)), dma((2,)), *[dma(six)] * 6, *[dma((2, N_EP))] * 2, *[dma((2, n_dp))] * 2, dma((4,)),
            ],
            compiler_params=pltpu.CompilerParams(collective_id=0, has_side_effects=True, vmem_limit_bytes=67043328),
        )(tokens, dy_out, dense_w1, dense_w2, idx1.T, gate1.T, idx2.T, gate2.T, wg1, wu1, wd1, wg2, wu2, wd2)
        tok, exp = outs
        grads = [jax.ShapeDtypeStruct((sub, d_model), BF16)] + [jax.ShapeDtypeStruct((2, piece, d_ff), BF16)] * 3
        res = list(pl.pallas_call(
            functools.partial(spread, n_tok, sub),
            out_shape=tuple([jax.ShapeDtypeStruct((n_tok, d_model), BF16)] + grads * 2),
            in_specs=[hbm] * 2,
            out_specs=[hbm] * 9,
            scratch_shapes=[pltpu.VMEM((n_tok + 2 * sub, d_model), BF16), pltpu.VMEM((2, 6, piece, d_ff), BF16), dma((11,))],
        )(tok, exp))
        for n in (4, 8):
            res[n] = jnp.swapaxes(res[n], 1, 2)
        return tuple(res)

    return jax.shard_map(local_step, mesh=mesh, in_specs=(tok_spec, tok_spec) + layer_specs + layer_specs,
                         out_specs=(tok_spec,) + grad_specs + grad_specs, check_vma=False)
```

```python
import functools

import jax
import jax.numpy as jnp
from jax import lax
from jax.experimental import pallas as pl
from jax.experimental.pallas import tpu as pltpu
from jax.sharding import PartitionSpec as P

MESH = pl.DeviceIdType.MESH
F32, BF16 = jnp.float32, jnp.bfloat16
N_EP = 4
scope = jax.named_scope
N_EXP = 8
CAP = 256


def nn(a, b):
    return lax.dot_general(a, b, (((1,), (0,)), ((), ())), preferred_element_type=F32)


def nt(a, b):
    return lax.dot_general(a, b, (((1,), (1,)), ((), ())), preferred_element_type=F32)


def tn(a, b):
    return lax.dot_general(a, b, (((0,), (0,)), ((), ())), preferred_element_type=F32)


def kernel(n_dp, x_ref, dy_ref, dense1, dense2, idx1, gate1, idx2, gate2,
           wg1_hbm, wu1_hbm, wd1_hbm, wg2_hbm, wu2_hbm, wd2_hbm,
           tok_out, exp_out,
           w_gate, w_up, w_down, auxs, auxb, posr, gater, posc, gatec, tri, ag, ret, x_end, merge_in, rows_in, t_a, t_b, t_gh, hid, g_a, g_b, g_out,
           acc, g_mix, part, gs, gr, g2, g3, d_send, d_a, d_bs, d_b, exp_v, dx_v, den_v,
           w_sem, aux_send, aux_recv, ag_right, ag_left, ag_recv, ret_send, ret_recv, end_send, end_recv, pair_send, pair_recv,
           one_send, one_recv, two_send, two_recv, da_send, da_recv, db_send, db_recv, out_sem):
    z = lax.axis_index('ep')
    dp = lax.axis_index('dp')
    n_chip = n_dp // 2
    core = dp % 2
    chip = dp // 2
    n_tok, d_model = x_ref.shape
    d_ff = t_a.shape[2]
    piece = d_model // n_dp

    def swapped(k):
        return jnp.where(k < 2, 1 - k, k)

    def order(k):
        low = jnp.where(jnp.logical_or(z == 1, z == 2), swapped(k), k)
        return jnp.where(z < 2, low, 3 - low)

    def order_owned(k):
        low = swapped(k)
        return jnp.where(z < 2, low, 3 - low)

    def owner(s):
        return jnp.where(s < 2, 1, 2)

    inner = jnp.logical_or(z == 1, z == 2)
    outer = jnp.logical_not(inner)
    near_mid = jnp.where(z < 2, 1, 2)
    near_end = jnp.where(z < 2, 0, 3)

    barrier = pltpu.get_barrier_semaphore()
    for k in range(1, N_EP):
        pl.semaphore_signal(barrier, inc=1, device_id={'ep': (z + k) % N_EP, 'dp': dp}, device_id_type=MESH)
    for k in range(1, n_dp):
        pl.semaphore_signal(barrier, inc=1, device_id={'ep': z, 'dp': (dp + k) % n_dp}, device_id_type=MESH)

    w_copies = []
    for n, (hbm, dst) in enumerate(((wg1_hbm, w_gate.at[0]), (wu1_hbm, w_up.at[0]), (wd1_hbm, w_down.at[0]),
                                    (wg2_hbm, w_gate.at[1]), (wu2_hbm, w_up.at[1]), (wd2_hbm, w_down.at[1]))):
        w_copies.append(pltpu.make_async_copy(hbm, dst, w_sem.at[n]))
        w_copies[-1].start()

    auxs[0:2] = idx1[...].astype(F32)
    auxs[2:4] = gate1[...]
    auxs[4:6] = idx2[...].astype(F32)
    auxs[6:8] = gate2[...]
    x = x_ref[...]
    ag[0, z] = (x.astype(F32) + nn(x, dense1[...])).astype(BF16)
    ag[2, z] = dy_ref[...]
    auxb[z] = auxs[...]

    with scope('barrier'):
        pl.semaphore_wait(barrier, N_EP - 1 + n_dp - 1)

    def col_copy(src, dst, send, recv, to):
        return pltpu.make_async_remote_copy(src_ref=src, dst_ref=dst, send_sem=send, recv_sem=recv,
                                            device_id={'ep': to, 'dp': dp}, device_id_type=MESH)

    def row_copy(src, dst, send, recv, to):
        return pltpu.make_async_remote_copy(src_ref=src, dst_ref=dst, send_sem=send, recv_sem=recv,
                                            device_id={'ep': z, 'dp': to}, device_id_type=MESH)

    def aux_copy(k):
        return col_copy(auxs, auxb.at[z], aux_send.at[k], aux_recv.at[z], (z + k) % N_EP)

    for k in range(1, N_EP):
        aux_copy(k).start()

    def ag_to_right(n, s):
        return col_copy(ag.at[n, s], ag.at[n, s], ag_right.at[n, s], ag_recv.at[n, s], jnp.minimum(z + 1, N_EP - 1))

    def ag_to_left(n, s):
        return col_copy(ag.at[n, s], ag.at[n, s], ag_left.at[n, s], ag_recv.at[n, s], jnp.maximum(z - 1, 0))

    def rightward(n, s):
        return jnp.logical_and((owner(s) if n % 2 else s) <= z, z < N_EP - 1)

    def leftward(n, s):
        return jnp.logical_and((owner(s) if n % 2 else s) >= z, z > 0)

    def ag_pass(n, s, right=True, left=True):
        if right is not False:
            @pl.when(jnp.logical_and(rightward(n, s), right))
            def _():
                ag_to_right(n, s).start()

        if left is not False:
            @pl.when(jnp.logical_and(leftward(n, s), left))
            def _():
                ag_to_left(n, s).start()

    def ag_take(n, s):
        with scope('agw%d' % n):
            ag_to_right(n, s).wait_recv()
        ag_pass(n, s)

    def ag_step(n, k):
        @pl.when(k == 1)
        def _():
            ag_take(n, order(1))

        @pl.when(jnp.logical_or(jnp.logical_and(k == 1, inner), jnp.logical_and(k == 2, outer)))
        def _():
            ag_take(n, order(2))

        @pl.when(k == 3)
        def _():
            ag_take(n, order(3))

    def owned_step(n, k, s, early):
        if early:
            @pl.when(jnp.logical_and(k == 0, inner))
            def _():
                ag_take(n, order_owned(2))

            @pl.when(jnp.logical_and(k == 2, inner))
            def _():
                ag_take(n, order_owned(3))

        @pl.when(outer if early else jnp.logical_or(k > 1, outer))
        def _():
            ag_take(n, s)

    def ag_drain(n):
        def body(s, carry):
            @pl.when(rightward(n, s))
            def _():
                ag_to_right(n, s).wait_send()

            @pl.when(leftward(n, s))
            def _():
                ag_to_left(n, s).wait_send()
            return carry
        lax.fori_loop(0, N_EP, body, 0)

    def ret_at(s):
        return jnp.where(owner(s) == z, N_EP + s % 2 * N_EP + z, s)

    def ret_copy(n, s):
        return col_copy(ret.at[n, s], ret.at[n, N_EP + s % 2 * N_EP + z], ret_send.at[n, s], ret_recv.at[n, s % 2 * N_EP + z], owner(s))

    def ret_start(n, s):
        @pl.when(owner(s) != z)
        def _():
            ret_copy(n, s).start()

    def ret_wait(n, p, frm):
        with scope('retw%d' % n):
            at = p * N_EP + frm
            col_copy(ret.at[n, 0], ret.at[n, N_EP + at], ret_send.at[n, 0], ret_recv.at[n, at], z).wait_recv()

    def ret_drain(n):
        def body(s, carry):
            away = owner(s) != z

            @pl.when(jnp.logical_and(away, jnp.logical_or(inner, s != order_owned(2))) if n == 2 else away)
            def _():
                ret_copy(n, s).wait_send()
            return carry
        lax.fori_loop(0, N_EP, body, 0)

    def merge_copy():
        return col_copy(ret.at[2, order_owned(2)], merge_in, end_send.at[2], end_recv.at[2], near_mid)

    def x_copy():
        return col_copy(x_ref, x_end, end_send.at[0], end_recv.at[0], near_mid)

    def dx_back():
        return col_copy(g_mix.at[0], tok_out.at[pl.ds(0, n_tok)], end_send.at[1], end_recv.at[1], near_end)

    ag_pass(0, z)
    ag_pass(2, z, right=z == 1, left=z == 2)

    r_io = lax.broadcasted_iota(jnp.int32, (n_tok, n_tok), 0)
    c_io = lax.broadcasted_iota(jnp.int32, (n_tok, n_tok), 1)
    tri[...] = (c_io < r_io).astype(F32).astype(BF16)
    lane = lax.broadcasted_iota(jnp.int32, (n_tok, N_EXP), 1)
    for k in range(1, N_EP):
        s = (z + k) % N_EP
        col_copy(auxs, auxb.at[s], aux_send.at[k], aux_recv.at[s], s).wait_recv()
    for p in range(2):
        cols = auxb[jnp.where(z < 2, 0, 2) + p].T
        hit0 = cols[:, 0:1] == lane.astype(F32)
        hit1 = cols[:, 1:2] == lane.astype(F32)
        hit = jnp.logical_or(hit0, hit1)
        rank = nn(tri[...], hit.astype(F32).astype(BF16))
        posc[p] = jnp.where(hit, rank, -1.0)
        gatec[p] = jnp.where(hit0, cols[:, 2:3], 0.0) + jnp.where(hit1, cols[:, 3:4], 0.0)
    hits = []
    for layer in range(2):
        for s in range(N_EP):
            for e in range(2):
                a = auxb[s]
                expert = (z * 2 + e).astype(F32)
                hit0 = a[4 * layer:4 * layer + 1] == expert
                hit1 = a[4 * layer + 1:4 * layer + 2] == expert
                hits.append(jnp.logical_or(hit0, hit1).astype(F32))
                gater[(layer * N_EP + s) * 2 + e] = (jnp.where(hit0, a[4 * layer + 2:4 * layer + 3], 0.0)
                                                     + jnp.where(hit1, a[4 * layer + 3:4 * layer + 4], 0.0))
    stack = jnp.concatenate(hits, axis=0)
    ranks = jnp.where(stack > 0.5, nt(stack.astype(BF16), tri[...]), -1.0)
    for n in range(4 * N_EP):
        posr[n] = ranks[n:n + 1]

    for copy in w_copies:
        copy.wait()

    slot = lax.broadcasted_iota(jnp.int32, (CAP, n_tok), 0).astype(F32)
    slot_lane = lax.broadcasted_iota(jnp.int32, (n_tok, CAP), 1).astype(F32)
    step = 32

    def select(layer, s):
        at = (layer * N_EP + s) * 2
        return [posr[at + e] == slot for e in range(2)]

    def as_bf16(picks):
        return jnp.concatenate([p.astype(F32).astype(BF16) for p in picks], axis=0)

    def take_rows(layer, s, n, pick):
        u = ag[n, s]
        if n == 1:
            u = (u.astype(F32) + nn(u, dense2[...])).astype(BF16)
        rows = nn(pick, u).astype(BF16)
        for e in range(2):
            rows_in[layer, e, s] = rows[e * CAP:(e + 1) * CAP]

    def up_project(layer, s, e):
        rows = rows_in[layer, e, s]
        t_a[e] = nn(rows, w_gate[layer, e])
        t_b[e] = nn(rows, w_up[layer, e])

    def forward(s):
        take_rows(0, s, 0, as_bf16(select(0, s)))
        for e in range(2):
            up_project(0, s, e)
        for e in range(2):
            for i in range(CAP // step):
                r = pl.ds(i * step, step)
                a = t_a[e, r, :]
                hid[e, s, r, :] = (a * jax.nn.sigmoid(a) * t_b[e, r, :]).astype(BF16)
            ret[0, ret_at(s), e * CAP:(e + 1) * CAP] = nn(hid[e, s], w_down[0, e]).astype(BF16)

    def backward(layer, s, n_dy, n_ret, n_u):
        picks = select(layer, s)
        pick = as_bf16(picks)
        at = (layer * N_EP + s) * 2
        if n_u is not None:
            take_rows(layer, s, n_u, pick)
        got = nn(pick, ag[n_dy, s])
        for e in range(2):
            gate = jnp.sum(jnp.where(picks[e], gater[at + e], 0.0), axis=1, keepdims=True)
            g_out[e, s] = (got[e * CAP:(e + 1) * CAP] * gate).astype(BF16)
        for e in range(2):
            up_project(layer, s, e)
            t_gh[e] = nt(g_out[e, s], w_down[layer, e]).astype(BF16)
        parts = []
        for e in range(2):
            for i in range(CAP // step):
                r = pl.ds(i * step, step)
                a = t_a[e, r, :]
                b = t_b[e, r, :]
                gh = t_gh[e, r, :].astype(F32)
                sig = jax.nn.sigmoid(a)
                act = a * sig
                hid[e, s, r, :] = (act * b).astype(BF16)
                g_a[e, s, r, :] = (gh * b * sig * (1.0 + a * (1.0 - sig))).astype(BF16)
                g_b[e, s, r, :] = (gh * act).astype(BF16)
            parts.append((nt(g_a[e, s], w_gate[layer, e]) + nt(g_b[e, s], w_up[layer, e])).astype(BF16))
        ret[n_ret, ret_at(s)] = tn(pick, jnp.concatenate(parts, axis=0)).astype(BF16)

    def mix(p, base):
        acc[...] = base.astype(F32)

        def body(k, carry):
            s = order(k)

            @pl.when(k > 0)
            def _():
                ret_wait(0, p, s)

            for e in range(2):
                here = lane == s * 2 + e
                pos = jnp.sum(jnp.where(here, posc[p], 0.0), axis=1, keepdims=True)
                weight = jnp.sum(jnp.where(here, gatec[p], 0.0), axis=1, keepdims=True)
                hot = (pos == slot_lane).astype(F32).astype(BF16)
                acc[...] += nn(hot, ret[0, N_EP + p * N_EP + s, e * CAP:(e + 1) * CAP]) * weight
            return carry
        lax.fori_loop(0, N_EP, body, 0)
        return acc[...].astype(BF16)

    def add_up(n, p, base, n_from=N_EP):
        total = base.astype(F32) + ret[n, N_EP + p * N_EP + z].astype(F32)
        for k in range(1, n_from):
            ret_wait(n, p, order(k))
            total += ret[n, N_EP + p * N_EP + order(k)].astype(F32)
        return total.astype(BF16)

    chip_x = chip % 2
    chip_y = chip // 2
    over_x = chip + 1 - 2 * chip_x
    over_y = (chip + 2) % n_chip

    def group(e):
        return jnp.where(e == 0, chip_x, chip_y)

    def place(e):
        return jnp.where(e == 0, chip_y, chip_x)

    def pair_copy(layer, e, q):
        return row_copy(gs.at[1 - core, e, q], gr.at[layer, e, q], pair_send.at[layer, e, q], pair_recv.at[layer, e, q], chip * 2 + 1 - core)

    def one_copy(layer, e, q):
        return row_copy(gr.at[layer, e, q, 1 - group(e)], g2.at[layer, e, q], one_send.at[layer, e, q], one_recv.at[layer, e, q],
                        jnp.where(e == 0, over_x, over_y) * 2 + core)

    def two_copy(layer, e, q):
        return row_copy(gr.at[layer, e, q, group(e), 1 - place(e)], g3.at[layer, e, q], two_send.at[layer, e, q], two_recv.at[layer, e, q],
                        jnp.where(e == 0, over_y, over_x) * 2 + core)

    def pair_finish(layer, e, q):
        pair_copy(layer, e, q).wait()
        for g in range(2):
            for p in range(2):
                gr[layer, e, q, g, p] = (gr[layer, e, q, g, p].astype(F32) + gs[core, e, q, g, p].astype(F32)).astype(BF16)
        one_copy(layer, e, q).start()

    def one_finish(layer):
        def body(n, carry):
            e, q = n % 2, (n // 2 + 2) % 3
            one_copy(layer, e, q).wait_recv()
            for p in range(2):
                gr[layer, e, q, group(e), p] = (gr[layer, e, q, group(e), p].astype(F32) + g2[layer, e, q, p].astype(F32)).astype(BF16)
            two_copy(layer, e, q).start()
            return carry
        lax.fori_loop(0, 6, body, 0)

    def two_finish(layer):
        def body(n, carry):
            e, q = n % 2, (n // 2 + 2) % 3
            two_copy(layer, e, q).wait_recv()
            exp_v[layer, q * 2 + e] = (gr[layer, e, q, group(e), place(e)].astype(F32) + g3[layer, e, q].astype(F32)).astype(BF16)
            one_copy(layer, e, q).wait_send()
            two_copy(layer, e, q).wait_send()
            return carry
        lax.fori_loop(0, 6, body, 0)
        exp_copy(layer).start()

    def exp_copy(layer):
        return pltpu.make_async_copy(exp_v.at[layer], exp_out.at[layer], out_sem.at[layer])

    def operands(layer, e, at, n):
        rows = rows_in[layer, e, pl.ds(at, n)].reshape(n * CAP, d_model)
        outs = g_out[e, pl.ds(at, n)].reshape(n * CAP, d_model)
        return [(j, left, right[e, pl.ds(at, n)].reshape(n * CAP, d_ff))
                for j, left, right in ((2, outs, hid), (0, rows, g_a), (1, rows, g_b))]

    def weight_part(layer, at, n):
        def body(e, carry):
            for j, left, right in operands(layer, e, at, n):
                part[e, j] = tn(left, right)
            return carry
        lax.fori_loop(0, 2, body, 0)

    def split_grad(layer, e, j, grad):
        for p in range(n_dp):
            y, x = p // 4, p // 2 % 2
            gs[p % 2, e, j, jnp.where(e == 0, x, y), jnp.where(e == 0, y, x)] = grad[p * piece:(p + 1) * piece].astype(BF16)
        pair_copy(layer, e, j).start()

    def weight_grads(layer):
        def body(e, carry):
            for j, left, right in operands(layer, e, 0, N_EP):
                split_grad(layer, e, j, tn(left, right))
            return carry
        lax.fori_loop(0, 2, body, 0)
        for j in (2, 0, 1):
            for e in range(2):
                pair_finish(layer, e, j)

    def weight_rest(layer, at):
        both = [operands(layer, e, at, 2) for e in range(2)]
        todo = [(e, both[e][q]) for q in range(3) for e in range(2)]
        for k, (e, (j, left, right)) in enumerate(todo):
            split_grad(layer, e, j, tn(left, right) + part[e, j])
            if k >= 2:
                pair_finish(layer, todo[k - 2][0], todo[k - 2][1][0])
        for e, (j, _, _) in todo[4:]:
            pair_finish(layer, e, j)

    sub = piece // N_EP

    def da_copy(layer, k):
        to = (z + k) % N_EP
        return col_copy(d_send.at[layer, to], d_a.at[layer, z], da_send.at[layer, k], da_recv.at[layer, z], to)

    def db_copy(layer, k):
        to = (dp + k) % n_dp
        return row_copy(d_bs.at[layer, to], d_b.at[layer, dp], db_send.at[layer, k], db_recv.at[layer, dp], to)

    def dense_start(layer, grad):
        for q in range(N_EP):
            for p in range(n_dp):
                at = p * piece + q * sub
                d_send[layer, q, p] = grad[at:at + sub].astype(BF16)
        for k in range(1, N_EP):
            da_copy(layer, k).start()
        d_a[layer, z] = d_send[layer, z]

    def dense_middle(layer):
        for m in (1, 2):
            @pl.when(z != m)
            def _():
                col_copy(d_send.at[layer, m], d_a.at[layer, m], da_send.at[layer, 0], da_recv.at[layer, m], m).wait_recv()
        d_bs[layer] = (d_a[layer, 1].astype(F32) + d_a[layer, 2].astype(F32)).astype(BF16)
        for k in range(1, n_dp):
            db_copy(layer, k).start()

    def dense_end(layer):
        total = d_bs[layer, dp].astype(F32)
        for k in range(1, n_dp):
            frm = (dp + k) % n_dp
            row_copy(d_bs.at[layer, frm], d_b.at[layer, frm], db_send.at[layer, k], db_recv.at[layer, frm], frm).wait_recv()
            total += d_b[layer, frm].astype(F32)
        den_v[layer * sub:(layer + 1) * sub] = total.astype(BF16)
        @pl.when(inner)
        def _():
            for k in range(1, N_EP):
                da_copy(layer, k).wait_send()
        for k in range(1, n_dp):
            db_copy(layer, k).wait_send()

    def forward_step(k, carry):
        s = order(k)
        ag_step(0, k)
        with scope('f1'):
            forward(s)
        ret_start(0, s)
        return carry
    lax.fori_loop(0, N_EP, forward_step, 0)

    ag_pass(2, z, right=z != 1, left=z != 2)

    @pl.when(outer)
    def _():
        x_copy().start()

    @pl.when(inner)
    def _():
        ag_take(2, 3 - z)

        def body(n, carry):
            s = jnp.where(n == 0, z, near_end)
            ag[1, s] = mix(s % 2, ag[0, s])
            ag_pass(1, s)

            @pl.when(n == 1)
            def _():
                with scope('dyw'):
                    ag_to_right(2, s).wait_recv()
                ag_pass(2, s, right=z == 1, left=z == 2)
            return carry
        lax.fori_loop(0, 2, body, 0)

    def second_step(k, carry):
        s = order_owned(k)

        owned_step(1, k, s, False)

        @pl.when(jnp.logical_or(k > 2, jnp.logical_and(outer, s != z)))
        def _():
            ag_take(2, s)
        with scope('fb2'):
            backward(1, s, 2, 1, 1)
        ret_start(1, s)
        return carry
    lax.fori_loop(0, N_EP, second_step, 0)
    with scope('wg1'):
        weight_grads(1)

    @pl.when(inner)
    def _():
        def body(n, carry):
            s = jnp.where(n == 0, z, near_end)
            gm = add_up(1, s % 2, ag[2, s])
            g_mix[n] = gm
            ag[3, s] = (gm.astype(F32) + nt(gm, dense2[...])).astype(BF16)
            ag_pass(3, s)
            return carry
        lax.fori_loop(0, 2, body, 0)
        dense_start(1, tn(ag[1, z], g_mix[0]) + tn(ag[1, near_end], g_mix[1]))

    early_at = jnp.where(z < 2, 0, 2)
    late_at = 2 - early_at

    def first_step(k, carry):
        s = order_owned(k)

        @pl.when(jnp.logical_and(k == 2, outer))
        def _():
            with scope('wpart'):
                weight_part(0, early_at, 2)

        @pl.when(jnp.logical_and(k == 3, outer))
        def _():
            with scope('dmid1'):
                dense_middle(1)
            with scope('one1'):
                one_finish(1)
        owned_step(3, k, s, True)
        with scope('b1'):
            backward(0, s, 3, 2, None)

        @pl.when(k != 2)
        def _():
            ret_start(2, s)

        @pl.when(jnp.logical_and(k == 2, outer))
        def _():
            merge_copy().start()
        return carry
    lax.fori_loop(0, N_EP, first_step, 0)

    @pl.when(inner)
    def _():
        dense_middle(1)
        one_finish(1)
        weight_part(0, early_at, 2)
    with scope('wg0'):
        weight_rest(0, late_at)
    for n in range(3):
        ag_drain(n)
    for n in range(2):
        ret_drain(n)

    @pl.when(outer)
    def _():
        x_copy().wait_send()
    for k in range(1, N_EP):
        aux_copy(k).wait_send()
    @pl.when(inner)
    def _():
        with scope('merge'):
            merge_copy().wait_recv()
        other = 3 - z
        ret[2, other] = (ret[2, other].astype(F32) + merge_in[...].astype(F32)).astype(BF16)
        ret_copy(2, other).start()
    with scope('one0'):
        one_finish(0)
    with scope('two1'):
        two_finish(1)
    with scope('dend1'):
        dense_end(1)

    def dx_copy():
        return pltpu.make_async_copy(dx_v, tok_out.at[pl.ds(0, n_tok)], out_sem.at[2])

    @pl.when(inner)
    def _():
        gm = add_up(2, z % 2, ag[3, z], N_EP - 1)
        dx_v[...] = (gm.astype(F32) + nt(gm, dense1[...])).astype(BF16)
        dx_copy().start()
        ge = add_up(2, near_end % 2, ag[3, near_end])
        g_mix[0] = (ge.astype(F32) + nt(ge, dense1[...])).astype(BF16)
        x_copy().wait_recv()
        dense_start(0, tn(x_ref[...], gm) + tn(x_end[...], ge))
        dx_back().start()
    with scope('dmid0'):
        dense_middle(0)
    with scope('two0'):
        two_finish(0)

    @pl.when(outer)
    def _():
        with scope('dxw'):
            dx_back().wait_recv()
        merge_copy().wait_send()
    with scope('dend0'):
        dense_end(0)
    den_copy = pltpu.make_async_copy(den_v, tok_out.at[pl.ds(n_tok, 2 * sub)], out_sem.at[3])
    den_copy.start()
    ag_drain(3)
    ret_drain(2)

    @pl.when(inner)
    def _():
        dx_back().wait_send()
        dx_copy().wait()
    exp_copy(1).wait()
    exp_copy(0).wait()
    den_copy.wait()


def spread(n_tok, sub, tok, exp, *refs):
    outs, tok_v, exp_v, sem = refs[:9], refs[9], refs[10], refs[11]
    parts = [(tok, tok_v), (exp, exp_v)]
    for n, (src, dst) in enumerate(parts):
        pltpu.make_async_copy(src, dst, sem.at[n]).start()
    pltpu.make_async_copy(tok, tok_v, sem.at[0]).wait()
    copies = [(tok_v.at[pl.ds(0, n_tok)], outs[0])]
    for layer in range(2):
        copies.append((tok_v.at[pl.ds(n_tok + layer * sub, sub)], outs[1 + 4 * layer]))
    for layer in range(2):
        for q in range(3):
            copies.append((exp_v.at[layer, pl.ds(2 * q, 2)], outs[2 + 4 * layer + q]))
    for n, (src, dst) in enumerate(copies):
        if n == 3:
            pltpu.make_async_copy(exp, exp_v, sem.at[1]).wait()
        pltpu.make_async_copy(src, dst, sem.at[2 + n]).start()
    for n, (src, dst) in enumerate(copies):
        pltpu.make_async_copy(src, dst, sem.at[2 + n]).wait()


def solution(mesh):
    n_dp = mesh.shape['dp']
    n_chip = n_dp // 2
    tok_spec = P(('dp', 'ep'), None)
    exp_spec = P('ep', None, None)
    layer_specs = (P(None, None), tok_spec, tok_spec, exp_spec, exp_spec, exp_spec)
    grad_specs = (P(('dp', 'ep'), None), P('ep', 'dp', None), P('ep', 'dp', None), P('ep', None, 'dp'))

    def local_step(tokens, dy_out, dense_w1, idx1, gate1, wg1, wu1, wd1, dense_w2, idx2, gate2, wg2, wu2, wd2):
        n_tok, d_model = tokens.shape
        d_ff = wg1.shape[2]
        piece = d_model // n_dp
        sub = piece // N_EP
        vmem = pl.BlockSpec(memory_space=pltpu.VMEM)
        hbm = pl.BlockSpec(memory_space=pl.ANY)
        dma = pltpu.SemaphoreType.DMA
        six = (2, 2, 3)
        outs = pl.pallas_call(
            functools.partial(kernel, n_dp),
            out_shape=(jax.ShapeDtypeStruct((n_tok + 2 * sub, d_model), BF16), jax.ShapeDtypeStruct((2, 6, piece, d_ff), BF16)),
            in_specs=[vmem] * 8 + [hbm] * 6,
            out_specs=[hbm] * 2,
            scratch_shapes=[
                pltpu.VMEM((2, 2, d_model, d_ff), BF16), pltpu.VMEM((2, 2, d_model, d_ff), BF16), pltpu.VMEM((2, 2, d_ff, d_model), BF16),
                pltpu.VMEM((8, n_tok), F32), pltpu.VMEM((N_EP, 8, n_tok), F32), pltpu.VMEM((4 * N_EP, 1, n_tok), F32), pltpu.VMEM((4 * N_EP, 1, n_tok), F32),
                pltpu.VMEM((2, n_tok, N_EXP), F32), pltpu.VMEM((2, n_tok, N_EXP), F32), pltpu.VMEM((n_tok, n_tok), BF16),
                pltpu.VMEM((4, N_EP, n_tok, d_model), BF16), pltpu.VMEM((3, 3 * N_EP, n_tok, d_model), BF16),
                pltpu.VMEM((n_tok, d_model), BF16), pltpu.VMEM((n_tok, d_model), BF16),
                pltpu.VMEM((2, 2, N_EP, CAP, d_model), BF16), pltpu.VMEM((2, CAP, d_ff), F32), pltpu.VMEM((2, CAP, d_ff), F32),
                pltpu.VMEM((2, CAP, d_ff), BF16), pltpu.VMEM((2, N_EP, CAP, d_ff), BF16), pltpu.VMEM((2, N_EP, CAP, d_ff), BF16),
                pltpu.VMEM((2, N_EP, CAP, d_ff), BF16), pltpu.VMEM((2, N_EP, CAP, d_model), BF16),
                pltpu.VMEM((n_tok, d_model), F32), pltpu.VMEM((2, n_tok, d_model), BF16),
                pltpu.VMEM((2, 3, d_model, d_ff), F32),
                *[pltpu.VMEM(six + (2, 2, piece, d_ff), BF16)] * 2, pltpu.VMEM(six + (2, piece, d_ff), BF16), pltpu.VMEM(six + (piece, d_ff), BF16),
                pltpu.VMEM((2, N_EP, n_dp, sub, d_model), BF16), pltpu.VMEM((2, N_EP, n_dp, sub, d_model), BF16),
                pltpu.VMEM((2, n_dp, sub, d_model), BF16), pltpu.VMEM((2, n_dp, sub, d_model), BF16),
                pltpu.VMEM((2, 6, piece, d_ff), BF16), pltpu.VMEM((n_tok, d_model), BF16), pltpu.VMEM((2 * sub, d_model), BF16),
                dma((6,)), dma((N_EP,)), dma((N_EP,)), *[dma((4, N_EP))] * 3, dma((3, N_EP)), dma((3, 2 * N_EP)),
                dma((3,)), dma((3,)), *[dma(six)] * 6, *[dma((2, N_EP))] * 2, *[dma((2, n_dp))] * 2, dma((4,)),
            ],
            compiler_params=pltpu.CompilerParams(collective_id=0, has_side_effects=True, vmem_limit_bytes=67043328),
        )(tokens, dy_out, dense_w1, dense_w2, idx1.T, gate1.T, idx2.T, gate2.T, wg1, wu1, wd1, wg2, wu2, wd2)
        tok, exp = outs
        grads = [jax.ShapeDtypeStruct((sub, d_model), BF16)] + [jax.ShapeDtypeStruct((2, piece, d_ff), BF16)] * 3
        res = list(pl.pallas_call(
            functools.partial(spread, n_tok, sub),
            out_shape=tuple([jax.ShapeDtypeStruct((n_tok, d_model), BF16)] + grads * 2),
            in_specs=[hbm] * 2,
            out_specs=[hbm] * 9,
            scratch_shapes=[pltpu.VMEM((n_tok + 2 * sub, d_model), BF16), pltpu.VMEM((2, 6, piece, d_ff), BF16), dma((11,))],
        )(tok, exp))
        for n in (4, 8):
            res[n] = jnp.swapaxes(res[n], 1, 2)
        return tuple(res)

    return jax.shard_map(local_step, mesh=mesh, in_specs=(tok_spec, tok_spec) + layer_specs + layer_specs,
                         out_specs=(tok_spec,) + grad_specs + grad_specs, check_vma=False)
```

```python
import functools

import jax
import jax.numpy as jnp
from jax import lax
from jax.experimental import pallas as pl
from jax.experimental.pallas import tpu as pltpu
from jax.sharding import PartitionSpec as P

MESH = pl.DeviceIdType.MESH
F32, BF16 = jnp.float32, jnp.bfloat16
N_EP = 4
N_EXP = 8
CAP = 256


def nn(a, b):
    return lax.dot_general(a, b, (((1,), (0,)), ((), ())), preferred_element_type=F32)


def nt(a, b):
    return lax.dot_general(a, b, (((1,), (1,)), ((), ())), preferred_element_type=F32)


def tn(a, b):
    return lax.dot_general(a, b, (((0,), (0,)), ((), ())), preferred_element_type=F32)


def kernel(n_dp, x_ref, dy_ref, dense1, dense2, idx1, gate1, idx2, gate2,
           wg1_hbm, wu1_hbm, wd1_hbm, wg2_hbm, wu2_hbm, wd2_hbm,
           tok_out, exp_out,
           w_gate, w_up, w_down, auxs, auxb, posr, gater, posc, gatec, tri, ag, ret, x_end, merge_in, rows_in, t_a, t_b, t_gh, hid, g_a, g_b, g_out,
           acc, g_mix, part, gs, gr, g2, g3, d_send, d_a, d_bs, d_b, exp_v, dx_v, den_v,
           w_sem, aux_send, aux_recv, ag_right, ag_left, ag_recv, ret_send, ret_recv, end_send, end_recv, pair_send, pair_recv,
           one_send, one_recv, two_send, two_recv, da_send, da_recv, db_send, db_recv, out_sem):
    z = lax.axis_index('ep')
    dp = lax.axis_index('dp')
    n_chip = n_dp // 2
    core = dp % 2
    chip = dp // 2
    n_tok, d_model = x_ref.shape
    d_ff = t_a.shape[2]
    piece = d_model // n_dp

    def swapped(k):
        return jnp.where(k < 2, 1 - k, k)

    def order(k):
        low = jnp.where(jnp.logical_or(z == 1, z == 2), swapped(k), k)
        return jnp.where(z < 2, low, 3 - low)

    def order_owned(k):
        low = swapped(k)
        return jnp.where(z < 2, low, 3 - low)

    def owner(s):
        return jnp.where(s < 2, 1, 2)

    inner = jnp.logical_or(z == 1, z == 2)
    outer = jnp.logical_not(inner)
    near_mid = jnp.where(z < 2, 1, 2)
    near_end = jnp.where(z < 2, 0, 3)

    barrier = pltpu.get_barrier_semaphore()
    for k in range(1, N_EP):
        pl.semaphore_signal(barrier, inc=1, device_id={'ep': (z + k) % N_EP, 'dp': dp}, device_id_type=MESH)
    for k in range(1, n_dp):
        pl.semaphore_signal(barrier, inc=1, device_id={'ep': z, 'dp': (dp + k) % n_dp}, device_id_type=MESH)

    w_copies = []
    for n, (hbm, dst) in enumerate(((wg1_hbm, w_gate.at[0]), (wu1_hbm, w_up.at[0]), (wd1_hbm, w_down.at[0]),
                                    (wg2_hbm, w_gate.at[1]), (wu2_hbm, w_up.at[1]), (wd2_hbm, w_down.at[1]))):
        w_copies.append(pltpu.make_async_copy(hbm, dst, w_sem.at[n]))
        w_copies[-1].start()

    auxs[0:2] = idx1[...].astype(F32)
    auxs[2:4] = gate1[...]
    auxs[4:6] = idx2[...].astype(F32)
    auxs[6:8] = gate2[...]
    x = x_ref[...]
    ag[0, z] = (x.astype(F32) + nn(x, dense1[...])).astype(BF16)
    ag[2, z] = dy_ref[...]
    auxb[z] = auxs[...]

    pl.semaphore_wait(barrier, N_EP - 1 + n_dp - 1)

    def col_copy(src, dst, send, recv, to):
        return pltpu.make_async_remote_copy(src_ref=src, dst_ref=dst, send_sem=send, recv_sem=recv,
                                            device_id={'ep': to, 'dp': dp}, device_id_type=MESH)

    def row_copy(src, dst, send, recv, to):
        return pltpu.make_async_remote_copy(src_ref=src, dst_ref=dst, send_sem=send, recv_sem=recv,
                                            device_id={'ep': z, 'dp': to}, device_id_type=MESH)

    def aux_copy(k):
        return col_copy(auxs, auxb.at[z], aux_send.at[k], aux_recv.at[z], (z + k) % N_EP)

    for k in range(1, N_EP):
        aux_copy(k).start()

    def ag_to_right(n, s):
        return col_copy(ag.at[n, s], ag.at[n, s], ag_right.at[n, s], ag_recv.at[n, s], jnp.minimum(z + 1, N_EP - 1))

    def ag_to_left(n, s):
        return col_copy(ag.at[n, s], ag.at[n, s], ag_left.at[n, s], ag_recv.at[n, s], jnp.maximum(z - 1, 0))

    def rightward(n, s):
        return jnp.logical_and((owner(s) if n % 2 else s) <= z, z < N_EP - 1)

    def leftward(n, s):
        return jnp.logical_and((owner(s) if n % 2 else s) >= z, z > 0)

    def ag_pass(n, s, right=True, left=True):
        if right is not False:
            @pl.when(jnp.logical_and(rightward(n, s), right))
            def _():
                ag_to_right(n, s).start()

        if left is not False:
            @pl.when(jnp.logical_and(leftward(n, s), left))
            def _():
                ag_to_left(n, s).start()

    def ag_take(n, s):
        ag_to_right(n, s).wait_recv()
        ag_pass(n, s)

    def ag_step(n, k):
        @pl.when(k == 1)
        def _():
            ag_take(n, order(1))

        @pl.when(jnp.logical_or(jnp.logical_and(k == 1, inner), jnp.logical_and(k == 2, outer)))
        def _():
            ag_take(n, order(2))

        @pl.when(k == 3)
        def _():
            ag_take(n, order(3))

    def owned_step(n, k, s, early):
        if early:
            @pl.when(jnp.logical_and(k == 0, inner))
            def _():
                ag_take(n, order_owned(2))

            @pl.when(jnp.logical_and(k == 2, inner))
            def _():
                ag_take(n, order_owned(3))

        @pl.when(outer if early else jnp.logical_or(k > 1, outer))
        def _():
            ag_take(n, s)

    def ag_drain(n):
        def body(s, carry):
            @pl.when(rightward(n, s))
            def _():
                ag_to_right(n, s).wait_send()

            @pl.when(leftward(n, s))
            def _():
                ag_to_left(n, s).wait_send()
            return carry
        lax.fori_loop(0, N_EP, body, 0)

    def ret_at(s):
        return jnp.where(owner(s) == z, N_EP + s % 2 * N_EP + z, s)

    def ret_copy(n, s):
        return col_copy(ret.at[n, s], ret.at[n, N_EP + s % 2 * N_EP + z], ret_send.at[n, s], ret_recv.at[n, s % 2 * N_EP + z], owner(s))

    def ret_start(n, s):
        @pl.when(owner(s) != z)
        def _():
            ret_copy(n, s).start()

    def ret_wait(n, p, frm):
        at = p * N_EP + frm
        col_copy(ret.at[n, 0], ret.at[n, N_EP + at], ret_send.at[n, 0], ret_recv.at[n, at], z).wait_recv()

    def ret_drain(n):
        def body(s, carry):
            away = owner(s) != z

            @pl.when(jnp.logical_and(away, jnp.logical_or(inner, s != order_owned(2))) if n == 2 else away)
            def _():
                ret_copy(n, s).wait_send()
            return carry
        lax.fori_loop(0, N_EP, body, 0)

    def merge_copy():
        return col_copy(ret.at[2, order_owned(2)], merge_in, end_send.at[2], end_recv.at[2], near_mid)

    def x_copy():
        return col_copy(x_ref, x_end, end_send.at[0], end_recv.at[0], near_mid)

    def dx_back():
        return col_copy(g_mix.at[0], dx_v, end_send.at[1], end_recv.at[1], near_end)

    ag_pass(0, z)
    ag_pass(2, z, right=z == 1, left=z == 2)

    r_io = lax.broadcasted_iota(jnp.int32, (n_tok, n_tok), 0)
    c_io = lax.broadcasted_iota(jnp.int32, (n_tok, n_tok), 1)
    tri[...] = (c_io < r_io).astype(F32).astype(BF16)
    lane = lax.broadcasted_iota(jnp.int32, (n_tok, N_EXP), 1)
    for k in range(1, N_EP):
        s = (z + k) % N_EP
        col_copy(auxs, auxb.at[s], aux_send.at[k], aux_recv.at[s], s).wait_recv()
    for p in range(2):
        cols = auxb[jnp.where(z < 2, 0, 2) + p].T
        hit0 = cols[:, 0:1] == lane.astype(F32)
        hit1 = cols[:, 1:2] == lane.astype(F32)
        hit = jnp.logical_or(hit0, hit1)
        rank = nn(tri[...], hit.astype(F32).astype(BF16))
        posc[p] = jnp.where(hit, rank, -1.0)
        gatec[p] = jnp.where(hit0, cols[:, 2:3], 0.0) + jnp.where(hit1, cols[:, 3:4], 0.0)
    hits = []
    for layer in range(2):
        for s in range(N_EP):
            for e in range(2):
                a = auxb[s]
                expert = (z * 2 + e).astype(F32)
                hit0 = a[4 * layer:4 * layer + 1] == expert
                hit1 = a[4 * layer + 1:4 * layer + 2] == expert
                hits.append(jnp.logical_or(hit0, hit1).astype(F32))
                gater[(layer * N_EP + s) * 2 + e] = (jnp.where(hit0, a[4 * layer + 2:4 * layer + 3], 0.0)
                                                     + jnp.where(hit1, a[4 * layer + 3:4 * layer + 4], 0.0))
    stack = jnp.concatenate(hits, axis=0)
    ranks = jnp.where(stack > 0.5, nt(stack.astype(BF16), tri[...]), -1.0)
    for n in range(4 * N_EP):
        posr[n] = ranks[n:n + 1]

    for copy in w_copies:
        copy.wait()

    slot = lax.broadcasted_iota(jnp.int32, (CAP, n_tok), 0).astype(F32)
    slot_lane = lax.broadcasted_iota(jnp.int32, (n_tok, CAP), 1).astype(F32)
    step = 32

    def select(layer, s):
        at = (layer * N_EP + s) * 2
        return [posr[at + e] == slot for e in range(2)]

    def as_bf16(picks):
        return jnp.concatenate([p.astype(F32).astype(BF16) for p in picks], axis=0)

    def take_rows(layer, s, n, pick):
        u = ag[n, s]
        if n == 1:
            u = (u.astype(F32) + nn(u, dense2[...])).astype(BF16)
        rows = nn(pick, u).astype(BF16)
        for e in range(2):
            rows_in[layer, e, s] = rows[e * CAP:(e + 1) * CAP]

    def up_project(layer, s, e):
        rows = rows_in[layer, e, s]
        t_a[e] = nn(rows, w_gate[layer, e])
        t_b[e] = nn(rows, w_up[layer, e])

    def forward(s):
        take_rows(0, s, 0, as_bf16(select(0, s)))
        for e in range(2):
            up_project(0, s, e)
        for e in range(2):
            for i in range(CAP // step):
                r = pl.ds(i * step, step)
                a = t_a[e, r, :]
                hid[e, s, r, :] = (a * jax.nn.sigmoid(a) * t_b[e, r, :]).astype(BF16)
            ret[0, ret_at(s), e * CAP:(e + 1) * CAP] = nn(hid[e, s], w_down[0, e]).astype(BF16)

    def backward(layer, s, n_dy, n_ret, n_u):
        picks = select(layer, s)
        pick = as_bf16(picks)
        at = (layer * N_EP + s) * 2
        if n_u is not None:
            take_rows(layer, s, n_u, pick)
        got = nn(pick, ag[n_dy, s])
        for e in range(2):
            gate = jnp.sum(jnp.where(picks[e], gater[at + e], 0.0), axis=1, keepdims=True)
            g_out[e, s] = (got[e * CAP:(e + 1) * CAP] * gate).astype(BF16)
        for e in range(2):
            up_project(layer, s, e)
            t_gh[e] = nt(g_out[e, s], w_down[layer, e]).astype(BF16)
        parts = []
        for e in range(2):
            for i in range(CAP // step):
                r = pl.ds(i * step, step)
                a = t_a[e, r, :]
                b = t_b[e, r, :]
                gh = t_gh[e, r, :].astype(F32)
                sig = jax.nn.sigmoid(a)
                act = a * sig
                hid[e, s, r, :] = (act * b).astype(BF16)
                g_a[e, s, r, :] = (gh * b * sig * (1.0 + a * (1.0 - sig))).astype(BF16)
                g_b[e, s, r, :] = (gh * act).astype(BF16)
            parts.append((nt(g_a[e, s], w_gate[layer, e]) + nt(g_b[e, s], w_up[layer, e])).astype(BF16))
        ret[n_ret, ret_at(s)] = tn(pick, jnp.concatenate(parts, axis=0)).astype(BF16)

    def mix(p, base):
        acc[...] = base.astype(F32)

        def body(k, carry):
            s = order(k)

            @pl.when(k > 0)
            def _():
                ret_wait(0, p, s)

            for e in range(2):
                here = lane == s * 2 + e
                pos = jnp.sum(jnp.where(here, posc[p], 0.0), axis=1, keepdims=True)
                weight = jnp.sum(jnp.where(here, gatec[p], 0.0), axis=1, keepdims=True)
                hot = (pos == slot_lane).astype(F32).astype(BF16)
                acc[...] += nn(hot, ret[0, N_EP + p * N_EP + s, e * CAP:(e + 1) * CAP]) * weight
            return carry
        lax.fori_loop(0, N_EP, body, 0)
        return acc[...].astype(BF16)

    def add_up(n, p, base, n_from=N_EP):
        total = base.astype(F32) + ret[n, N_EP + p * N_EP + z].astype(F32)
        for k in range(1, n_from):
            ret_wait(n, p, order(k))
            total += ret[n, N_EP + p * N_EP + order(k)].astype(F32)
        return total.astype(BF16)

    chip_x = chip % 2
    chip_y = chip // 2
    over_x = chip + 1 - 2 * chip_x
    over_y = (chip + 2) % n_chip

    def group(e):
        return jnp.where(e == 0, chip_x, chip_y)

    def place(e):
        return jnp.where(e == 0, chip_y, chip_x)

    def pair_copy(layer, e, q):
        return row_copy(gs.at[1 - core, e, q], gr.at[layer, e, q], pair_send.at[layer, e, q], pair_recv.at[layer, e, q], chip * 2 + 1 - core)

    def one_copy(layer, e, q):
        return row_copy(gr.at[layer, e, q, 1 - group(e)], g2.at[layer, e, q], one_send.at[layer, e, q], one_recv.at[layer, e, q],
                        jnp.where(e == 0, over_x, over_y) * 2 + core)

    def two_copy(layer, e, q):
        return row_copy(gr.at[layer, e, q, group(e), 1 - place(e)], g3.at[layer, e, q], two_send.at[layer, e, q], two_recv.at[layer, e, q],
                        jnp.where(e == 0, over_y, over_x) * 2 + core)

    def pair_finish(layer, e, q):
        pair_copy(layer, e, q).wait()
        for g in range(2):
            for p in range(2):
                gr[layer, e, q, g, p] = (gr[layer, e, q, g, p].astype(F32) + gs[core, e, q, g, p].astype(F32)).astype(BF16)
        one_copy(layer, e, q).start()

    def one_finish(layer):
        def body(n, carry):
            e, q = n % 2, (n // 2 + 2) % 3
            one_copy(layer, e, q).wait_recv()
            for p in range(2):
                gr[layer, e, q, group(e), p] = (gr[layer, e, q, group(e), p].astype(F32) + g2[layer, e, q, p].astype(F32)).astype(BF16)
            two_copy(layer, e, q).start()
            return carry
        lax.fori_loop(0, 6, body, 0)

    def two_finish(layer):
        def body(n, carry):
            e, q = n % 2, (n // 2 + 2) % 3
            two_copy(layer, e, q).wait_recv()
            exp_v[layer, q * 2 + e] = (gr[layer, e, q, group(e), place(e)].astype(F32) + g3[layer, e, q].astype(F32)).astype(BF16)
            one_copy(layer, e, q).wait_send()
            two_copy(layer, e, q).wait_send()
            return carry
        lax.fori_loop(0, 6, body, 0)
        exp_copy(layer).start()

    def exp_copy(layer):
        return pltpu.make_async_copy(exp_v.at[layer], exp_out.at[layer], out_sem.at[layer])

    def operands(layer, e, at, n):
        rows = rows_in[layer, e, pl.ds(at, n)].reshape(n * CAP, d_model)
        outs = g_out[e, pl.ds(at, n)].reshape(n * CAP, d_model)
        return [(j, left, right[e, pl.ds(at, n)].reshape(n * CAP, d_ff))
                for j, left, right in ((2, outs, hid), (0, rows, g_a), (1, rows, g_b))]

    def weight_part(layer, at, n):
        def body(e, carry):
            for j, left, right in operands(layer, e, at, n):
                part[e, j] = tn(left, right)
            return carry
        lax.fori_loop(0, 2, body, 0)

    def split_grad(layer, e, j, grad):
        for p in range(n_dp):
            y, x = p // 4, p // 2 % 2
            gs[p % 2, e, j, jnp.where(e == 0, x, y), jnp.where(e == 0, y, x)] = grad[p * piece:(p + 1) * piece].astype(BF16)
        pair_copy(layer, e, j).start()

    def weight_grads(layer):
        def body(e, carry):
            for j, left, right in operands(layer, e, 0, N_EP):
                split_grad(layer, e, j, tn(left, right))
            return carry
        lax.fori_loop(0, 2, body, 0)
        for j in (2, 0, 1):
            for e in range(2):
                pair_finish(layer, e, j)

    def weight_rest(layer, at):
        both = [operands(layer, e, at, 2) for e in range(2)]
        todo = [(e, both[e][q]) for q in range(3) for e in range(2)]
        for k, (e, (j, left, right)) in enumerate(todo):
            split_grad(layer, e, j, tn(left, right) + part[e, j])
            if k >= 2:
                pair_finish(layer, todo[k - 2][0], todo[k - 2][1][0])
        for e, (j, _, _) in todo[4:]:
            pair_finish(layer, e, j)

    sub = piece // N_EP

    def da_copy(layer, k):
        to = (z + k) % N_EP
        return col_copy(d_send.at[layer, to], d_a.at[layer, z], da_send.at[layer, k], da_recv.at[layer, z], to)

    def db_copy(layer, k):
        to = (dp + k) % n_dp
        return row_copy(d_bs.at[layer, to], d_b.at[layer, dp], db_send.at[layer, k], db_recv.at[layer, dp], to)

    def dense_start(layer, grad):
        for q in range(N_EP):
            for p in range(n_dp):
                at = p * piece + q * sub
                d_send[layer, q, p] = grad[at:at + sub].astype(BF16)
        for k in range(1, N_EP):
            da_copy(layer, k).start()
        d_a[layer, z] = d_send[layer, z]

    def dense_middle(layer):
        for m in (1, 2):
            @pl.when(z != m)
            def _():
                col_copy(d_send.at[layer, m], d_a.at[layer, m], da_send.at[layer, 0], da_recv.at[layer, m], m).wait_recv()
        d_bs[layer] = (d_a[layer, 1].astype(F32) + d_a[layer, 2].astype(F32)).astype(BF16)
        for k in range(1, n_dp):
            db_copy(layer, k).start()

    def dense_end(layer):
        total = d_bs[layer, dp].astype(F32)
        for k in range(1, n_dp):
            frm = (dp + k) % n_dp
            row_copy(d_bs.at[layer, frm], d_b.at[layer, frm], db_send.at[layer, k], db_recv.at[layer, frm], frm).wait_recv()
            total += d_b[layer, frm].astype(F32)
        den_v[layer * sub:(layer + 1) * sub] = total.astype(BF16)
        @pl.when(inner)
        def _():
            for k in range(1, N_EP):
                da_copy(layer, k).wait_send()
        for k in range(1, n_dp):
            db_copy(layer, k).wait_send()

    def forward_step(k, carry):
        s = order(k)
        ag_step(0, k)
        forward(s)
        ret_start(0, s)
        return carry
    lax.fori_loop(0, N_EP, forward_step, 0)

    ag_pass(2, z, right=z != 1, left=z != 2)

    @pl.when(outer)
    def _():
        x_copy().start()

    @pl.when(inner)
    def _():
        ag_take(2, 3 - z)

        def body(n, carry):
            s = jnp.where(n == 0, z, near_end)
            ag[1, s] = mix(s % 2, ag[0, s])
            ag_pass(1, s)

            @pl.when(n == 1)
            def _():
                ag_to_right(2, s).wait_recv()
                ag_pass(2, s, right=z == 1, left=z == 2)
            return carry
        lax.fori_loop(0, 2, body, 0)

    def second_step(k, carry):
        s = order_owned(k)

        owned_step(1, k, s, False)

        @pl.when(jnp.logical_or(k > 2, jnp.logical_and(outer, s != z)))
        def _():
            ag_take(2, s)
        backward(1, s, 2, 1, 1)
        ret_start(1, s)
        return carry
    lax.fori_loop(0, N_EP, second_step, 0)
    weight_grads(1)

    @pl.when(inner)
    def _():
        def body(n, carry):
            s = jnp.where(n == 0, z, near_end)
            gm = add_up(1, s % 2, ag[2, s])
            g_mix[n] = gm
            ag[3, s] = (gm.astype(F32) + nt(gm, dense2[...])).astype(BF16)
            ag_pass(3, s)
            return carry
        lax.fori_loop(0, 2, body, 0)
        dense_start(1, tn(ag[1, z], g_mix[0]) + tn(ag[1, near_end], g_mix[1]))

    early_at = jnp.where(z < 2, 0, 2)
    late_at = 2 - early_at

    def first_step(k, carry):
        s = order_owned(k)

        @pl.when(jnp.logical_and(k == 2, outer))
        def _():
            weight_part(0, early_at, 2)

        @pl.when(jnp.logical_and(k == 3, outer))
        def _():
            dense_middle(1)
            one_finish(1)
        owned_step(3, k, s, True)
        backward(0, s, 3, 2, None)

        @pl.when(k != 2)
        def _():
            ret_start(2, s)

        @pl.when(jnp.logical_and(k == 2, outer))
        def _():
            merge_copy().start()
        return carry
    lax.fori_loop(0, N_EP, first_step, 0)

    @pl.when(inner)
    def _():
        dense_middle(1)
        one_finish(1)
        weight_part(0, early_at, 2)
    weight_rest(0, late_at)
    for n in range(3):
        ag_drain(n)
    for n in range(2):
        ret_drain(n)

    @pl.when(outer)
    def _():
        x_copy().wait_send()
    for k in range(1, N_EP):
        aux_copy(k).wait_send()
    @pl.when(inner)
    def _():
        merge_copy().wait_recv()
        other = 3 - z
        ret[2, other] = (ret[2, other].astype(F32) + merge_in[...].astype(F32)).astype(BF16)
        ret_copy(2, other).start()
    one_finish(0)
    two_finish(1)
    dense_end(1)

    def dx_copy():
        return pltpu.make_async_copy(dx_v, tok_out.at[pl.ds(0, n_tok)], out_sem.at[2])

    @pl.when(inner)
    def _():
        gm = add_up(2, z % 2, ag[3, z], N_EP - 1)
        dx_v[...] = (gm.astype(F32) + nt(gm, dense1[...])).astype(BF16)
        dx_copy().start()
        ge = add_up(2, near_end % 2, ag[3, near_end])
        g_mix[0] = (ge.astype(F32) + nt(ge, dense1[...])).astype(BF16)
        x_copy().wait_recv()
        dense_start(0, tn(x_ref[...], gm) + tn(x_end[...], ge))
        dx_back().start()
    dense_middle(0)
    two_finish(0)

    @pl.when(outer)
    def _():
        dx_back().wait_recv()
        dx_copy().start()
        merge_copy().wait_send()
    dense_end(0)
    den_copy = pltpu.make_async_copy(den_v, tok_out.at[pl.ds(n_tok, 2 * sub)], out_sem.at[3])
    den_copy.start()
    ag_drain(3)
    ret_drain(2)

    @pl.when(inner)
    def _():
        dx_back().wait_send()
    exp_copy(1).wait()
    exp_copy(0).wait()
    dx_copy().wait()
    den_copy.wait()


def spread(n_tok, sub, tok, exp, *refs):
    outs, tok_v, exp_v, sem = refs[:9], refs[9], refs[10], refs[11]
    parts = [(tok, tok_v), (exp, exp_v)]
    for n, (src, dst) in enumerate(parts):
        pltpu.make_async_copy(src, dst, sem.at[n]).start()
    pltpu.make_async_copy(tok, tok_v, sem.at[0]).wait()
    copies = [(tok_v.at[pl.ds(0, n_tok)], outs[0])]
    for layer in range(2):
        copies.append((tok_v.at[pl.ds(n_tok + layer * sub, sub)], outs[1 + 4 * layer]))
    for layer in range(2):
        for q in range(3):
            copies.append((exp_v.at[layer, pl.ds(2 * q, 2)], outs[2 + 4 * layer + q]))
    for n, (src, dst) in enumerate(copies):
        if n == 3:
            pltpu.make_async_copy(exp, exp_v, sem.at[1]).wait()
        pltpu.make_async_copy(src, dst, sem.at[2 + n]).start()
    for n, (src, dst) in enumerate(copies):
        pltpu.make_async_copy(src, dst, sem.at[2 + n]).wait()


def solution(mesh):
    n_dp = mesh.shape['dp']
    n_chip = n_dp // 2
    tok_spec = P(('dp', 'ep'), None)
    exp_spec = P('ep', None, None)
    layer_specs = (P(None, None), tok_spec, tok_spec, exp_spec, exp_spec, exp_spec)
    grad_specs = (P(('dp', 'ep'), None), P('ep', 'dp', None), P('ep', 'dp', None), P('ep', None, 'dp'))

    def local_step(tokens, dy_out, dense_w1, idx1, gate1, wg1, wu1, wd1, dense_w2, idx2, gate2, wg2, wu2, wd2):
        n_tok, d_model = tokens.shape
        d_ff = wg1.shape[2]
        piece = d_model // n_dp
        sub = piece // N_EP
        vmem = pl.BlockSpec(memory_space=pltpu.VMEM)
        hbm = pl.BlockSpec(memory_space=pl.ANY)
        dma = pltpu.SemaphoreType.DMA
        six = (2, 2, 3)
        outs = pl.pallas_call(
            functools.partial(kernel, n_dp),
            out_shape=(jax.ShapeDtypeStruct((n_tok + 2 * sub, d_model), BF16), jax.ShapeDtypeStruct((2, 6, piece, d_ff), BF16)),
            in_specs=[vmem] * 8 + [hbm] * 6,
            out_specs=[hbm] * 2,
            scratch_shapes=[
                pltpu.VMEM((2, 2, d_model, d_ff), BF16), pltpu.VMEM((2, 2, d_model, d_ff), BF16), pltpu.VMEM((2, 2, d_ff, d_model), BF16),
                pltpu.VMEM((8, n_tok), F32), pltpu.VMEM((N_EP, 8, n_tok), F32), pltpu.VMEM((4 * N_EP, 1, n_tok), F32), pltpu.VMEM((4 * N_EP, 1, n_tok), F32),
                pltpu.VMEM((2, n_tok, N_EXP), F32), pltpu.VMEM((2, n_tok, N_EXP), F32), pltpu.VMEM((n_tok, n_tok), BF16),
                pltpu.VMEM((4, N_EP, n_tok, d_model), BF16), pltpu.VMEM((3, 3 * N_EP, n_tok, d_model), BF16),
                pltpu.VMEM((n_tok, d_model), BF16), pltpu.VMEM((n_tok, d_model), BF16),
                pltpu.VMEM((2, 2, N_EP, CAP, d_model), BF16), pltpu.VMEM((2, CAP, d_ff), F32), pltpu.VMEM((2, CAP, d_ff), F32),
                pltpu.VMEM((2, CAP, d_ff), BF16), pltpu.VMEM((2, N_EP, CAP, d_ff), BF16), pltpu.VMEM((2, N_EP, CAP, d_ff), BF16),
                pltpu.VMEM((2, N_EP, CAP, d_ff), BF16), pltpu.VMEM((2, N_EP, CAP, d_model), BF16),
                pltpu.VMEM((n_tok, d_model), F32), pltpu.VMEM((2, n_tok, d_model), BF16),
                pltpu.VMEM((2, 3, d_model, d_ff), F32),
                *[pltpu.VMEM(six + (2, 2, piece, d_ff), BF16)] * 2, pltpu.VMEM(six + (2, piece, d_ff), BF16), pltpu.VMEM(six + (piece, d_ff), BF16),
                pltpu.VMEM((2, N_EP, n_dp, sub, d_model), BF16), pltpu.VMEM((2, N_EP, n_dp, sub, d_model), BF16),
                pltpu.VMEM((2, n_dp, sub, d_model), BF16), pltpu.VMEM((2, n_dp, sub, d_model), BF16),
                pltpu.VMEM((2, 6, piece, d_ff), BF16), pltpu.VMEM((n_tok, d_model), BF16), pltpu.VMEM((2 * sub, d_model), BF16),
                dma((6,)), dma((N_EP,)), dma((N_EP,)), *[dma((4, N_EP))] * 3, dma((3, N_EP)), dma((3, 2 * N_EP)),
                dma((3,)), dma((3,)), *[dma(six)] * 6, *[dma((2, N_EP))] * 2, *[dma((2, n_dp))] * 2, dma((4,)),
            ],
            compiler_params=pltpu.CompilerParams(collective_id=0, has_side_effects=True, vmem_limit_bytes=67043328),
        )(tokens, dy_out, dense_w1, dense_w2, idx1.T, gate1.T, idx2.T, gate2.T, wg1, wu1, wd1, wg2, wu2, wd2)
        tok, exp = outs
        grads = [jax.ShapeDtypeStruct((sub, d_model), BF16)] + [jax.ShapeDtypeStruct((2, piece, d_ff), BF16)] * 3
        res = list(pl.pallas_call(
            functools.partial(spread, n_tok, sub),
            out_shape=tuple([jax.ShapeDtypeStruct((n_tok, d_model), BF16)] + grads * 2),
            in_specs=[hbm] * 2,
            out_specs=[hbm] * 9,
            scratch_shapes=[pltpu.VMEM((n_tok + 2 * sub, d_model), BF16), pltpu.VMEM((2, 6, piece, d_ff), BF16), dma((11,))],
        )(tok, exp))
        for n in (4, 8):
            res[n] = jnp.swapaxes(res[n], 1, 2)
        return tuple(res)

    return jax.shard_map(local_step, mesh=mesh, in_specs=(tok_spec, tok_spec) + layer_specs + layer_specs,
                         out_specs=(tok_spec,) + grad_specs + grad_specs, check_vma=False)
```

```python
import functools

import jax
import jax.numpy as jnp
from jax import lax
from jax.experimental import pallas as pl
from jax.experimental.pallas import tpu as pltpu
from jax.sharding import PartitionSpec as P

MESH = pl.DeviceIdType.MESH
F32, BF16 = jnp.float32, jnp.bfloat16
N_EP = 4
N_EXP = 8
CAP = 256


def nn(a, b):
    return lax.dot_general(a, b, (((1,), (0,)), ((), ())), preferred_element_type=F32)


def nt(a, b):
    return lax.dot_general(a, b, (((1,), (1,)), ((), ())), preferred_element_type=F32)


def tn(a, b):
    return lax.dot_general(a, b, (((0,), (0,)), ((), ())), preferred_element_type=F32)


def kernel(n_dp, x_ref, dy_ref, dense1, dense2, idx1, gate1, idx2, gate2,
           wg1_hbm, wu1_hbm, wd1_hbm, wg2_hbm, wu2_hbm, wd2_hbm,
           tok_out, exp_out,
           w_gate, w_up, w_down, auxs, auxb, posr, gater, posc, gatec, tri, ag, ret, x_end, merge_in, rows_in, t_a, t_b, t_gh, hid, g_a, g_b, g_out,
           acc, g_mix, part, gs, gr, g2, g3, d_send, d_a, d_bs, d_b, exp_v, dx_v, den_v,
           w_sem, aux_send, aux_recv, ag_right, ag_left, ag_recv, ret_send, ret_recv, end_send, end_recv, pair_send, pair_recv,
           one_send, one_recv, two_send, two_recv, da_send, da_recv, db_send, db_recv, out_sem):
    z = lax.axis_index('ep')
    dp = lax.axis_index('dp')
    n_chip = n_dp // 2
    core = dp % 2
    chip = dp // 2
    n_tok, d_model = x_ref.shape
    d_ff = t_a.shape[2]
    piece = d_model // n_dp

    def swapped(k):
        return jnp.where(k < 2, 1 - k, k)

    def order(k):
        low = jnp.where(jnp.logical_or(z == 1, z == 2), swapped(k), k)
        return jnp.where(z < 2, low, 3 - low)

    def order_owned(k):
        low = swapped(k)
        return jnp.where(z < 2, low, 3 - low)

    def owner(s):
        return jnp.where(s < 2, 1, 2)

    inner = jnp.logical_or(z == 1, z == 2)
    outer = jnp.logical_not(inner)
    near_mid = jnp.where(z < 2, 1, 2)
    near_end = jnp.where(z < 2, 0, 3)

    barrier = pltpu.get_barrier_semaphore()
    for k in range(1, N_EP):
        pl.semaphore_signal(barrier, inc=1, device_id={'ep': (z + k) % N_EP, 'dp': dp}, device_id_type=MESH)
    for k in range(1, n_dp):
        pl.semaphore_signal(barrier, inc=1, device_id={'ep': z, 'dp': (dp + k) % n_dp}, device_id_type=MESH)

    w_copies = []
    for n, (hbm, dst) in enumerate(((wg1_hbm, w_gate.at[0]), (wu1_hbm, w_up.at[0]), (wd1_hbm, w_down.at[0]),
                                    (wg2_hbm, w_gate.at[1]), (wu2_hbm, w_up.at[1]), (wd2_hbm, w_down.at[1]))):
        w_copies.append(pltpu.make_async_copy(hbm, dst, w_sem.at[n]))
        w_copies[-1].start()

    auxs[0:2] = idx1[...].astype(F32)
    auxs[2:4] = gate1[...]
    auxs[4:6] = idx2[...].astype(F32)
    auxs[6:8] = gate2[...]
    x = x_ref[...]
    ag[0, z] = (x.astype(F32) + nn(x, dense1[...])).astype(BF16)
    ag[2, z] = dy_ref[...]
    auxb[z] = auxs[...]

    pl.semaphore_wait(barrier, N_EP - 1 + n_dp - 1)

    def col_copy(src, dst, send, recv, to):
        return pltpu.make_async_remote_copy(src_ref=src, dst_ref=dst, send_sem=send, recv_sem=recv,
                                            device_id={'ep': to, 'dp': dp}, device_id_type=MESH)

    def row_copy(src, dst, send, recv, to):
        return pltpu.make_async_remote_copy(src_ref=src, dst_ref=dst, send_sem=send, recv_sem=recv,
                                            device_id={'ep': z, 'dp': to}, device_id_type=MESH)

    def aux_copy(k):
        return col_copy(auxs, auxb.at[z], aux_send.at[k], aux_recv.at[z], (z + k) % N_EP)

    for k in range(1, N_EP):
        aux_copy(k).start()

    def ag_to_right(n, s):
        return col_copy(ag.at[n, s], ag.at[n, s], ag_right.at[n, s], ag_recv.at[n, s], jnp.minimum(z + 1, N_EP - 1))

    def ag_to_left(n, s):
        return col_copy(ag.at[n, s], ag.at[n, s], ag_left.at[n, s], ag_recv.at[n, s], jnp.maximum(z - 1, 0))

    def rightward(n, s):
        return jnp.logical_and((owner(s) if n % 2 else s) <= z, z < N_EP - 1)

    def leftward(n, s):
        return jnp.logical_and((owner(s) if n % 2 else s) >= z, z > 0)

    def ag_pass(n, s, right=True, left=True):
        if right is not False:
            @pl.when(jnp.logical_and(rightward(n, s), right))
            def _():
                ag_to_right(n, s).start()

        if left is not False:
            @pl.when(jnp.logical_and(leftward(n, s), left))
            def _():
                ag_to_left(n, s).start()

    def ag_take(n, s):
        ag_to_right(n, s).wait_recv()
        ag_pass(n, s)

    def ag_step(n, k):
        @pl.when(k == 1)
        def _():
            ag_take(n, order(1))

        @pl.when(jnp.logical_or(jnp.logical_and(k == 1, inner), jnp.logical_and(k == 2, outer)))
        def _():
            ag_take(n, order(2))

        @pl.when(k == 3)
        def _():
            ag_take(n, order(3))

    def owned_step(n, k, s, early):
        if early:
            @pl.when(jnp.logical_and(k == 1, inner))
            def _():
                ag_take(n, order_owned(2))

            @pl.when(jnp.logical_and(k == 3, inner))
            def _():
                ag_take(n, order_owned(3))

        @pl.when(outer if early else jnp.logical_or(k > 1, outer))
        def _():
            ag_take(n, s)

    def ag_drain(n):
        def body(s, carry):
            @pl.when(rightward(n, s))
            def _():
                ag_to_right(n, s).wait_send()

            @pl.when(leftward(n, s))
            def _():
                ag_to_left(n, s).wait_send()
            return carry
        lax.fori_loop(0, N_EP, body, 0)

    def ret_at(s):
        return jnp.where(owner(s) == z, N_EP + s % 2 * N_EP + z, s)

    def ret_copy(n, s):
        return col_copy(ret.at[n, s], ret.at[n, N_EP + s % 2 * N_EP + z], ret_send.at[n, s], ret_recv.at[n, s % 2 * N_EP + z], owner(s))

    def ret_start(n, s):
        @pl.when(owner(s) != z)
        def _():
            ret_copy(n, s).start()

    def ret_wait(n, p, frm):
        at = p * N_EP + frm
        col_copy(ret.at[n, 0], ret.at[n, N_EP + at], ret_send.at[n, 0], ret_recv.at[n, at], z).wait_recv()

    def ret_drain(n):
        def body(s, carry):
            away = owner(s) != z

            @pl.when(jnp.logical_and(away, jnp.logical_or(inner, s != order_owned(2))) if n == 2 else away)
            def _():
                ret_copy(n, s).wait_send()
            return carry
        lax.fori_loop(0, N_EP, body, 0)

    def merge_copy():
        return col_copy(ret.at[2, order_owned(2)], merge_in, end_send.at[2], end_recv.at[2], near_mid)

    def x_copy():
        return col_copy(x_ref, x_end, end_send.at[0], end_recv.at[0], near_mid)

    def dx_back():
        return col_copy(g_mix.at[0], dx_v, end_send.at[1], end_recv.at[1], near_end)

    ag_pass(0, z)
    ag_pass(2, z, right=z == 1, left=z == 2)

    r_io = lax.broadcasted_iota(jnp.int32, (n_tok, n_tok), 0)
    c_io = lax.broadcasted_iota(jnp.int32, (n_tok, n_tok), 1)
    tri[...] = (c_io < r_io).astype(F32).astype(BF16)
    lane = lax.broadcasted_iota(jnp.int32, (n_tok, N_EXP), 1)
    for k in range(1, N_EP):
        s = (z + k) % N_EP
        col_copy(auxs, auxb.at[s], aux_send.at[k], aux_recv.at[s], s).wait_recv()
    for p in range(2):
        cols = auxb[jnp.where(z < 2, 0, 2) + p].T
        hit0 = cols[:, 0:1] == lane.astype(F32)
        hit1 = cols[:, 1:2] == lane.astype(F32)
        hit = jnp.logical_or(hit0, hit1)
        rank = nn(tri[...], hit.astype(F32).astype(BF16))
        posc[p] = jnp.where(hit, rank, -1.0)
        gatec[p] = jnp.where(hit0, cols[:, 2:3], 0.0) + jnp.where(hit1, cols[:, 3:4], 0.0)
    hits = []
    for layer in range(2):
        for s in range(N_EP):
            for e in range(2):
                a = auxb[s]
                expert = (z * 2 + e).astype(F32)
                hit0 = a[4 * layer:4 * layer + 1] == expert
                hit1 = a[4 * layer + 1:4 * layer + 2] == expert
                hits.append(jnp.logical_or(hit0, hit1).astype(F32))
                gater[(layer * N_EP + s) * 2 + e] = (jnp.where(hit0, a[4 * layer + 2:4 * layer + 3], 0.0)
                                                     + jnp.where(hit1, a[4 * layer + 3:4 * layer + 4], 0.0))
    stack = jnp.concatenate(hits, axis=0)
    ranks = jnp.where(stack > 0.5, nt(stack.astype(BF16), tri[...]), -1.0)
    for n in range(4 * N_EP):
        posr[n] = ranks[n:n + 1]

    for copy in w_copies:
        copy.wait()

    slot = lax.broadcasted_iota(jnp.int32, (CAP, n_tok), 0).astype(F32)
    slot_lane = lax.broadcasted_iota(jnp.int32, (n_tok, CAP), 1).astype(F32)
    step = 32

    def select(layer, s):
        at = (layer * N_EP + s) * 2
        return [posr[at + e] == slot for e in range(2)]

    def as_bf16(picks):
        return jnp.concatenate([p.astype(F32).astype(BF16) for p in picks], axis=0)

    def take_rows(layer, s, n, pick):
        u = ag[n, s]
        if n == 1:
            u = (u.astype(F32) + nn(u, dense2[...])).astype(BF16)
        rows = nn(pick, u).astype(BF16)
        for e in range(2):
            rows_in[layer, e, s] = rows[e * CAP:(e + 1) * CAP]

    def up_project(layer, s, e):
        rows = rows_in[layer, e, s]
        t_a[e] = nn(rows, w_gate[layer, e])
        t_b[e] = nn(rows, w_up[layer, e])

    def forward(s):
        take_rows(0, s, 0, as_bf16(select(0, s)))
        for e in range(2):
            up_project(0, s, e)
        for e in range(2):
            for i in range(CAP // step):
                r = pl.ds(i * step, step)
                a = t_a[e, r, :]
                hid[e, s, r, :] = (a * jax.nn.sigmoid(a) * t_b[e, r, :]).astype(BF16)
            ret[0, ret_at(s), e * CAP:(e + 1) * CAP] = nn(hid[e, s], w_down[0, e]).astype(BF16)

    def backward(layer, s, n_dy, n_ret, n_u):
        picks = select(layer, s)
        pick = as_bf16(picks)
        at = (layer * N_EP + s) * 2
        if n_u is not None:
            take_rows(layer, s, n_u, pick)
        got = nn(pick, ag[n_dy, s])
        for e in range(2):
            gate = jnp.sum(jnp.where(picks[e], gater[at + e], 0.0), axis=1, keepdims=True)
            g_out[e, s] = (got[e * CAP:(e + 1) * CAP] * gate).astype(BF16)
        for e in range(2):
            up_project(layer, s, e)
            t_gh[e] = nt(g_out[e, s], w_down[layer, e]).astype(BF16)
        parts = []
        for e in range(2):
            for i in range(CAP // step):
                r = pl.ds(i * step, step)
                a = t_a[e, r, :]
                b = t_b[e, r, :]
                gh = t_gh[e, r, :].astype(F32)
                sig = jax.nn.sigmoid(a)
                act = a * sig
                hid[e, s, r, :] = (act * b).astype(BF16)
                g_a[e, s, r, :] = (gh * b * sig * (1.0 + a * (1.0 - sig))).astype(BF16)
                g_b[e, s, r, :] = (gh * act).astype(BF16)
            parts.append((nt(g_a[e, s], w_gate[layer, e]) + nt(g_b[e, s], w_up[layer, e])).astype(BF16))
        ret[n_ret, ret_at(s)] = tn(pick, jnp.concatenate(parts, axis=0)).astype(BF16)

    def mix(p, base):
        acc[...] = base.astype(F32)

        def body(k, carry):
            s = order(k)

            @pl.when(k > 0)
            def _():
                ret_wait(0, p, s)

            for e in range(2):
                here = lane == s * 2 + e
                pos = jnp.sum(jnp.where(here, posc[p], 0.0), axis=1, keepdims=True)
                weight = jnp.sum(jnp.where(here, gatec[p], 0.0), axis=1, keepdims=True)
                hot = (pos == slot_lane).astype(F32).astype(BF16)
                acc[...] += nn(hot, ret[0, N_EP + p * N_EP + s, e * CAP:(e + 1) * CAP]) * weight
            return carry
        lax.fori_loop(0, N_EP, body, 0)
        return acc[...].astype(BF16)

    def add_up(n, p, base, n_from=N_EP):
        total = base.astype(F32) + ret[n, N_EP + p * N_EP + z].astype(F32)
        for k in range(1, n_from):
            ret_wait(n, p, order(k))
            total += ret[n, N_EP + p * N_EP + order(k)].astype(F32)
        return total.astype(BF16)

    chip_x = chip % 2
    chip_y = chip // 2
    over_x = chip + 1 - 2 * chip_x
    over_y = (chip + 2) % n_chip

    def group(e):
        return jnp.where(e == 0, chip_x, chip_y)

    def place(e):
        return jnp.where(e == 0, chip_y, chip_x)

    def pair_copy(layer, e, q):
        return row_copy(gs.at[1 - core, e, q], gr.at[layer, e, q], pair_send.at[layer, e, q], pair_recv.at[layer, e, q], chip * 2 + 1 - core)

    def one_copy(layer, e, q):
        return row_copy(gr.at[layer, e, q, 1 - group(e)], g2.at[layer, e, q], one_send.at[layer, e, q], one_recv.at[layer, e, q],
                        jnp.where(e == 0, over_x, over_y) * 2 + core)

    def two_copy(layer, e, q):
        return row_copy(gr.at[layer, e, q, group(e), 1 - place(e)], g3.at[layer, e, q], two_send.at[layer, e, q], two_recv.at[layer, e, q],
                        jnp.where(e == 0, over_y, over_x) * 2 + core)

    def pair_finish(layer, e, q):
        pair_copy(layer, e, q).wait()
        for g in range(2):
            for p in range(2):
                gr[layer, e, q, g, p] = (gr[layer, e, q, g, p].astype(F32) + gs[core, e, q, g, p].astype(F32)).astype(BF16)
        one_copy(layer, e, q).start()

    def one_finish(layer):
        def body(n, carry):
            e, q = n % 2, (n // 2 + 2) % 3
            one_copy(layer, e, q).wait_recv()
            for p in range(2):
                gr[layer, e, q, group(e), p] = (gr[layer, e, q, group(e), p].astype(F32) + g2[layer, e, q, p].astype(F32)).astype(BF16)
            two_copy(layer, e, q).start()
            return carry
        lax.fori_loop(0, 6, body, 0)

    def two_finish(layer):
        def body(n, carry):
            e, q = n % 2, (n // 2 + 2) % 3
            two_copy(layer, e, q).wait_recv()
            exp_v[layer, q * 2 + e] = (gr[layer, e, q, group(e), place(e)].astype(F32) + g3[layer, e, q].astype(F32)).astype(BF16)
            one_copy(layer, e, q).wait_send()
            two_copy(layer, e, q).wait_send()
            return carry
        lax.fori_loop(0, 6, body, 0)
        exp_copy(layer).start()

    def exp_copy(layer):
        return pltpu.make_async_copy(exp_v.at[layer], exp_out.at[layer], out_sem.at[layer])

    def operands(layer, e, at, n):
        rows = rows_in[layer, e, pl.ds(at, n)].reshape(n * CAP, d_model)
        outs = g_out[e, pl.ds(at, n)].reshape(n * CAP, d_model)
        return [(j, left, right[e, pl.ds(at, n)].reshape(n * CAP, d_ff))
                for j, left, right in ((2, outs, hid), (0, rows, g_a), (1, rows, g_b))]

    def weight_part(layer, at, n):
        def body(e, carry):
            for j, left, right in operands(layer, e, at, n):
                part[e, j] = tn(left, right)
            return carry
        lax.fori_loop(0, 2, body, 0)

    def split_grad(layer, e, j, grad):
        for p in range(n_dp):
            y, x = p // 4, p // 2 % 2
            gs[p % 2, e, j, jnp.where(e == 0, x, y), jnp.where(e == 0, y, x)] = grad[p * piece:(p + 1) * piece].astype(BF16)
        pair_copy(layer, e, j).start()

    def weight_grads(layer):
        def body(e, carry):
            for j, left, right in operands(layer, e, 0, N_EP):
                split_grad(layer, e, j, tn(left, right))
            return carry
        lax.fori_loop(0, 2, body, 0)
        for j in (2, 0, 1):
            for e in range(2):
                pair_finish(layer, e, j)

    def weight_rest(layer, at):
        both = [operands(layer, e, at, 2) for e in range(2)]
        todo = [(e, both[e][q]) for q in range(3) for e in range(2)]
        for k, (e, (j, left, right)) in enumerate(todo):
            split_grad(layer, e, j, tn(left, right) + part[e, j])
            if k >= 2:
                pair_finish(layer, todo[k - 2][0], todo[k - 2][1][0])
        for e, (j, _, _) in todo[4:]:
            pair_finish(layer, e, j)

    sub = piece // N_EP

    def da_copy(layer, k):
        to = (z + k) % N_EP
        return col_copy(d_send.at[layer, to], d_a.at[layer, z], da_send.at[layer, k], da_recv.at[layer, z], to)

    def db_copy(layer, k):
        to = (dp + k) % n_dp
        return row_copy(d_bs.at[layer, to], d_b.at[layer, dp], db_send.at[layer, k], db_recv.at[layer, dp], to)

    def dense_start(layer, grad):
        for q in range(N_EP):
            for p in range(n_dp):
                at = p * piece + q * sub
                d_send[layer, q, p] = grad[at:at + sub].astype(BF16)
        for k in range(1, N_EP):
            da_copy(layer, k).start()
        d_a[layer, z] = d_send[layer, z]

    def dense_middle(layer):
        for m in (1, 2):
            @pl.when(z != m)
            def _():
                col_copy(d_send.at[layer, m], d_a.at[layer, m], da_send.at[layer, 0], da_recv.at[layer, m], m).wait_recv()
        d_bs[layer] = (d_a[layer, 1].astype(F32) + d_a[layer, 2].astype(F32)).astype(BF16)
        for k in range(1, n_dp):
            db_copy(layer, k).start()

    def dense_end(layer):
        total = d_bs[layer, dp].astype(F32)
        for k in range(1, n_dp):
            frm = (dp + k) % n_dp
            row_copy(d_bs.at[layer, frm], d_b.at[layer, frm], db_send.at[layer, k], db_recv.at[layer, frm], frm).wait_recv()
            total += d_b[layer, frm].astype(F32)
        den_v[layer * sub:(layer + 1) * sub] = total.astype(BF16)
        @pl.when(inner)
        def _():
            for k in range(1, N_EP):
                da_copy(layer, k).wait_send()
        for k in range(1, n_dp):
            db_copy(layer, k).wait_send()

    def forward_step(k, carry):
        s = order(k)
        ag_step(0, k)
        forward(s)
        ret_start(0, s)
        return carry
    lax.fori_loop(0, N_EP, forward_step, 0)

    ag_pass(2, z, right=z != 1, left=z != 2)

    @pl.when(outer)
    def _():
        x_copy().start()

    @pl.when(inner)
    def _():
        ag_take(2, 3 - z)

        def body(n, carry):
            s = jnp.where(n == 0, z, near_end)
            ag[1, s] = mix(s % 2, ag[0, s])
            ag_pass(1, s)

            @pl.when(n == 1)
            def _():
                ag_to_right(2, s).wait_recv()
                ag_pass(2, s, right=z == 1, left=z == 2)
            return carry
        lax.fori_loop(0, 2, body, 0)

    def second_step(k, carry):
        s = order_owned(k)

        owned_step(1, k, s, False)

        @pl.when(jnp.logical_or(k > 2, jnp.logical_and(outer, s != z)))
        def _():
            ag_take(2, s)
        backward(1, s, 2, 1, 1)
        ret_start(1, s)
        return carry
    lax.fori_loop(0, N_EP, second_step, 0)
    weight_grads(1)

    @pl.when(inner)
    def _():
        def body(n, carry):
            s = jnp.where(n == 0, z, near_end)
            gm = add_up(1, s % 2, ag[2, s])
            g_mix[n] = gm
            ag[3, s] = (gm.astype(F32) + nt(gm, dense2[...])).astype(BF16)
            ag_pass(3, s)
            return carry
        lax.fori_loop(0, 2, body, 0)
        dense_start(1, tn(ag[1, z], g_mix[0]) + tn(ag[1, near_end], g_mix[1]))

    early_at = jnp.where(z < 2, 0, 2)
    late_at = 2 - early_at

    def first_step(k, carry):
        s = order_owned(k)

        @pl.when(jnp.logical_and(k == 2, outer))
        def _():
            weight_part(0, early_at, 2)

        @pl.when(jnp.logical_and(k == 3, outer))
        def _():
            dense_middle(1)
            one_finish(1)
        owned_step(3, k, s, True)
        backward(0, s, 3, 2, None)

        @pl.when(k != 2)
        def _():
            ret_start(2, s)

        @pl.when(jnp.logical_and(k == 2, outer))
        def _():
            merge_copy().start()
        return carry
    lax.fori_loop(0, N_EP, first_step, 0)

    @pl.when(inner)
    def _():
        dense_middle(1)
        one_finish(1)
        weight_part(0, early_at, 2)
    weight_rest(0, late_at)
    for n in range(3):
        ag_drain(n)
    for n in range(2):
        ret_drain(n)

    @pl.when(outer)
    def _():
        x_copy().wait_send()
    for k in range(1, N_EP):
        aux_copy(k).wait_send()
    @pl.when(inner)
    def _():
        merge_copy().wait_recv()
        other = 3 - z
        ret[2, other] = (ret[2, other].astype(F32) + merge_in[...].astype(F32)).astype(BF16)
        ret_copy(2, other).start()
    one_finish(0)
    two_finish(1)
    dense_end(1)

    def dx_copy():
        return pltpu.make_async_copy(dx_v, tok_out.at[pl.ds(0, n_tok)], out_sem.at[2])

    @pl.when(inner)
    def _():
        gm = add_up(2, z % 2, ag[3, z], N_EP - 1)
        dx_v[...] = (gm.astype(F32) + nt(gm, dense1[...])).astype(BF16)
        dx_copy().start()
        ge = add_up(2, near_end % 2, ag[3, near_end])
        g_mix[0] = (ge.astype(F32) + nt(ge, dense1[...])).astype(BF16)
        x_copy().wait_recv()
        dense_start(0, tn(x_ref[...], gm) + tn(x_end[...], ge))
        dx_back().start()
    dense_middle(0)
    two_finish(0)

    @pl.when(outer)
    def _():
        dx_back().wait_recv()
        dx_copy().start()
        merge_copy().wait_send()
    dense_end(0)
    den_copy = pltpu.make_async_copy(den_v, tok_out.at[pl.ds(n_tok, 2 * sub)], out_sem.at[3])
    den_copy.start()
    ag_drain(3)
    ret_drain(2)

    @pl.when(inner)
    def _():
        dx_back().wait_send()
    exp_copy(1).wait()
    exp_copy(0).wait()
    dx_copy().wait()
    den_copy.wait()


def spread(n_tok, sub, tok, exp, *refs):
    outs, tok_v, exp_v, sem = refs[:9], refs[9], refs[10], refs[11]
    parts = [(tok, tok_v), (exp, exp_v)]
    for n, (src, dst) in enumerate(parts):
        pltpu.make_async_copy(src, dst, sem.at[n]).start()
    pltpu.make_async_copy(tok, tok_v, sem.at[0]).wait()
    copies = [(tok_v.at[pl.ds(0, n_tok)], outs[0])]
    for layer in range(2):
        copies.append((tok_v.at[pl.ds(n_tok + layer * sub, sub)], outs[1 + 4 * layer]))
    for layer in range(2):
        for q in range(3):
            copies.append((exp_v.at[layer, pl.ds(2 * q, 2)], outs[2 + 4 * layer + q]))
    for n, (src, dst) in enumerate(copies):
        if n == 3:
            pltpu.make_async_copy(exp, exp_v, sem.at[1]).wait()
        pltpu.make_async_copy(src, dst, sem.at[2 + n]).start()
    for n, (src, dst) in enumerate(copies):
        pltpu.make_async_copy(src, dst, sem.at[2 + n]).wait()


def solution(mesh):
    n_dp = mesh.shape['dp']
    n_chip = n_dp // 2
    tok_spec = P(('dp', 'ep'), None)
    exp_spec = P('ep', None, None)
    layer_specs = (P(None, None), tok_spec, tok_spec, exp_spec, exp_spec, exp_spec)
    grad_specs = (P(('dp', 'ep'), None), P('ep', 'dp', None), P('ep', 'dp', None), P('ep', None, 'dp'))

    def local_step(tokens, dy_out, dense_w1, idx1, gate1, wg1, wu1, wd1, dense_w2, idx2, gate2, wg2, wu2, wd2):
        n_tok, d_model = tokens.shape
        d_ff = wg1.shape[2]
        piece = d_model // n_dp
        sub = piece // N_EP
        vmem = pl.BlockSpec(memory_space=pltpu.VMEM)
        hbm = pl.BlockSpec(memory_space=pl.ANY)
        dma = pltpu.SemaphoreType.DMA
        six = (2, 2, 3)
        outs = pl.pallas_call(
            functools.partial(kernel, n_dp),
            out_shape=(jax.ShapeDtypeStruct((n_tok + 2 * sub, d_model), BF16), jax.ShapeDtypeStruct((2, 6, piece, d_ff), BF16)),
            in_specs=[vmem] * 8 + [hbm] * 6,
            out_specs=[hbm] * 2,
            scratch_shapes=[
                pltpu.VMEM((2, 2, d_model, d_ff), BF16), pltpu.VMEM((2, 2, d_model, d_ff), BF16), pltpu.VMEM((2, 2, d_ff, d_model), BF16),
                pltpu.VMEM((8, n_tok), F32), pltpu.VMEM((N_EP, 8, n_tok), F32), pltpu.VMEM((4 * N_EP, 1, n_tok), F32), pltpu.VMEM((4 * N_EP, 1, n_tok), F32),
                pltpu.VMEM((2, n_tok, N_EXP), F32), pltpu.VMEM((2, n_tok, N_EXP), F32), pltpu.VMEM((n_tok, n_tok), BF16),
                pltpu.VMEM((4, N_EP, n_tok, d_model), BF16), pltpu.VMEM((3, 3 * N_EP, n_tok, d_model), BF16),
                pltpu.VMEM((n_tok, d_model), BF16), pltpu.VMEM((n_tok, d_model), BF16),
                pltpu.VMEM((2, 2, N_EP, CAP, d_model), BF16), pltpu.VMEM((2, CAP, d_ff), F32), pltpu.VMEM((2, CAP, d_ff), F32),
                pltpu.VMEM((2, CAP, d_ff), BF16), pltpu.VMEM((2, N_EP, CAP, d_ff), BF16), pltpu.VMEM((2, N_EP, CAP, d_ff), BF16),
                pltpu.VMEM((2, N_EP, CAP, d_ff), BF16), pltpu.VMEM((2, N_EP, CAP, d_model), BF16),
                pltpu.VMEM((n_tok, d_model), F32), pltpu.VMEM((2, n_tok, d_model), BF16),
                pltpu.VMEM((2, 3, d_model, d_ff), F32),
                *[pltpu.VMEM(six + (2, 2, piece, d_ff), BF16)] * 2, pltpu.VMEM(six + (2, piece, d_ff), BF16), pltpu.VMEM(six + (piece, d_ff), BF16),
                pltpu.VMEM((2, N_EP, n_dp, sub, d_model), BF16), pltpu.VMEM((2, N_EP, n_dp, sub, d_model), BF16),
                pltpu.VMEM((2, n_dp, sub, d_model), BF16), pltpu.VMEM((2, n_dp, sub, d_model), BF16),
                pltpu.VMEM((2, 6, piece, d_ff), BF16), pltpu.VMEM((n_tok, d_model), BF16), pltpu.VMEM((2 * sub, d_model), BF16),
                dma((6,)), dma((N_EP,)), dma((N_EP,)), *[dma((4, N_EP))] * 3, dma((3, N_EP)), dma((3, 2 * N_EP)),
                dma((3,)), dma((3,)), *[dma(six)] * 6, *[dma((2, N_EP))] * 2, *[dma((2, n_dp))] * 2, dma((4,)),
            ],
            compiler_params=pltpu.CompilerParams(collective_id=0, has_side_effects=True, vmem_limit_bytes=67043328),
        )(tokens, dy_out, dense_w1, dense_w2, idx1.T, gate1.T, idx2.T, gate2.T, wg1, wu1, wd1, wg2, wu2, wd2)
        tok, exp = outs
        grads = [jax.ShapeDtypeStruct((sub, d_model), BF16)] + [jax.ShapeDtypeStruct((2, piece, d_ff), BF16)] * 3
        res = list(pl.pallas_call(
            functools.partial(spread, n_tok, sub),
            out_shape=tuple([jax.ShapeDtypeStruct((n_tok, d_model), BF16)] + grads * 2),
            in_specs=[hbm] * 2,
            out_specs=[hbm] * 9,
            scratch_shapes=[pltpu.VMEM((n_tok + 2 * sub, d_model), BF16), pltpu.VMEM((2, 6, piece, d_ff), BF16), dma((11,))],
        )(tok, exp))
        for n in (4, 8):
            res[n] = jnp.swapaxes(res[n], 1, 2)
        return tuple(res)

    return jax.shard_map(local_step, mesh=mesh, in_specs=(tok_spec, tok_spec) + layer_specs + layer_specs,
                         out_specs=(tok_spec,) + grad_specs + grad_specs, check_vma=False)
```
